256 devices in a mesh: seq: 32 (over z, x), head: 8 (over y, core).
Axes of the slice: x: 4, y: 4, z: 8, core: 2. Of those that a mesh axis runs over, the one named last changes fastest.
Arguments:
- tokens: bfloat16 [8192, 2560], P(('seq', 'head')), may hold values from -6 to 6
- w_xz: bfloat16 [2560, 2, 5120], P(None, None, 'head'), may hold values from -0.125 to 0.125
- w_bc: bfloat16 [2560, 256], replicated, may hold values from -0.125 to 0.125
- w_dt: bfloat16 [2560, 80], P(None, 'head'), may hold values from -0.125 to 0.125
- dt_bias: float32 [80], P('head'), may hold values from -2 to 1
- a_log: float32 [80], P('head'), may hold values from -16 to 0
- conv_x: bfloat16 [4, 5120], P(None, 'head'), may hold values from -3 to 3
- conv_bc: bfloat16 [4, 256], replicated, may hold values from -3 to 3
- norm_gain: float32 [5120], P('head'), may hold values from 0.5 to 1.5
- w_out: bfloat16 [5120, 2560], P('head'), may hold values from -0.078125 to 0.078125
Outputs:
- layer_out: bfloat16 [8192, 2560], P(('seq', 'head'))
The draws below stay inside these ranges and needn't reach their ends.
All inputs are finite; a program needn't handle non-finite values.
Results may differ from the reference program's by a relative error of at most 0.02.
Values may be sent and summed in bfloat16 or wider, within the bound.
No kernel may reach another device: no remote copies, remote signals or barrier semaphores. Data moves between devices by JAX's collectives and lax.ppermute only.
A program may use at most 64 MiB of HBM per device.

```python
import jax
import jax.numpy as jnp
from jax import lax

D = 2560
HEADS = 80
HEAD_DIM = 64
STATE = 128
SPAN = 256
CONV = 4
DI = 5120
TOKENS = 8192
N_HEAD = 8


def draw_a_log(key, part):
    key_pick, key_strong, key_weak = jax.random.split(jax.random.fold_in(key, 7), 3)
    keepers = 5
    lasting = jax.random.randint(key_pick, (HEADS,), 0, 10) < keepers
    strong = jax.random.uniform(key_strong, (HEADS,), jnp.float32, jnp.log(0.03), jnp.log(0.08))
    weak = jax.random.uniform(key_weak, (HEADS,), jnp.float32, jnp.log(0.2 / TOKENS), jnp.log(1.0 / TOKENS))
    return jnp.where(lasting, weak, strong).astype(jnp.float32)


def level_of(own_key, dims, cuts, smallest, top_value):
    factor_of = 1.0
    for dim, parts in cuts:
        draws = jax.random.uniform(jax.random.fold_in(jax.random.fold_in(own_key, 6), dim), (parts,), jnp.float32, smallest / len(cuts), top_value / len(cuts))
        factor_of = factor_of * jnp.repeat(jnp.exp(draws), dims[dim] // parts).reshape((-1,) + (1,) * (len(dims) - 1 - dim))
    return factor_of


def gaussian(rng, shape, spread, bound, shards=(), kind=jnp.bfloat16):
    values = jax.random.normal(rng, shape, jnp.float32) * spread
    if len(shards) > 0:
        values = level_of(rng, shape, shards, -0.22, 0.18) * values
    return jnp.clip(values, min=-bound, max=bound).astype(kind)


def setup_inputs(seed: int = 0) -> dict:
    arg_keys = jax.random.split(jax.random.key(seed), 11)
    tokens = gaussian(arg_keys[0], (TOKENS, D), 1.0, 6.0, ((0, 256),))
    w_xz = gaussian(arg_keys[1], (D, 2, DI), D ** -0.5, 0.125, ((2, 8),))
    w_bc = gaussian(arg_keys[2], (D, 2 * STATE), D ** -0.5, 0.125)
    w_dt = gaussian(arg_keys[3], (D, HEADS), D ** -0.5, 0.125, ((1, 8),))
    dt_bias = jnp.clip(-2.0 + 3.0 * jax.random.uniform(arg_keys[4], (HEADS,), jnp.float32) ** level_of(arg_keys[4], (HEADS,), ((0, 8),), -0.2, 0.2), -2.0, 1.0)
    a_log = draw_a_log(jax.random.fold_in(arg_keys[10], 71), 0)
    conv_x = gaussian(arg_keys[6], (CONV, DI), CONV ** -0.5, 3.0, ((1, 8),))
    conv_bc = gaussian(arg_keys[7], (CONV, 2 * STATE), CONV ** -0.5, 3.0)
    norm_gain = jnp.clip(1.0 + 0.1 * jax.random.normal(arg_keys[8], (DI,), jnp.float32), 0.5, 1.5)
    w_out = gaussian(arg_keys[9], (DI, D), DI ** -0.5, 0.078125, ((0, 8),))
    return dict(tokens=tokens, w_xz=w_xz, w_bc=w_bc, w_dt=w_dt, dt_bias=dt_bias, a_log=a_log, conv_x=conv_x, conv_bc=conv_bc, norm_gain=norm_gain, w_out=w_out)


def causal_mix(values, kernel):
    kernel_size = kernel.shape[0]
    row_count = values.shape[0]
    padded = jnp.concatenate([jnp.zeros((kernel_size - 1, values.shape[1]), values.dtype), values], axis=0)
    summed = jnp.zeros(values.shape, jnp.float32)
    for offset in range(kernel_size):
        summed = summed + kernel[offset].astype(jnp.float32) * padded[offset:offset + row_count].astype(jnp.float32)
    return jax.nn.silu(summed).astype(jnp.bfloat16)

def span_update(carried, inputs):
    value_block, b_block, c_block, step_block, decay_block = inputs
    block_len = value_block.shape[0]
    cumulative = jnp.cumsum(decay_block, axis=0)
    cum_heads = cumulative.T
    differ = cum_heads[:, :, None] - cum_heads[:, None, :]
    causal_mask = (jnp.arange(block_len)[:, None] >= jnp.arange(block_len)[None, :])[None]
    scores = jnp.dot(c_block, b_block.T, preferred_element_type=jnp.float32)
    weights = jnp.where(causal_mask, jnp.exp(jnp.where(causal_mask, differ, 0.0)), 0.0)
    weights = (weights * scores[None] * step_block.T[:, None, :]).astype(jnp.bfloat16).astype(jnp.float32)
    value_wide = value_block.astype(jnp.float32)
    c_wide = c_block.astype(jnp.float32)
    b_wide = b_block.astype(jnp.float32)
    start_state = carried.astype(jnp.bfloat16).astype(jnp.float32)
    inside = jnp.einsum('hts,shp->thp', weights, value_wide, precision=lax.Precision.HIGHEST)
    carried_out = jnp.exp(cumulative)[:, :, None] * jnp.einsum('tn,hpn->thp', c_wide, start_state, precision=lax.Precision.HIGHEST)
    final_decay = cumulative[-1]
    tail_weight = jnp.exp(final_decay[None] - cumulative) * step_block
    scaled = (tail_weight[:, :, None] * value_wide).astype(jnp.bfloat16).astype(jnp.float32)
    new_state = jnp.exp(final_decay)[:, None, None] * carried + jnp.einsum('shp,sn->hpn', scaled, b_wide, precision=lax.Precision.HIGHEST)
    return (new_state, inside + carried_out)

def reference(tokens, w_xz, w_bc, w_dt, dt_bias, a_log, conv_x, conv_bc, norm_gain, w_out):
    total_rows = tokens.shape[0]
    projected = jnp.dot(tokens, w_xz.reshape(D, 2 * DI), preferred_element_type=jnp.float32).astype(jnp.bfloat16)
    value_pre = projected[:, :DI]
    gate_pre = projected[:, DI:]
    bc_pre = jnp.dot(tokens, w_bc, preferred_element_type=jnp.float32).astype(jnp.bfloat16)
    step_size = jax.nn.softplus(jnp.dot(tokens, w_dt, preferred_element_type=jnp.float32) + dt_bias[None])
    values = causal_mix(value_pre, conv_x)
    bc_mixed = causal_mix(bc_pre, conv_bc)
    b_input = bc_mixed[:, :STATE]
    c_input = bc_mixed[:, STATE:]
    log_decay = step_size * (-jnp.exp(a_log))[None]
    blocks = total_rows // SPAN
    inputs = (values.reshape(blocks, SPAN, HEADS, HEAD_DIM), b_input.reshape(blocks, SPAN, STATE), c_input.reshape(blocks, SPAN, STATE), step_size.reshape(blocks, SPAN, HEADS), log_decay.reshape(blocks, SPAN, HEADS))
    _, outputs = lax.scan(span_update, jnp.zeros((HEADS, HEAD_DIM, STATE), jnp.float32), inputs)
    ssm_out = outputs.reshape(total_rows, DI)
    gated = ssm_out * jax.nn.silu(gate_pre.astype(jnp.float32))
    scale = lax.rsqrt(lax.optimization_barrier(jnp.sum(gated * gated, axis=1, keepdims=True)) / DI + 1.0)
    normed = (gated * scale * norm_gain[None]).astype(jnp.bfloat16)
    group_width = DI // N_HEAD
    groups = normed.reshape(total_rows, N_HEAD, group_width).transpose(1, 0, 2)
    weight_groups = w_out.reshape(N_HEAD, group_width, D)

    def add_group(running, group_pair):
        part_sum = jnp.dot(group_pair[0], group_pair[1], preferred_element_type=jnp.float32).astype(jnp.bfloat16)
        part_sum = lax.optimization_barrier(part_sum)
        return (running + part_sum.astype(jnp.float32), None)
    summed, _ = lax.scan(add_group, jnp.zeros((total_rows, D), jnp.float32), (groups, weight_groups))
    return summed.astype(jnp.bfloat16)
```

```python
import jax
import jax.numpy as jnp
from jax import lax
from jax.experimental import pallas as pl
from jax.experimental.pallas import tpu as pltpu
from jax.sharding import Mesh
from jax.sharding import PartitionSpec as P

DI = 5120
SEQ = ("z", "x")
ALL = ("z", "x", "y", "c")
HEAD = ("y", "c")
BF = jnp.bfloat16
F32 = jnp.float32
ROWS = 32
BLOCK = 256
WIDTH = 640
STATE = 128
PRE = WIDTH + 2 * STATE
MODEL = 2560
WIDE = MODEL + 128
PIECE = 40


def whole(count):
    return [pl.BlockSpec(memory_space=pltpu.VMEM)] * count


def call(body, outs, args, scratch=(), flops=0, name=None):
    return pl.pallas_call(
        body,
        out_shape=[jax.ShapeDtypeStruct(s, t) for s, t in outs],
        in_specs=whole(len(args)),
        out_specs=whole(len(outs)),
        scratch_shapes=[pltpu.VMEM(s, t) for s, t in scratch],
        compiler_params=pltpu.CompilerParams(vmem_limit_bytes=24 << 20),
        cost_estimate=pl.CostEstimate(flops=flops, transcendentals=0, bytes_accessed=flops // 500),
        name=name,
    )(*args)


def shifted(value, axis, steps):
    size = lax.axis_size(axis)
    return lax.ppermute(value, axis, [(i, (i + steps) % size) for i in range(size)])


def row_at(index, rows):
    return pl.ds(pl.multiple_of(index * rows, rows), rows)


def project_kernel(t0, t1, t2, t3, o0, o1, o2, o3, w, all_out, pre_out, tail_out, dt_out):
    y, c = lax.axis_index("y"), lax.axis_index("c")
    for d, (own, other) in enumerate(((t0, o0), (t1, o1), (t2, o2), (t3, o3))):
        source = lax.rem(y + 4 - d, 4)
        all_out[row_at(source * 2 + c, ROWS), :] = own[...]
        all_out[row_at(source * 2 + 1 - c, ROWS), :] = other[...]
    tokens = all_out[...]
    for n in range(4):
        cols = slice(256 * n, 256 * n + 256)
        part = jnp.dot(tokens, w[:, cols], preferred_element_type=F32)
        if n < 3:
            pre_out[:, cols] = part.astype(BF)
            tail_out[:, cols] = part[BLOCK - 8 :].astype(BF)
        else:
            pre_out[:, 768:896] = part[:, :128].astype(BF)
            tail_out[:, 768:896] = part[BLOCK - 8 :, :128].astype(BF)
            dt_out[...] = part[:, 128:]


def gate_kernel(tokens, w, out):
    gate = jnp.dot(tokens[...], w[...], preferred_element_type=F32).astype(BF).astype(F32)
    out[...] = jax.nn.silu(gate)


def spread(value, pair):
    rows = value.shape[0]
    lane = lax.broadcasted_iota(jnp.int32, (rows, 128), 1)
    left = jnp.broadcast_to(value[:, 2 * pair : 2 * pair + 1], (rows, 128))
    right = jnp.broadcast_to(value[:, 2 * pair + 1 : 2 * pair + 2], (rows, 128))
    return jnp.where(lane < 64, left, right)


def halves(value):
    high = value.astype(BF)
    return high, (value - high.astype(F32)).astype(BF)


def decay_rows(factor):
    high, low = halves(factor)
    row = lax.broadcasted_iota(jnp.int32, factor.shape, 0)
    return jnp.where(row == 0, high.astype(F32), jnp.where(row == 1, low.astype(F32), 0.0)).astype(BF)


def local_kernel(
    pre, tail, dt_pre, conv_x, conv_bc, bias, a_log, v_out, b_out, c_out, dt_out, cum_out, p0, p1, p2, p3, ext, state
):
    x = lax.axis_index("x")
    ext[0:8, :] = tail[...].astype(F32)
    ext[8 : 8 + BLOCK, :] = pre[...].astype(F32)
    step = jax.nn.softplus(dt_pre[...] + bias[...])
    decay = step * (-jnp.exp(a_log[...]))
    row = lax.broadcasted_iota(jnp.int32, decay.shape, 0)
    cum = decay
    for k in (1, 2, 4, 8, 16, 32, 64, 128):
        cum = cum + jnp.where(row >= k, pltpu.roll(cum, k, 0), 0.0)
    dt_out[...] = step
    cum_out[...] = cum
    last = cum[BLOCK - 1 : BLOCK, :]
    tail_weight = jnp.exp(last - cum) * step

    def mixed(first, kernel, lo):
        total = jnp.zeros((BLOCK, 128), F32)
        for k in range(4):
            total = total + kernel[k : k + 1, lo : lo + 128].astype(F32) * ext[5 + k : 5 + k + BLOCK, first : first + 128]
        return jax.nn.silu(total).astype(BF)

    b = mixed(WIDTH, conv_bc, 0)
    b_out[...] = b
    c_out[...] = mixed(WIDTH + STATE, conv_bc, STATE)
    factor = jnp.broadcast_to(jnp.exp(last), (8, 128))
    b_rows = b.astype(F32).T.astype(BF)
    for pair in range(5):
        cols = slice(128 * pair, 128 * pair + 128)
        v = mixed(128 * pair, conv_x, 128 * pair)
        v_out[:, cols] = v
        scaled = (spread(tail_weight, pair) * v.astype(F32)).astype(BF)
        state[:, cols] = jnp.dot(b_rows, scaled, preferred_element_type=F32)
        extra = decay_rows(spread(factor, pair))
        for out in (p0, p1, p2, p3):
            out[32:40, cols] = extra
    for d, out in enumerate((p0, p1, p2, p3)):
        out[0:32, :] = state[row_at(lax.rem(x + d, 4), 32), :].astype(BF)


def inside_kernel(v, b, c, step, cum, out):
    scores = jnp.dot(c[...], b[...].astype(F32).T.astype(BF), preferred_element_type=F32)
    t = lax.broadcasted_iota(jnp.int32, (BLOCK, BLOCK), 0)
    s = lax.broadcasted_iota(jnp.int32, (BLOCK, BLOCK), 1)
    scores = jnp.where(t >= s, scores, 0.0)
    cum_all = cum[...]
    cum_rows = cum_all.T
    step_rows = step[...].T
    lane = lax.broadcasted_iota(jnp.int32, (BLOCK, 128), 1)
    for pair in range(5):
        cols = slice(128 * pair, 128 * pair + 128)
        value = v[:, cols]
        parts = []
        for h in (2 * pair, 2 * pair + 1):
            differ = jnp.broadcast_to(cum_all[:, h : h + 1], (BLOCK, BLOCK)) - cum_rows[h : h + 1, :]
            weight = jnp.exp(jnp.minimum(differ, 0.0)) * (scores * step_rows[h : h + 1, :])
            parts.append(jnp.dot(weight.astype(BF), value, preferred_element_type=F32))
        out[:, cols] = jnp.where(lane < 64, parts[0], parts[1])


def load_rows(pieces, held):
    x = lax.axis_index("x")
    for d, piece in enumerate(pieces):
        held[lax.rem(x + 4 - d, 4)] = piece[...].astype(F32)


def factor_of(held, k):
    return held[k, 32:33, :] + held[k, 33:34, :]


def row_total_kernel(q0, q1, q2, q3, out, held):
    load_rows((q0, q1, q2, q3), held)
    total, factor = held[0, 0:32, :], factor_of(held, 0)
    for k in range(1, 4):
        a = factor_of(held, k)
        total = total * a + held[k, 0:32, :]
        factor = factor * a
    extra = decay_rows(jnp.broadcast_to(factor, (8, WIDTH)))
    for k in range(8):
        out[k, 0:32, :] = total.astype(BF)
        out[k, 32:40, :] = extra


def incoming_kernel(q0, q1, q2, q3, totals, e0, e1, e2, e3, held, ready):
    z, x = lax.axis_index("z"), lax.axis_index("x")
    load_rows((q0, q1, q2, q3), held)
    carry = jnp.zeros((32, WIDTH), F32)
    for k in range(7):
        a = totals[k, 32:33, :].astype(F32) + totals[k, 33:34, :].astype(F32)
        carry = jnp.where(k < z, carry * a + totals[k, 0:32, :].astype(F32), carry)
    ready[0] = carry
    for k in range(3):
        carry = carry * factor_of(held, k) + held[k, 0:32, :]
        ready[k + 1] = carry
    for d, out in enumerate((e0, e1, e2, e3)):
        out[...] = ready[lax.rem(x + d, 4)].astype(BF)


def gated_kernel(e0, e1, e2, e3, c, cum, inside, gate, gain, w, g_out, sq_out, send_out, state, pick):
    x, core = lax.axis_index("x"), lax.axis_index("c")
    for d, piece in enumerate((e0, e1, e2, e3)):
        state[row_at(lax.rem(x + 4 - d, 4), 32), :] = piece[...]
    grown = jnp.exp(cum[...])
    squares = jnp.zeros((BLOCK, 128), F32)
    for pair in range(5):
        cols = slice(128 * pair, 128 * pair + 128)
        came = jnp.dot(c[...], state[:, cols], preferred_element_type=F32)
        gated = (inside[:, cols] + spread(grown, pair) * came) * gate[:, cols]
        squares = squares + gated * gated
        g_out[:, cols] = (gated * gain[:, cols]).astype(BF)
    sq_out[...] = jnp.broadcast_to(jnp.sum(squares, axis=1, keepdims=True), (BLOCK, 128))
    for k in range(4):
        rows = row_at(2 * k + 1 - core, ROWS)
        pick[32 * k : 32 * k + 32, :] = g_out[rows, :]
        send_out[32 * k : 32 * k + 32, MODEL:] = square_cols(sq_out[rows, :])
    left = pick[...]
    for n in range(10):
        cols = slice(256 * n, 256 * n + 256)
        send_out[:, cols] = jnp.dot(left, w[:, cols], preferred_element_type=F32).astype(BF)


def square_cols(total):
    high, low = halves(total)
    lane = lax.broadcasted_iota(jnp.int32, total.shape, 1)
    return jnp.where(lane == 0, high.astype(F32), jnp.where(lane == 1, low.astype(F32), 0.0)).astype(BF)


def own_kernel(g, sq, w, out, pick):
    core = lax.axis_index("c")
    lane = lax.broadcasted_iota(jnp.int32, (ROWS, 128), 1)
    for k in range(4):
        rows = row_at(2 * k + core, ROWS)
        pick[32 * k : 32 * k + 32, :] = g[rows, :]
        out[32 * k : 32 * k + 32, MODEL:] = jnp.where(lane == 0, sq[rows, :], 0.0)
    left = pick[...]
    for n in range(10):
        cols = slice(256 * n, 256 * n + 256)
        out[:, cols] = jnp.dot(left, w[:, cols], preferred_element_type=F32)


def pair_kernel(own, came, f0, f1, f2, f3):
    y = lax.axis_index("y")
    for d, out in enumerate((f0, f1, f2, f3)):
        rows = row_at(lax.rem(y + d, 4), ROWS)
        total = own[rows, :] + came[rows, :].astype(F32)
        out[:, :MODEL] = total[:, :MODEL].astype(out.dtype)
        both = jnp.sum(total[:, MODEL:], axis=1, keepdims=True)
        out[:, MODEL:] = square_cols(jnp.broadcast_to(both, (ROWS, 128))).astype(out.dtype)


def finish_kernel(f0, g1, g2, g3, out):
    total = f0[...] + g1[...].astype(F32) + g2[...].astype(F32) + g3[...].astype(F32)
    squares = jnp.sum(total[:, MODEL:], axis=1, keepdims=True)
    out[...] = (total[:, :MODEL] * lax.rsqrt(squares / DI + 1.0)).astype(BF)


def body(tokens, w_xz, w_bc, w_dt, dt_bias, a_log, conv_x, conv_bc, norm_gain, w_out):
    heads = w_dt.shape[1]
    lanes = ((0, 0), (0, 128 - heads))
    near = [tokens] + [shifted(tokens, "y", d) for d in (1, 2, 3)]
    far = [shifted(piece, "c", 1) for piece in near]
    w_first = jnp.concatenate([w_xz[:, 0], w_bc, jnp.pad(w_dt, lanes)], axis=1)
    w_gate = w_xz[:, 1]
    bias = jnp.pad(dt_bias[None], lanes)
    rates = jnp.pad(a_log[None], lanes)
    everything, pre, tail, dt_pre = call(
        project_kernel,
        [((BLOCK, MODEL), BF), ((BLOCK, PRE), BF), ((8, PRE), BF), ((BLOCK, 128), F32)],
        [*near, *far, w_first],
        flops=2 * BLOCK * MODEL * 1024,
        name="project",
    )
    tail = lax.ppermute(tail, SEQ, [(i, i + 1) for i in range(31)])
    (gate,) = call(gate_kernel, [((BLOCK, WIDTH), F32)], [everything, w_gate], flops=2 * BLOCK * MODEL * WIDTH, name="gate")
    v, b, c, step, cum, p0, p1, p2, p3 = call(
        local_kernel,
        [((BLOCK, WIDTH), BF), ((BLOCK, STATE), BF), ((BLOCK, STATE), BF), ((BLOCK, 128), F32), ((BLOCK, 128), F32)]
        + [((PIECE, WIDTH), BF)] * 4,
        [pre, tail, dt_pre, conv_x, conv_bc, bias, rates],
        scratch=[((BLOCK + 8, PRE), F32), ((STATE, WIDTH), F32)],
        flops=2 * BLOCK * STATE * WIDTH,
        name="local",
    )
    rows = [p0] + [shifted(piece, "x", d) for d, piece in ((1, p1), (2, p2), (3, p3))]
    (inside,) = call(
        inside_kernel, [((BLOCK, WIDTH), F32)], [v, b, c, step, cum], flops=20 * BLOCK * BLOCK * 256, name="inside"
    )
    (totals,) = call(row_total_kernel, [((8, PIECE, WIDTH), BF)], rows, scratch=[((4, PIECE, WIDTH), F32)], name="rowtotal")
    totals = lax.all_to_all(totals, "z", 0, 0, tiled=True)
    e0, e1, e2, e3 = call(
        incoming_kernel,
        [((32, WIDTH), BF)] * 4,
        [*rows, totals],
        scratch=[((4, PIECE, WIDTH), F32), ((4, 32, WIDTH), F32)],
        name="incoming",
    )
    states = [e0] + [shifted(piece, "x", d) for d, piece in ((1, e1), (2, e2), (3, e3))]
    g, squares, send = call(
        gated_kernel,
        [((BLOCK, WIDTH), BF), ((BLOCK, 128), F32), ((128, WIDE), BF)],
        [*states, c, cum, inside, gate, norm_gain[None], w_out],
        scratch=[((STATE, WIDTH), BF), ((128, WIDTH), BF)],
        flops=2 * 128 * WIDTH * MODEL,
        name="gated",
    )
    came = shifted(send, "c", 1)
    (own,) = call(
        own_kernel, [((128, WIDE), F32)], [g, squares, w_out], scratch=[((128, WIDTH), BF)], flops=2 * 128 * WIDTH * MODEL, name="own"
    )
    f0, f1, f2, f3 = call(pair_kernel, [((ROWS, WIDE), F32)] + [((ROWS, WIDE), BF)] * 3, [own, came], name="pair")
    parts = [f0] + [shifted(piece, "y", d) for d, piece in ((1, f1), (2, f2), (3, f3))]
    (out,) = call(finish_kernel, [((ROWS, MODEL), BF)], parts, name="finish")
    return out


def solution(mesh):
    split = Mesh(mesh.devices.reshape(8, 4, 4, 2), ALL)
    in_specs = (
        P(ALL, None),
        P(None, None, HEAD),
        P(),
        P(None, HEAD),
        P(HEAD),
        P(HEAD),
        P(None, HEAD),
        P(),
        P(HEAD),
        P(HEAD, None),
    )
    return jax.shard_map(body, mesh=split, in_specs=in_specs, out_specs=P(ALL, None), check_vma=False)
```

```python
import jax
import jax.numpy as jnp
from jax import lax
from jax.experimental import pallas as pl
from jax.experimental.pallas import tpu as pltpu
from jax.sharding import Mesh
from jax.sharding import PartitionSpec as P

DI = 5120
SEQ = ("z", "x")
ALL = ("z", "x", "y", "c")
HEAD = ("y", "c")
BF = jnp.bfloat16
F32 = jnp.float32
ROWS = 32
BLOCK = 256
WIDTH = 640
STATE = 128
PRE = WIDTH + 2 * STATE
MODEL = 2560
WIDE = MODEL + 128
PIECE = 40


def whole(count):
    return [pl.BlockSpec(memory_space=pltpu.VMEM)] * count


def call(body, outs, args, scratch=(), flops=0, name=None):
    return pl.pallas_call(
        body,
        out_shape=[jax.ShapeDtypeStruct(s, t) for s, t in outs],
        in_specs=whole(len(args)),
        out_specs=whole(len(outs)),
        scratch_shapes=[pltpu.VMEM(s, t) for s, t in scratch],
        compiler_params=pltpu.CompilerParams(vmem_limit_bytes=24 << 20),
        cost_estimate=pl.CostEstimate(flops=flops, transcendentals=0, bytes_accessed=flops // 500),
        name=name,
    )(*args)


def shifted(value, axis, steps):
    size = lax.axis_size(axis)
    return lax.ppermute(value, axis, [(i, (i + steps) % size) for i in range(size)])


def row_at(index, rows):
    return pl.ds(pl.multiple_of(index * rows, rows), rows)


def project_kernel(t0, t1, t2, t3, o0, o1, o2, o3, w, w_bc, w_dt, early, all_out, pre_out, tail_out, dt_out, w_steps):
    y, c = lax.axis_index("y"), lax.axis_index("c")
    for d, (own, other) in enumerate(((t0, o0), (t1, o1), (t2, o2), (t3, o3))):
        source = lax.rem(y + 4 - d, 4)
        all_out[row_at(source * 2 + c, ROWS), :] = own[...]
        all_out[row_at(source * 2 + 1 - c, ROWS), :] = other[...]
    tokens = all_out[...]
    w_steps[...] = jnp.zeros(w_steps.shape, BF)
    w_steps[0 : w_dt.shape[0], :] = w_dt[...]
    for lo, hi in ((0, 256), (256, 512), (512, WIDTH)):
        part = jnp.dot(tokens, w[:, lo:hi], preferred_element_type=F32).astype(BF)
        pre_out[:, lo:hi] = part
        tail_out[:, lo:hi] = part[BLOCK - 8 :]
    part = jnp.dot(tokens, w_bc[...], preferred_element_type=F32).astype(BF)
    pre_out[:, WIDTH:] = part
    tail_out[:, WIDTH:] = part[BLOCK - 8 :]
    dt_out[...] = lax.dot_general(tokens, w_steps[...], (((1,), (1,)), ((), ())), preferred_element_type=F32)


def gate_kernel(tokens, w, out):
    for lo, hi in ((0, 256), (256, 512), (512, WIDTH)):
        gate = jnp.dot(tokens[...], w[:, WIDTH + lo : WIDTH + hi], preferred_element_type=F32)
        out[:, lo:hi] = jax.nn.silu(gate.astype(BF).astype(F32))


def spread(value, pair):
    rows = value.shape[0]
    lane = lax.broadcasted_iota(jnp.int32, (rows, 128), 1)
    left = jnp.broadcast_to(value[:, 2 * pair : 2 * pair + 1], (rows, 128))
    right = jnp.broadcast_to(value[:, 2 * pair + 1 : 2 * pair + 2], (rows, 128))
    return jnp.where(lane < 64, left, right)


def halves(value):
    high = value.astype(BF)
    return high, (value - high.astype(F32)).astype(BF)


def decay_rows(factor):
    high, low = halves(factor)
    row = lax.broadcasted_iota(jnp.int32, factor.shape, 0)
    return jnp.where(row == 0, high.astype(F32), jnp.where(row == 1, low.astype(F32), 0.0)).astype(BF)


def local_kernel(
    pre,
    tail,
    dt_pre,
    conv_x,
    conv_bc,
    bias,
    a_log,
    before,
    v_out,
    b_out,
    c_out,
    dt_out,
    cum_out,
    p0,
    p1,
    p2,
    p3,
    ext,
    state,
    small,
):
    x = lax.axis_index("x")
    ext[0:8, :] = tail[...].astype(F32)
    ext[8 : 8 + BLOCK, :] = pre[...].astype(F32)
    small[...] = jnp.zeros(small.shape, F32)
    small[0:1, 0 : bias.shape[1]] = bias[...]
    small[1:2, 0 : bias.shape[1]] = a_log[...]
    step = jax.nn.softplus(dt_pre[...] + small[0:1, :])
    decay = step * (-jnp.exp(small[1:2, :]))
    row = lax.broadcasted_iota(jnp.int32, decay.shape, 0)
    cum = decay
    for k in (1, 2, 4, 8, 16, 32, 64, 128):
        cum = cum + jnp.where(row >= k, pltpu.roll(cum, k, 0), 0.0)
    dt_out[...] = step
    cum_out[...] = cum
    last = cum[BLOCK - 1 : BLOCK, :]
    tail_weight = jnp.exp(last - cum) * step

    def mixed(first, kernel, lo):
        total = jnp.zeros((BLOCK, 128), F32)
        for k in range(4):
            total = total + kernel[k : k + 1, lo : lo + 128].astype(F32) * ext[5 + k : 5 + k + BLOCK, first : first + 128]
        return jax.nn.silu(total).astype(BF)

    b = mixed(WIDTH, conv_bc, 0)
    b_out[...] = b
    c_out[...] = mixed(WIDTH + STATE, conv_bc, STATE)
    factor = jnp.broadcast_to(jnp.exp(last), (8, 128))
    b_rows = b.astype(F32).T.astype(BF)
    for pair in range(5):
        cols = slice(128 * pair, 128 * pair + 128)
        v = mixed(128 * pair, conv_x, 128 * pair)
        v_out[:, cols] = v
        scaled = (spread(tail_weight, pair) * v.astype(F32)).astype(BF)
        state[:, cols] = jnp.dot(b_rows, scaled, preferred_element_type=F32)
        extra = decay_rows(spread(factor, pair))
        for out in (p0, p1, p2, p3):
            out[32:40, cols] = extra
    for d, out in enumerate((p0, p1, p2, p3)):
        out[0:32, :] = state[row_at(lax.rem(x + d, 4), 32), :].astype(BF)


def inside_kernel(v, b, c, step, cum, out):
    scores = jnp.dot(c[...], b[...].astype(F32).T.astype(BF), preferred_element_type=F32)
    t = lax.broadcasted_iota(jnp.int32, (BLOCK, BLOCK), 0)
    s = lax.broadcasted_iota(jnp.int32, (BLOCK, BLOCK), 1)
    scores = jnp.where(t >= s, scores, 0.0)
    cum_all = cum[...]
    cum_rows = cum_all.T
    step_rows = step[...].T
    lane = lax.broadcasted_iota(jnp.int32, (BLOCK, 128), 1)
    for pair in range(5):
        cols = slice(128 * pair, 128 * pair + 128)
        value = v[:, cols]
        parts = []
        for h in (2 * pair, 2 * pair + 1):
            differ = jnp.broadcast_to(cum_all[:, h : h + 1], (BLOCK, BLOCK)) - cum_rows[h : h + 1, :]
            weight = jnp.exp(jnp.minimum(differ, 0.0)) * (scores * step_rows[h : h + 1, :])
            parts.append(jnp.dot(weight.astype(BF), value, preferred_element_type=F32))
        out[:, cols] = jnp.where(lane < 64, parts[0], parts[1])


def load_rows(pieces, held):
    x = lax.axis_index("x")
    for d, piece in enumerate(pieces):
        held[lax.rem(x + 4 - d, 4)] = piece[...].astype(F32)


def factor_of(held, k):
    return held[k, 32:33, :] + held[k, 33:34, :]


def row_total_kernel(q0, q1, q2, q3, before, out, held):
    load_rows((q0, q1, q2, q3), held)
    total, factor = held[0, 0:32, :], factor_of(held, 0)
    for k in range(1, 4):
        a = factor_of(held, k)
        total = total * a + held[k, 0:32, :]
        factor = factor * a
    extra = decay_rows(jnp.broadcast_to(factor, (8, WIDTH)))
    for k in range(8):
        out[k, 0:32, :] = total.astype(BF)
        out[k, 32:40, :] = extra


def incoming_kernel(q0, q1, q2, q3, totals, e0, e1, e2, e3, held, ready):
    z, x = lax.axis_index("z"), lax.axis_index("x")
    load_rows((q0, q1, q2, q3), held)
    carry = jnp.zeros((32, WIDTH), F32)
    for k in range(7):
        a = totals[k, 32:33, :].astype(F32) + totals[k, 33:34, :].astype(F32)
        carry = jnp.where(k < z, carry * a + totals[k, 0:32, :].astype(F32), carry)
    ready[0] = carry
    for k in range(3):
        carry = carry * factor_of(held, k) + held[k, 0:32, :]
        ready[k + 1] = carry
    for d, out in enumerate((e0, e1, e2, e3)):
        out[...] = ready[lax.rem(x + d, 4)].astype(BF)


def gated_kernel(e0, e1, e2, e3, c, cum, inside, gate, gain, w, g_out, sq_out, send_out, state, pick):
    x, core = lax.axis_index("x"), lax.axis_index("c")
    for d, piece in enumerate((e0, e1, e2, e3)):
        state[row_at(lax.rem(x + 4 - d, 4), 32), :] = piece[...]
    grown = jnp.exp(cum[...])
    squares = jnp.zeros((BLOCK, 128), F32)
    for pair in range(5):
        cols = slice(128 * pair, 128 * pair + 128)
        came = jnp.dot(c[...], state[:, cols], preferred_element_type=F32)
        gated = (inside[:, cols] + spread(grown, pair) * came) * gate[:, cols]
        squares = squares + gated * gated
        g_out[:, cols] = (gated * gain[:, cols]).astype(BF)
    sq_out[...] = jnp.broadcast_to(jnp.sum(squares, axis=1, keepdims=True), (BLOCK, 128))
    for k in range(4):
        rows = row_at(2 * k + 1 - core, ROWS)
        pick[32 * k : 32 * k + 32, :] = g_out[rows, :]
        send_out[32 * k : 32 * k + 32, MODEL:] = square_cols(sq_out[rows, :])
    left = pick[...]
    for n in range(10):
        cols = slice(256 * n, 256 * n + 256)
        send_out[:, cols] = jnp.dot(left, w[:, cols], preferred_element_type=F32).astype(BF)


def square_cols(total):
    high, low = halves(total)
    lane = lax.broadcasted_iota(jnp.int32, total.shape, 1)
    return jnp.where(lane == 0, high.astype(F32), jnp.where(lane == 1, low.astype(F32), 0.0)).astype(BF)


def own_kernel(g, sq, w, out, pick):
    core = lax.axis_index("c")
    lane = lax.broadcasted_iota(jnp.int32, (ROWS, 128), 1)
    for k in range(4):
        rows = row_at(2 * k + core, ROWS)
        pick[32 * k : 32 * k + 32, :] = g[rows, :]
        out[32 * k : 32 * k + 32, MODEL:] = jnp.where(lane == 0, sq[rows, :], 0.0)
    left = pick[...]
    for n in range(10):
        cols = slice(256 * n, 256 * n + 256)
        out[:, cols] = jnp.dot(left, w[:, cols], preferred_element_type=F32)


def pair_kernel(own, came, f0, f1, f2, f3):
    y = lax.axis_index("y")
    for d, out in enumerate((f0, f1, f2, f3)):
        rows = row_at(lax.rem(y + d, 4), ROWS)
        total = own[rows, :] + came[rows, :].astype(F32)
        out[:, :MODEL] = total[:, :MODEL].astype(out.dtype)
        both = jnp.sum(total[:, MODEL:], axis=1, keepdims=True)
        out[:, MODEL:] = square_cols(jnp.broadcast_to(both, (ROWS, 128))).astype(out.dtype)


def finish_kernel(f0, g1, g2, g3, out):
    total = f0[...] + g1[...].astype(F32) + g2[...].astype(F32) + g3[...].astype(F32)
    squares = jnp.sum(total[:, MODEL:], axis=1, keepdims=True)
    out[...] = (total[:, :MODEL] * lax.rsqrt(squares / DI + 1.0)).astype(BF)


def body(tokens, w_xz, w_bc, w_dt, dt_bias, a_log, conv_x, conv_bc, norm_gain, w_out):
    near = [tokens] + [shifted(tokens, "y", d) for d in (1, 2, 3)]
    w_both = w_xz.reshape(MODEL, 2 * WIDTH)
    near[1:] = [lax.optimization_barrier((piece, w_both))[0] for piece in near[1:]]
    far = [shifted(piece, "c", 1) for piece in near]
    gain = norm_gain[None]
    everything, pre, tail, dt_pre = call(
        project_kernel,
        [((BLOCK, MODEL), BF), ((BLOCK, PRE), BF), ((8, PRE), BF), ((BLOCK, 128), F32)],
        [*near, *far, w_both, w_bc, w_dt.T, gain],
        scratch=[((128, MODEL), BF)],
        flops=2 * BLOCK * MODEL * 1024,
        name="project",
    )
    tail = lax.ppermute(tail, SEQ, [(i, i + 1) for i in range(31)])
    (gate,) = call(gate_kernel, [((BLOCK, WIDTH), F32)], [everything, w_both], flops=2 * BLOCK * MODEL * WIDTH, name="gate")
    v, b, c, step, cum, p0, p1, p2, p3 = call(
        local_kernel,
        [((BLOCK, WIDTH), BF), ((BLOCK, STATE), BF), ((BLOCK, STATE), BF), ((BLOCK, 128), F32), ((BLOCK, 128), F32)]
        + [((PIECE, WIDTH), BF)] * 4,
        [pre, tail, dt_pre, conv_x, conv_bc, dt_bias[None], a_log[None], gate],
        scratch=[((BLOCK + 8, PRE), F32), ((STATE, WIDTH), F32), ((8, 128), F32)],
        flops=2 * BLOCK * STATE * WIDTH,
        name="local",
    )
    rows = [p0] + [shifted(piece, "x", d) for d, piece in ((1, p1), (2, p2), (3, p3))]
    (inside,) = call(
        inside_kernel, [((BLOCK, WIDTH), F32)], [v, b, c, step, cum], flops=20 * BLOCK * BLOCK * 256, name="inside"
    )
    (totals,) = call(row_total_kernel, [((8, PIECE, WIDTH), BF)], [*rows, inside], scratch=[((4, PIECE, WIDTH), F32)], name="rowtotal")
    totals = lax.all_to_all(totals, "z", 0, 0, tiled=True)
    e0, e1, e2, e3 = call(
        incoming_kernel,
        [((32, WIDTH), BF)] * 4,
        [*rows, totals],
        scratch=[((4, PIECE, WIDTH), F32), ((4, 32, WIDTH), F32)],
        name="incoming",
    )
    states = [e0] + [shifted(piece, "x", d) for d, piece in ((1, e1), (2, e2), (3, e3))]
    g, squares, send = call(
        gated_kernel,
        [((BLOCK, WIDTH), BF), ((BLOCK, 128), F32), ((128, WIDE), BF)],
        [*states, c, cum, inside, gate, gain, w_out],
        scratch=[((STATE, WIDTH), BF), ((128, WIDTH), BF)],
        flops=2 * 128 * WIDTH * MODEL,
        name="gated",
    )
    came = shifted(send, "c", 1)
    (own,) = call(
        own_kernel, [((128, WIDE), F32)], [g, squares, w_out], scratch=[((128, WIDTH), BF)], flops=2 * 128 * WIDTH * MODEL, name="own"
    )
    f0, f1, f2, f3 = call(pair_kernel, [((ROWS, WIDE), F32)] + [((ROWS, WIDE), BF)] * 3, [own, came], name="pair")
    parts = [f0] + [shifted(piece, "y", d) for d, piece in ((1, f1), (2, f2), (3, f3))]
    (out,) = call(finish_kernel, [((ROWS, MODEL), BF)], parts, name="finish")
    return out


def solution(mesh):
    split = Mesh(mesh.devices.reshape(8, 4, 4, 2), ALL)
    in_specs = (
        P(ALL, None),
        P(None, None, HEAD),
        P(),
        P(None, HEAD),
        P(HEAD),
        P(HEAD),
        P(None, HEAD),
        P(),
        P(HEAD),
        P(HEAD, None),
    )
    return jax.shard_map(body, mesh=split, in_specs=in_specs, out_specs=P(ALL, None), check_vma=False)
```

```python
import jax
import jax.numpy as jnp
from jax import lax
from jax.experimental import pallas as pl
from jax.experimental.pallas import tpu as pltpu
from jax.sharding import Mesh
from jax.sharding import PartitionSpec as P

DI = 5120
SEQ = ("z", "x")
ALL = ("z", "x", "y", "c")
HEAD = ("y", "c")
BF = jnp.bfloat16
F32 = jnp.float32
ROWS = 32
BLOCK = 256
WIDTH = 640
STATE = 128
PRE = WIDTH + 2 * STATE
MODEL = 2560
WIDE = MODEL + 128
PIECE = 40


def whole(count):
    return [pl.BlockSpec(memory_space=pltpu.VMEM)] * count


def call(body, outs, args, scratch=(), flops=0, name=None):
    return pl.pallas_call(
        body,
        out_shape=[jax.ShapeDtypeStruct(s, t) for s, t in outs],
        in_specs=whole(len(args)),
        out_specs=whole(len(outs)),
        scratch_shapes=[pltpu.VMEM(s, t) for s, t in scratch],
        compiler_params=pltpu.CompilerParams(vmem_limit_bytes=24 << 20),
        cost_estimate=pl.CostEstimate(flops=flops, transcendentals=0, bytes_accessed=flops // 500),
        name=name,
    )(*args)


def shifted(value, axis, steps):
    size = lax.axis_size(axis)
    return lax.ppermute(value, axis, [(i, (i + steps) % size) for i in range(size)])


def row_at(index, rows):
    return pl.ds(pl.multiple_of(index * rows, rows), rows)


def project_kernel(t0, t1, t2, t3, o0, o1, o2, o3, w, w_bc, w_dt, early, all_out, pre_out, tail_out, dt_out, w_steps):
    y, c = lax.axis_index("y"), lax.axis_index("c")
    for d, (own, other) in enumerate(((t0, o0), (t1, o1), (t2, o2), (t3, o3))):
        source = lax.rem(y + 4 - d, 4)
        all_out[row_at(source * 2 + c, ROWS), :] = own[...]
        all_out[row_at(source * 2 + 1 - c, ROWS), :] = other[...]
    tokens = all_out[...]
    w_steps[...] = jnp.zeros(w_steps.shape, BF)
    w_steps[0 : w_dt.shape[0], :] = w_dt[...]
    for lo, hi in ((0, 256), (256, 512), (512, WIDTH)):
        part = jnp.dot(tokens, w[:, lo:hi], preferred_element_type=F32).astype(BF)
        pre_out[:, lo:hi] = part
        tail_out[:, lo:hi] = part[BLOCK - 8 :]
    part = jnp.dot(tokens, w_bc[...], preferred_element_type=F32).astype(BF)
    pre_out[:, WIDTH:] = part
    tail_out[:, WIDTH:] = part[BLOCK - 8 :]
    dt_out[...] = lax.dot_general(tokens, w_steps[...], (((1,), (1,)), ((), ())), preferred_element_type=F32)


def gate_kernel(tokens, w, out):
    for lo, hi in ((0, 256), (256, 512), (512, WIDTH)):
        gate = jnp.dot(tokens[...], w[:, WIDTH + lo : WIDTH + hi], preferred_element_type=F32)
        out[:, lo:hi] = jax.nn.silu(gate.astype(BF).astype(F32))


def spread(value, pair):
    rows = value.shape[0]
    lane = lax.broadcasted_iota(jnp.int32, (rows, 128), 1)
    left = jnp.broadcast_to(value[:, 2 * pair : 2 * pair + 1], (rows, 128))
    right = jnp.broadcast_to(value[:, 2 * pair + 1 : 2 * pair + 2], (rows, 128))
    return jnp.where(lane < 64, left, right)


def halves(value):
    high = value.astype(BF)
    return high, (value - high.astype(F32)).astype(BF)


def decay_rows(factor):
    high, low = halves(factor)
    row = lax.broadcasted_iota(jnp.int32, factor.shape, 0)
    return jnp.where(row == 0, high.astype(F32), jnp.where(row == 1, low.astype(F32), 0.0)).astype(BF)


def local_kernel(
    pre,
    tail,
    dt_pre,
    conv_x,
    conv_bc,
    bias,
    a_log,
    before,
    v_out,
    b_out,
    c_out,
    dt_out,
    cum_out,
    p0,
    p1,
    p2,
    p3,
    ext,
    state,
    small,
):
    x = lax.axis_index("x")
    ext[0:8, :] = tail[...].astype(F32)
    ext[8 : 8 + BLOCK, :] = pre[...].astype(F32)
    small[...] = jnp.zeros(small.shape, F32)
    small[0:1, 0 : bias.shape[1]] = bias[...]
    small[1:2, 0 : bias.shape[1]] = a_log[...]
    step = jax.nn.softplus(dt_pre[...] + small[0:1, :])
    decay = step * (-jnp.exp(small[1:2, :]))
    row = lax.broadcasted_iota(jnp.int32, decay.shape, 0)
    cum = decay
    for k in (1, 2, 4, 8, 16, 32, 64, 128):
        cum = cum + jnp.where(row >= k, pltpu.roll(cum, k, 0), 0.0)
    dt_out[...] = step
    cum_out[...] = cum
    last = cum[BLOCK - 1 : BLOCK, :]
    tail_weight = jnp.exp(last - cum) * step

    def mixed(first, kernel, lo):
        total = jnp.zeros((BLOCK, 128), F32)
        for k in range(4):
            total = total + kernel[k : k + 1, lo : lo + 128].astype(F32) * ext[5 + k : 5 + k + BLOCK, first : first + 128]
        return jax.nn.silu(total).astype(BF)

    b = mixed(WIDTH, conv_bc, 0)
    b_out[...] = b
    c_out[...] = mixed(WIDTH + STATE, conv_bc, STATE)
    factor = jnp.broadcast_to(jnp.exp(last), (8, 128))
    b_rows = b.astype(F32).T.astype(BF)
    for pair in range(5):
        cols = slice(128 * pair, 128 * pair + 128)
        v = mixed(128 * pair, conv_x, 128 * pair)
        v_out[:, cols] = v
        scaled = (spread(tail_weight, pair) * v.astype(F32)).astype(BF)
        state[:, cols] = jnp.dot(b_rows, scaled, preferred_element_type=F32)
        extra = decay_rows(spread(factor, pair))
        for out in (p0, p1, p2, p3):
            out[32:40, cols] = extra
    for d, out in enumerate((p0, p1, p2, p3)):
        out[0:32, :] = state[row_at(lax.rem(x + d, 4), 32), :].astype(BF)


def inside_kernel(v, b, c, step, cum, out):
    scores = jnp.dot(c[...], b[...].astype(F32).T.astype(BF), preferred_element_type=F32)
    t = lax.broadcasted_iota(jnp.int32, (BLOCK, BLOCK), 0)
    s = lax.broadcasted_iota(jnp.int32, (BLOCK, BLOCK), 1)
    scores = jnp.where(t >= s, scores, 0.0)
    cum_all = cum[...]
    cum_rows = cum_all.T
    step_rows = step[...].T
    lane = lax.broadcasted_iota(jnp.int32, (BLOCK, 128), 1)
    for pair in range(5):
        cols = slice(128 * pair, 128 * pair + 128)
        value = v[:, cols]
        parts = []
        for h in (2 * pair, 2 * pair + 1):
            differ = jnp.broadcast_to(cum_all[:, h : h + 1], (BLOCK, BLOCK)) - cum_rows[h : h + 1, :]
            weight = jnp.exp(jnp.minimum(differ, 0.0)) * (scores * step_rows[h : h + 1, :])
            parts.append(jnp.dot(weight.astype(BF), value, preferred_element_type=F32))
        out[:, cols] = jnp.where(lane < 64, parts[0], parts[1])


def load_rows(pieces, held):
    x = lax.axis_index("x")
    for d, piece in enumerate(pieces):
        held[lax.rem(x + 4 - d, 4)] = piece[...].astype(F32)


def factor_of(held, k):
    return held[k, 32:33, :] + held[k, 33:34, :]


def pack(out, total, factor):
    out[0:32, :] = total.astype(BF)
    out[32:40, :] = decay_rows(jnp.broadcast_to(factor, (8, WIDTH)))


def unpack(ref):
    return ref[0:32, :].astype(F32), ref[32:33, :].astype(F32) + ref[33:34, :].astype(F32)


def follow(earlier, later):
    return earlier[0] * later[1] + later[0], earlier[1] * later[1]


def choose(test, yes, no):
    return jnp.where(test, yes[0], no[0]), jnp.where(test, yes[1], no[1])


def row_total_kernel(q0, q1, q2, q3, before, out, held):
    load_rows((q0, q1, q2, q3), held)
    total = held[0, 0:32, :], factor_of(held, 0)
    for k in range(1, 4):
        total = follow(total, (held[k, 0:32, :], factor_of(held, k)))
    pack(out, *total)


def two_rows(row, other):
    odd = lax.rem(lax.axis_index("z"), 2) == 1
    mine, theirs = unpack(row), unpack(other)
    return odd, theirs, follow(choose(odd, theirs, mine), choose(odd, mine, theirs))


def pair_total_kernel(row, other, out):
    pack(out, *two_rows(row, other)[2])


def quad_total_kernel(row, other, previous, out):
    pack(out, *follow(unpack(previous), two_rows(row, other)[2]))


def incoming_kernel(q0, q1, q2, q3, row, other, previous, low, high, e0, e1, e2, e3, held, ready):
    z, x = lax.axis_index("z"), lax.axis_index("x")
    load_rows((q0, q1, q2, q3), held)
    odd, theirs, _ = two_rows(row, other)
    carry = choose(odd, theirs, (jnp.zeros((32, WIDTH), F32), jnp.ones((1, WIDTH), F32)))
    second = lax.rem(z, 4) >= 2
    carry = choose(second, follow(unpack(previous), carry), carry)
    quad = choose(second, unpack(high), unpack(low))
    carry, _ = choose(z >= 4, follow(quad, carry), carry)
    ready[0] = carry
    for k in range(3):
        carry = carry * factor_of(held, k) + held[k, 0:32, :]
        ready[k + 1] = carry
    for d, out in enumerate((e0, e1, e2, e3)):
        out[...] = ready[lax.rem(x + d, 4)].astype(BF)


def gated_kernel(e0, e1, e2, e3, c, cum, inside, gate, gain, w, g_out, sq_out, send_out, state, pick):
    x, core = lax.axis_index("x"), lax.axis_index("c")
    for d, piece in enumerate((e0, e1, e2, e3)):
        state[row_at(lax.rem(x + 4 - d, 4), 32), :] = piece[...]
    grown = jnp.exp(cum[...])
    squares = jnp.zeros((BLOCK, 128), F32)
    for pair in range(5):
        cols = slice(128 * pair, 128 * pair + 128)
        came = jnp.dot(c[...], state[:, cols], preferred_element_type=F32)
        gated = (inside[:, cols] + spread(grown, pair) * came) * gate[:, cols]
        squares = squares + gated * gated
        g_out[:, cols] = (gated * gain[:, cols]).astype(BF)
    sq_out[...] = jnp.broadcast_to(jnp.sum(squares, axis=1, keepdims=True), (BLOCK, 128))
    for k in range(4):
        rows = row_at(2 * k + 1 - core, ROWS)
        pick[32 * k : 32 * k + 32, :] = g_out[rows, :]
        send_out[32 * k : 32 * k + 32, MODEL:] = square_cols(sq_out[rows, :])
    left = pick[...]
    for n in range(10):
        cols = slice(256 * n, 256 * n + 256)
        send_out[:, cols] = jnp.dot(left, w[:, cols], preferred_element_type=F32).astype(BF)


def square_cols(total):
    high, low = halves(total)
    lane = lax.broadcasted_iota(jnp.int32, total.shape, 1)
    return jnp.where(lane == 0, high.astype(F32), jnp.where(lane == 1, low.astype(F32), 0.0)).astype(BF)


def own_kernel(g, sq, w, out, pick):
    core = lax.axis_index("c")
    lane = lax.broadcasted_iota(jnp.int32, (ROWS, 128), 1)
    for k in range(4):
        rows = row_at(2 * k + core, ROWS)
        pick[32 * k : 32 * k + 32, :] = g[rows, :]
        out[32 * k : 32 * k + 32, MODEL:] = jnp.where(lane == 0, sq[rows, :], 0.0)
    left = pick[...]
    for n in range(10):
        cols = slice(256 * n, 256 * n + 256)
        out[:, cols] = jnp.dot(left, w[:, cols], preferred_element_type=F32)


def pair_kernel(own, came, f0, f1, f2, f3):
    y = lax.axis_index("y")
    for d, out in enumerate((f0, f1, f2, f3)):
        rows = row_at(lax.rem(y + d, 4), ROWS)
        total = own[rows, :] + came[rows, :].astype(F32)
        out[:, :MODEL] = total[:, :MODEL].astype(out.dtype)
        both = jnp.sum(total[:, MODEL:], axis=1, keepdims=True)
        out[:, MODEL:] = square_cols(jnp.broadcast_to(both, (ROWS, 128))).astype(out.dtype)


def finish_kernel(f0, g1, g2, g3, out):
    total = f0[...] + g1[...].astype(F32) + g2[...].astype(F32) + g3[...].astype(F32)
    squares = jnp.sum(total[:, MODEL:], axis=1, keepdims=True)
    out[...] = (total[:, :MODEL] * lax.rsqrt(squares / DI + 1.0)).astype(BF)


def body(tokens, w_xz, w_bc, w_dt, dt_bias, a_log, conv_x, conv_bc, norm_gain, w_out):
    near = [tokens] + [shifted(tokens, "y", d) for d in (1, 2, 3)]
    w_both = w_xz.reshape(MODEL, 2 * WIDTH)
    near[1:] = [lax.optimization_barrier((piece, w_both))[0] for piece in near[1:]]
    far = [shifted(piece, "c", 1) for piece in near]
    gain = norm_gain[None]
    everything, pre, tail, dt_pre = call(
        project_kernel,
        [((BLOCK, MODEL), BF), ((BLOCK, PRE), BF), ((8, PRE), BF), ((BLOCK, 128), F32)],
        [*near, *far, w_both, w_bc, w_dt.T, gain],
        scratch=[((128, MODEL), BF)],
        flops=2 * BLOCK * MODEL * 1024,
        name="project",
    )
    tail = lax.ppermute(tail, SEQ, [(i, i + 1) for i in range(31)])
    (gate,) = call(gate_kernel, [((BLOCK, WIDTH), F32)], [everything, w_both], flops=2 * BLOCK * MODEL * WIDTH, name="gate")
    v, b, c, step, cum, p0, p1, p2, p3 = call(
        local_kernel,
        [((BLOCK, WIDTH), BF), ((BLOCK, STATE), BF), ((BLOCK, STATE), BF), ((BLOCK, 128), F32), ((BLOCK, 128), F32)]
        + [((PIECE, WIDTH), BF)] * 4,
        [pre, tail, dt_pre, conv_x, conv_bc, dt_bias[None], a_log[None], gate],
        scratch=[((BLOCK + 8, PRE), F32), ((STATE, WIDTH), F32), ((8, 128), F32)],
        flops=2 * BLOCK * STATE * WIDTH,
        name="local",
    )
    rows = [p0] + [shifted(piece, "x", d) for d, piece in ((1, p1), (2, p2), (3, p3))]
    (inside,) = call(
        inside_kernel, [((BLOCK, WIDTH), F32)], [v, b, c, step, cum], flops=20 * BLOCK * BLOCK * 256, name="inside"
    )
    piece = [((PIECE, WIDTH), BF)]
    (row,) = call(row_total_kernel, piece, [*rows, inside], scratch=[((4, PIECE, WIDTH), F32)], name="rowtotal")
    other = lax.ppermute(row, "z", [(i, i ^ 1) for i in range(8)])
    (two,) = call(pair_total_kernel, piece, [row, other], name="pairtotal")
    previous = lax.ppermute(two, "z", [(0, 2), (1, 3), (4, 6), (5, 7)])
    (four,) = call(quad_total_kernel, piece, [row, other, previous], name="quadtotal")
    low = lax.ppermute(four, "z", [(2, 4), (3, 5)])
    high = lax.ppermute(four, "z", [(2, 6), (3, 7)])
    e0, e1, e2, e3 = call(
        incoming_kernel,
        [((32, WIDTH), BF)] * 4,
        [*rows, row, other, previous, low, high],
        scratch=[((4, PIECE, WIDTH), F32), ((4, 32, WIDTH), F32)],
        name="incoming",
    )
    states = [e0] + [shifted(piece, "x", d) for d, piece in ((1, e1), (2, e2), (3, e3))]
    g, squares, send = call(
        gated_kernel,
        [((BLOCK, WIDTH), BF), ((BLOCK, 128), F32), ((128, WIDE), BF)],
        [*states, c, cum, inside, gate, gain, w_out],
        scratch=[((STATE, WIDTH), BF), ((128, WIDTH), BF)],
        flops=2 * 128 * WIDTH * MODEL,
        name="gated",
    )
    came = shifted(send, "c", 1)
    (own,) = call(
        own_kernel, [((128, WIDE), F32)], [g, squares, w_out], scratch=[((128, WIDTH), BF)], flops=2 * 128 * WIDTH * MODEL, name="own"
    )
    f0, f1, f2, f3 = call(pair_kernel, [((ROWS, WIDE), F32)] + [((ROWS, WIDE), BF)] * 3, [own, came], name="pair")
    parts = [f0] + [shifted(piece, "y", d) for d, piece in ((1, f1), (2, f2), (3, f3))]
    (out,) = call(finish_kernel, [((ROWS, MODEL), BF)], parts, name="finish")
    return out


def solution(mesh):
    split = Mesh(mesh.devices.reshape(8, 4, 4, 2), ALL)
    in_specs = (
        P(ALL, None),
        P(None, None, HEAD),
        P(),
        P(None, HEAD),
        P(HEAD),
        P(HEAD),
        P(None, HEAD),
        P(),
        P(HEAD),
        P(HEAD, None),
    )
    return jax.shard_map(body, mesh=split, in_specs=in_specs, out_specs=P(ALL, None), check_vma=False)
```

```python
import jax
import jax.numpy as jnp
from jax import lax
from jax.experimental import pallas as pl
from jax.experimental.pallas import tpu as pltpu
from jax.sharding import Mesh
from jax.sharding import PartitionSpec as P

DI = 5120
SEQ = ("z", "x")
ALL = ("z", "x", "y", "c")
HEAD = ("y", "c")
BF = jnp.bfloat16
F32 = jnp.float32
ROWS = 32
BLOCK = 256
WIDTH = 640
STATE = 128
PRE = WIDTH + 2 * STATE
MODEL = 2560
WIDE = MODEL + 128
PIECE = 40


def whole(count):
    return [pl.BlockSpec(memory_space=pltpu.VMEM)] * count


def call(body, outs, args, scratch=(), flops=0, name=None):
    return pl.pallas_call(
        body,
        out_shape=[jax.ShapeDtypeStruct(s, t) for s, t in outs],
        in_specs=whole(len(args)),
        out_specs=whole(len(outs)),
        scratch_shapes=[pltpu.VMEM(s, t) for s, t in scratch],
        compiler_params=pltpu.CompilerParams(vmem_limit_bytes=24 << 20),
        cost_estimate=pl.CostEstimate(flops=flops, transcendentals=0, bytes_accessed=flops // 500),
        name=name,
    )(*args)


def shifted(value, axis, steps):
    size = lax.axis_size(axis)
    return lax.ppermute(value, axis, [(i, (i + steps) % size) for i in range(size)])


def row_at(index, rows):
    return pl.ds(pl.multiple_of(index * rows, rows), rows)


def project_kernel(t0, t1, t2, t3, o0, o1, o2, o3, w, w_bc, w_dt, early, all_out, pre_out, tail_out, dt_out, w_steps):
    y, c = lax.axis_index("y"), lax.axis_index("c")
    for d, (own, other) in enumerate(((t0, o0), (t1, o1), (t2, o2), (t3, o3))):
        source = lax.rem(y + 4 - d, 4)
        all_out[row_at(source * 2 + c, ROWS), :] = own[...]
        all_out[row_at(source * 2 + 1 - c, ROWS), :] = other[...]
    tokens = all_out[...]
    w_steps[...] = jnp.zeros(w_steps.shape, BF)
    w_steps[0 : w_dt.shape[0], :] = w_dt[...]
    for lo, hi in ((0, 256), (256, 512), (512, WIDTH)):
        part = jnp.dot(tokens, w[:, lo:hi], preferred_element_type=F32).astype(BF)
        pre_out[:, lo:hi] = part
        tail_out[:, lo:hi] = part[BLOCK - 8 :]
    part = jnp.dot(tokens, w_bc[...], preferred_element_type=F32).astype(BF)
    pre_out[:, WIDTH:] = part
    tail_out[:, WIDTH:] = part[BLOCK - 8 :]
    dt_out[...] = lax.dot_general(tokens, w_steps[...], (((1,), (1,)), ((), ())), preferred_element_type=F32)


def gate_kernel(tokens, w, out):
    for lo, hi in ((0, 256), (256, 512), (512, WIDTH)):
        gate = jnp.dot(tokens[...], w[:, WIDTH + lo : WIDTH + hi], preferred_element_type=F32)
        out[:, lo:hi] = jax.nn.silu(gate.astype(BF).astype(F32))


def spread(value, pair):
    rows = value.shape[0]
    lane = lax.broadcasted_iota(jnp.int32, (rows, 128), 1)
    left = jnp.broadcast_to(value[:, 2 * pair : 2 * pair + 1], (rows, 128))
    right = jnp.broadcast_to(value[:, 2 * pair + 1 : 2 * pair + 2], (rows, 128))
    return jnp.where(lane < 64, left, right)


def halves(value):
    high = value.astype(BF)
    return high, (value - high.astype(F32)).astype(BF)


def decay_rows(factor):
    high, low = halves(factor)
    row = lax.broadcasted_iota(jnp.int32, factor.shape, 0)
    return jnp.where(row == 0, high.astype(F32), jnp.where(row == 1, low.astype(F32), 0.0)).astype(BF)


def local_kernel(
    pre,
    tail,
    dt_pre,
    conv_x,
    conv_bc,
    bias,
    a_log,
    before,
    v_out,
    b_out,
    c_out,
    dt_out,
    cum_out,
    p0,
    p1,
    p2,
    p3,
    ext,
    state,
    small,
):
    x = lax.axis_index("x")
    ext[0:8, :] = tail[...].astype(F32)
    ext[8 : 8 + BLOCK, :] = pre[...].astype(F32)
    small[...] = jnp.zeros(small.shape, F32)
    small[0:1, 0 : bias.shape[1]] = bias[...]
    small[1:2, 0 : bias.shape[1]] = a_log[...]
    step = jax.nn.softplus(dt_pre[...] + small[0:1, :])
    decay = step * (-jnp.exp(small[1:2, :]))
    row = lax.broadcasted_iota(jnp.int32, decay.shape, 0)
    cum = decay
    for k in (1, 2, 4, 8, 16, 32, 64, 128):
        cum = cum + jnp.where(row >= k, pltpu.roll(cum, k, 0), 0.0)
    dt_out[...] = step
    cum_out[...] = cum
    last = cum[BLOCK - 1 : BLOCK, :]
    tail_weight = jnp.exp(last - cum) * step

    def mixed(first, kernel, lo):
        total = jnp.zeros((BLOCK, 128), F32)
        for k in range(4):
            total = total + kernel[k : k + 1, lo : lo + 128].astype(F32) * ext[5 + k : 5 + k + BLOCK, first : first + 128]
        return jax.nn.silu(total).astype(BF)

    b = mixed(WIDTH, conv_bc, 0)
    b_out[...] = b
    c_out[...] = mixed(WIDTH + STATE, conv_bc, STATE)
    factor = jnp.broadcast_to(jnp.exp(last), (8, 128))
    b_rows = b.astype(F32).T.astype(BF)
    for pair in range(5):
        cols = slice(128 * pair, 128 * pair + 128)
        v = mixed(128 * pair, conv_x, 128 * pair)
        v_out[:, cols] = v
        scaled = (spread(tail_weight, pair) * v.astype(F32)).astype(BF)
        state[:, cols] = jnp.dot(b_rows, scaled, preferred_element_type=F32)
        extra = decay_rows(spread(factor, pair))
        for out in (p0, p1, p2, p3):
            out[32:40, cols] = extra
    for d, out in enumerate((p0, p1, p2, p3)):
        out[0:32, :] = state[row_at(lax.rem(x + d, 4), 32), :].astype(BF)


def inside_kernel(v, b, c, step, cum, out):
    scores = jnp.dot(c[...], b[...].astype(F32).T.astype(BF), preferred_element_type=F32)
    t = lax.broadcasted_iota(jnp.int32, (BLOCK, BLOCK), 0)
    s = lax.broadcasted_iota(jnp.int32, (BLOCK, BLOCK), 1)
    scores = jnp.where(t >= s, scores, 0.0)
    cum_all = cum[...]
    cum_rows = cum_all.T
    step_rows = step[...].T
    lane = lax.broadcasted_iota(jnp.int32, (BLOCK, 128), 1)
    for pair in range(5):
        cols = slice(128 * pair, 128 * pair + 128)
        value = v[:, cols]
        parts = []
        for h in (2 * pair, 2 * pair + 1):
            differ = jnp.broadcast_to(cum_all[:, h : h + 1], (BLOCK, BLOCK)) - cum_rows[h : h + 1, :]
            weight = jnp.exp(jnp.minimum(differ, 0.0)) * (scores * step_rows[h : h + 1, :])
            parts.append(jnp.dot(weight.astype(BF), value, preferred_element_type=F32))
        out[:, cols] = jnp.where(lane < 64, parts[0], parts[1])


def load_rows(pieces, held):
    x = lax.axis_index("x")
    for d, piece in enumerate(pieces):
        held[lax.rem(x + 4 - d, 4)] = piece[...].astype(F32)


def factor_of(held, k):
    return held[k, 32:33, :] + held[k, 33:34, :]


def pack(out, total, factor):
    out[0:32, :] = total.astype(BF)
    out[32:40, :] = decay_rows(jnp.broadcast_to(factor, (8, WIDTH)))


def unpack(ref):
    return ref[0:32, :].astype(F32), ref[32:33, :].astype(F32) + ref[33:34, :].astype(F32)


def follow(earlier, later):
    return earlier[0] * later[1] + later[0], earlier[1] * later[1]


def choose(test, yes, no):
    return jnp.where(test, yes[0], no[0]), jnp.where(test, yes[1], no[1])


def row_total_kernel(q0, q1, q2, q3, before, out, held):
    load_rows((q0, q1, q2, q3), held)
    total = held[0, 0:32, :], factor_of(held, 0)
    for k in range(1, 4):
        total = follow(total, (held[k, 0:32, :], factor_of(held, k)))
    pack(out, *total)


def two_rows(row, other):
    odd = lax.rem(lax.axis_index("z"), 2) == 1
    mine, theirs = unpack(row), unpack(other)
    return odd, theirs, follow(choose(odd, theirs, mine), choose(odd, mine, theirs))


def pair_total_kernel(row, other, out):
    pack(out, *two_rows(row, other)[2])


def quad_total_kernel(row, other, previous, out):
    first = lax.axis_index("z") < 2
    mine, theirs = two_rows(row, other)[2], unpack(previous)
    pack(out, *follow(choose(first, mine, theirs), choose(first, theirs, mine)))


def incoming_kernel(q0, q1, q2, q3, row, other, previous, quad, e0, e1, e2, e3, held, ready):
    z, x = lax.axis_index("z"), lax.axis_index("x")
    load_rows((q0, q1, q2, q3), held)
    odd, theirs, _ = two_rows(row, other)
    carry = choose(odd, theirs, (jnp.zeros((32, WIDTH), F32), jnp.ones((1, WIDTH), F32)))
    second = lax.rem(z, 4) >= 2
    carry = choose(second, follow(unpack(previous), carry), carry)
    carry, _ = choose(z >= 4, follow(unpack(quad), carry), carry)
    ready[0] = carry
    for k in range(3):
        carry = carry * factor_of(held, k) + held[k, 0:32, :]
        ready[k + 1] = carry
    for d, out in enumerate((e0, e1, e2, e3)):
        out[...] = ready[lax.rem(x + d, 4)].astype(BF)


def gated_kernel(e0, e1, e2, e3, c, cum, inside, gate, gain, w, g_out, sq_out, send_out, state, pick):
    x, core = lax.axis_index("x"), lax.axis_index("c")
    for d, piece in enumerate((e0, e1, e2, e3)):
        state[row_at(lax.rem(x + 4 - d, 4), 32), :] = piece[...]
    grown = jnp.exp(cum[...])
    squares = jnp.zeros((BLOCK, 128), F32)
    for pair in range(5):
        cols = slice(128 * pair, 128 * pair + 128)
        came = jnp.dot(c[...], state[:, cols], preferred_element_type=F32)
        gated = (inside[:, cols] + spread(grown, pair) * came) * gate[:, cols]
        squares = squares + gated * gated
        g_out[:, cols] = (gated * gain[:, cols]).astype(BF)
    sq_out[...] = jnp.broadcast_to(jnp.sum(squares, axis=1, keepdims=True), (BLOCK, 128))
    for k in range(4):
        rows = row_at(2 * k + 1 - core, ROWS)
        pick[32 * k : 32 * k + 32, :] = g_out[rows, :]
        send_out[32 * k : 32 * k + 32, MODEL:] = square_cols(sq_out[rows, :])
    left = pick[...]
    for n in range(10):
        cols = slice(256 * n, 256 * n + 256)
        send_out[:, cols] = jnp.dot(left, w[:, cols], preferred_element_type=F32).astype(BF)


def square_cols(total):
    high, low = halves(total)
    lane = lax.broadcasted_iota(jnp.int32, total.shape, 1)
    return jnp.where(lane == 0, high.astype(F32), jnp.where(lane == 1, low.astype(F32), 0.0)).astype(BF)


def own_kernel(g, sq, w, out, pick):
    core = lax.axis_index("c")
    lane = lax.broadcasted_iota(jnp.int32, (ROWS, 128), 1)
    for k in range(4):
        rows = row_at(2 * k + core, ROWS)
        pick[32 * k : 32 * k + 32, :] = g[rows, :]
        out[32 * k : 32 * k + 32, MODEL:] = jnp.where(lane == 0, sq[rows, :], 0.0)
    left = pick[...]
    for n in range(10):
        cols = slice(256 * n, 256 * n + 256)
        out[:, cols] = jnp.dot(left, w[:, cols], preferred_element_type=F32)


def pair_kernel(own, came, f0, f1, f2, f3):
    y = lax.axis_index("y")
    for d, out in enumerate((f0, f1, f2, f3)):
        rows = row_at(lax.rem(y + d, 4), ROWS)
        total = own[rows, :] + came[rows, :].astype(F32)
        out[:, :MODEL] = total[:, :MODEL].astype(out.dtype)
        both = jnp.sum(total[:, MODEL:], axis=1, keepdims=True)
        out[:, MODEL:] = square_cols(jnp.broadcast_to(both, (ROWS, 128))).astype(out.dtype)


def finish_kernel(f0, g1, g2, g3, out):
    total = f0[...] + g1[...].astype(F32) + g2[...].astype(F32) + g3[...].astype(F32)
    squares = jnp.sum(total[:, MODEL:], axis=1, keepdims=True)
    out[...] = (total[:, :MODEL] * lax.rsqrt(squares / DI + 1.0)).astype(BF)


def body(tokens, w_xz, w_bc, w_dt, dt_bias, a_log, conv_x, conv_bc, norm_gain, w_out):
    near = [tokens] + [shifted(tokens, "y", d) for d in (1, 2, 3)]
    w_both = w_xz.reshape(MODEL, 2 * WIDTH)
    near[1:] = [lax.optimization_barrier((piece, w_both))[0] for piece in near[1:]]
    far = [shifted(piece, "c", 1) for piece in near]
    gain = norm_gain[None]
    everything, pre, tail, dt_pre = call(
        project_kernel,
        [((BLOCK, MODEL), BF), ((BLOCK, PRE), BF), ((8, PRE), BF), ((BLOCK, 128), F32)],
        [*near, *far, w_both, w_bc, w_dt.T, gain],
        scratch=[((128, MODEL), BF)],
        flops=2 * BLOCK * MODEL * 1024,
        name="project",
    )
    tail = lax.ppermute(tail, SEQ, [(i, i + 1) for i in range(31)])
    (gate,) = call(gate_kernel, [((BLOCK, WIDTH), F32)], [everything, w_both], flops=2 * BLOCK * MODEL * WIDTH, name="gate")
    v, b, c, step, cum, p0, p1, p2, p3 = call(
        local_kernel,
        [((BLOCK, WIDTH), BF), ((BLOCK, STATE), BF), ((BLOCK, STATE), BF), ((BLOCK, 128), F32), ((BLOCK, 128), F32)]
        + [((PIECE, WIDTH), BF)] * 4,
        [pre, tail, dt_pre, conv_x, conv_bc, dt_bias[None], a_log[None], gate],
        scratch=[((BLOCK + 8, PRE), F32), ((STATE, WIDTH), F32), ((8, 128), F32)],
        flops=2 * BLOCK * STATE * WIDTH,
        name="local",
    )
    rows = [p0] + [shifted(piece, "x", d) for d, piece in ((1, p1), (2, p2), (3, p3))]
    (inside,) = call(
        inside_kernel, [((BLOCK, WIDTH), F32)], [v, b, c, step, cum], flops=20 * BLOCK * BLOCK * 256, name="inside"
    )
    piece = [((PIECE, WIDTH), BF)]
    (row,) = call(row_total_kernel, piece, [*rows, inside], scratch=[((4, PIECE, WIDTH), F32)], name="rowtotal")
    other = lax.ppermute(row, "z", [(i, i ^ 1) for i in range(8)])
    (two,) = call(pair_total_kernel, piece, [row, other], name="pairtotal")
    previous = lax.ppermute(two, "z", [(0, 2), (1, 3), (2, 0), (3, 1), (4, 6), (5, 7)])
    (four,) = call(quad_total_kernel, piece, [row, other, previous], name="quadtotal")
    quad = lax.ppermute(four, "z", [(0, 7), (1, 6), (2, 5), (3, 4)])
    e0, e1, e2, e3 = call(
        incoming_kernel,
        [((32, WIDTH), BF)] * 4,
        [*rows, row, other, previous, quad],
        scratch=[((4, PIECE, WIDTH), F32), ((4, 32, WIDTH), F32)],
        name="incoming",
    )
    states = [e0] + [shifted(piece, "x", d) for d, piece in ((1, e1), (2, e2), (3, e3))]
    g, squares, send = call(
        gated_kernel,
        [((BLOCK, WIDTH), BF), ((BLOCK, 128), F32), ((128, WIDE), BF)],
        [*states, c, cum, inside, gate, gain, w_out],
        scratch=[((STATE, WIDTH), BF), ((128, WIDTH), BF)],
        flops=2 * 128 * WIDTH * MODEL,
        name="gated",
    )
    came = shifted(send, "c", 1)
    (own,) = call(
        own_kernel, [((128, WIDE), F32)], [g, squares, w_out], scratch=[((128, WIDTH), BF)], flops=2 * 128 * WIDTH * MODEL, name="own"
    )
    f0, f1, f2, f3 = call(pair_kernel, [((ROWS, WIDE), F32)] + [((ROWS, WIDE), BF)] * 3, [own, came], name="pair")
    parts = [f0] + [shifted(piece, "y", d) for d, piece in ((1, f1), (2, f2), (3, f3))]
    (out,) = call(finish_kernel, [((ROWS, MODEL), BF)], parts, name="finish")
    return out


def solution(mesh):
    split = Mesh(mesh.devices.reshape(8, 4, 4, 2), ALL)
    in_specs = (
        P(ALL, None),
        P(None, None, HEAD),
        P(),
        P(None, HEAD),
        P(HEAD),
        P(HEAD),
        P(None, HEAD),
        P(),
        P(HEAD),
        P(HEAD, None),
    )
    return jax.shard_map(body, mesh=split, in_specs=in_specs, out_specs=P(ALL, None), check_vma=False)
```

```python
import jax
import jax.numpy as jnp
from jax import lax
from jax.experimental import pallas as pl
from jax.experimental.pallas import tpu as pltpu
from jax.sharding import Mesh
from jax.sharding import PartitionSpec as P

DI = 5120
SEQ = ("z", "x")
ALL = ("z", "x", "y", "c")
HEAD = ("y", "c")
BF = jnp.bfloat16
F32 = jnp.float32
ROWS = 32
BLOCK = 256
WIDTH = 640
STATE = 128
PRE = WIDTH + 2 * STATE
MODEL = 2560
WIDE = MODEL + 128
PIECE = 40


def whole(count):
    return [pl.BlockSpec(memory_space=pltpu.VMEM)] * count


def call(body, outs, args, scratch=(), flops=0, name=None):
    return pl.pallas_call(
        body,
        out_shape=[jax.ShapeDtypeStruct(s, t) for s, t in outs],
        in_specs=whole(len(args)),
        out_specs=whole(len(outs)),
        scratch_shapes=[pltpu.VMEM(s, t) for s, t in scratch],
        compiler_params=pltpu.CompilerParams(vmem_limit_bytes=24 << 20),
        cost_estimate=pl.CostEstimate(flops=flops, transcendentals=0, bytes_accessed=flops // 500),
        name=name,
    )(*args)


def swapped(value, axis, mask):
    return lax.ppermute(value, axis, [(i, i ^ mask) for i in range(lax.axis_size(axis))])


def other_index(index, mask):
    return lax.bitwise_xor(index, jnp.int32(mask))


def row_at(index, rows):
    return pl.ds(pl.multiple_of(index * rows, rows), rows)


def project_kernel(t0, t1, t2, t3, o0, o1, o2, o3, w, w_bc, w_dt, early, all_out, pre_out, tail_out, dt_out, w_steps):
    y, c = lax.axis_index("y"), lax.axis_index("c")
    for d, (own, other) in enumerate(((t0, o0), (t1, o1), (t2, o2), (t3, o3))):
        source = other_index(y, d)
        all_out[row_at(source * 2 + c, ROWS), :] = own[...]
        all_out[row_at(source * 2 + 1 - c, ROWS), :] = other[...]
    tokens = all_out[...]
    w_steps[...] = jnp.zeros(w_steps.shape, BF)
    w_steps[0 : w_dt.shape[0], :] = w_dt[...]
    for lo, hi in ((0, 256), (256, 512), (512, WIDTH)):
        part = jnp.dot(tokens, w[:, lo:hi], preferred_element_type=F32).astype(BF)
        pre_out[:, lo:hi] = part
        tail_out[:, lo:hi] = part[BLOCK - 8 :]
    part = jnp.dot(tokens, w_bc[...], preferred_element_type=F32).astype(BF)
    pre_out[:, WIDTH:] = part
    tail_out[:, WIDTH:] = part[BLOCK - 8 :]
    dt_out[...] = lax.dot_general(tokens, w_steps[...], (((1,), (1,)), ((), ())), preferred_element_type=F32)


def gate_kernel(tokens, w, out):
    for lo, hi in ((0, 256), (256, 512), (512, WIDTH)):
        gate = jnp.dot(tokens[...], w[:, WIDTH + lo : WIDTH + hi], preferred_element_type=F32)
        out[:, lo:hi] = jax.nn.silu(gate.astype(BF).astype(F32))


def spread(value, pair):
    rows = value.shape[0]
    lane = lax.broadcasted_iota(jnp.int32, (rows, 128), 1)
    left = jnp.broadcast_to(value[:, 2 * pair : 2 * pair + 1], (rows, 128))
    right = jnp.broadcast_to(value[:, 2 * pair + 1 : 2 * pair + 2], (rows, 128))
    return jnp.where(lane < 64, left, right)


def halves(value):
    high = value.astype(BF)
    return high, (value - high.astype(F32)).astype(BF)


def decay_rows(factor):
    high, low = halves(factor)
    row = lax.broadcasted_iota(jnp.int32, factor.shape, 0)
    return jnp.where(row == 0, high.astype(F32), jnp.where(row == 1, low.astype(F32), 0.0)).astype(BF)


def local_kernel(
    pre,
    tail,
    dt_pre,
    conv_x,
    conv_bc,
    bias,
    a_log,
    before,
    v_out,
    b_out,
    c_out,
    dt_out,
    cum_out,
    p0,
    p1,
    p2,
    p3,
    ext,
    state,
    small,
):
    x = lax.axis_index("x")
    ext[0:8, :] = tail[...].astype(F32)
    ext[8 : 8 + BLOCK, :] = pre[...].astype(F32)
    small[...] = jnp.zeros(small.shape, F32)
    small[0:1, 0 : bias.shape[1]] = bias[...]
    small[1:2, 0 : bias.shape[1]] = a_log[...]
    step = jax.nn.softplus(dt_pre[...] + small[0:1, :])
    decay = step * (-jnp.exp(small[1:2, :]))
    row = lax.broadcasted_iota(jnp.int32, decay.shape, 0)
    cum = decay
    for k in (1, 2, 4, 8, 16, 32, 64, 128):
        cum = cum + jnp.where(row >= k, pltpu.roll(cum, k, 0), 0.0)
    dt_out[...] = step
    cum_out[...] = cum
    last = cum[BLOCK - 1 : BLOCK, :]
    tail_weight = jnp.exp(last - cum) * step

    def mixed(first, kernel, lo):
        total = jnp.zeros((BLOCK, 128), F32)
        for k in range(4):
            total = total + kernel[k : k + 1, lo : lo + 128].astype(F32) * ext[5 + k : 5 + k + BLOCK, first : first + 128]
        return jax.nn.silu(total).astype(BF)

    b = mixed(WIDTH, conv_bc, 0)
    b_out[...] = b
    c_out[...] = mixed(WIDTH + STATE, conv_bc, STATE)
    factor = jnp.broadcast_to(jnp.exp(last), (8, 128))
    b_rows = b.astype(F32).T.astype(BF)
    for pair in range(5):
        cols = slice(128 * pair, 128 * pair + 128)
        v = mixed(128 * pair, conv_x, 128 * pair)
        v_out[:, cols] = v
        scaled = (spread(tail_weight, pair) * v.astype(F32)).astype(BF)
        state[:, cols] = jnp.dot(b_rows, scaled, preferred_element_type=F32)
        extra = decay_rows(spread(factor, pair))
        for out in (p0, p1, p2, p3):
            out[32:40, cols] = extra
    for d, out in enumerate((p0, p1, p2, p3)):
        out[0:32, :] = state[row_at(other_index(x, d), 32), :].astype(BF)


def inside_kernel(v, b, c, step, cum, out):
    scores = jnp.dot(c[...], b[...].astype(F32).T.astype(BF), preferred_element_type=F32)
    t = lax.broadcasted_iota(jnp.int32, (BLOCK, BLOCK), 0)
    s = lax.broadcasted_iota(jnp.int32, (BLOCK, BLOCK), 1)
    scores = jnp.where(t >= s, scores, 0.0)
    cum_all = cum[...]
    cum_rows = cum_all.T
    step_rows = step[...].T
    lane = lax.broadcasted_iota(jnp.int32, (BLOCK, 128), 1)
    for pair in range(5):
        cols = slice(128 * pair, 128 * pair + 128)
        value = v[:, cols]
        parts = []
        for h in (2 * pair, 2 * pair + 1):
            differ = jnp.broadcast_to(cum_all[:, h : h + 1], (BLOCK, BLOCK)) - cum_rows[h : h + 1, :]
            weight = jnp.exp(jnp.minimum(differ, 0.0)) * (scores * step_rows[h : h + 1, :])
            parts.append(jnp.dot(weight.astype(BF), value, preferred_element_type=F32))
        out[:, cols] = jnp.where(lane < 64, parts[0], parts[1])


def load_rows(pieces, held):
    x = lax.axis_index("x")
    for d, piece in enumerate(pieces):
        held[other_index(x, d)] = piece[...].astype(F32)


def factor_of(held, k):
    return held[k, 32:33, :] + held[k, 33:34, :]


def pack(out, total, factor):
    out[0:32, :] = total.astype(BF)
    out[32:40, :] = decay_rows(jnp.broadcast_to(factor, (8, WIDTH)))


def unpack(ref):
    return ref[0:32, :].astype(F32), ref[32:33, :].astype(F32) + ref[33:34, :].astype(F32)


def follow(earlier, later):
    return earlier[0] * later[1] + later[0], earlier[1] * later[1]


def choose(test, yes, no):
    return jnp.where(test, yes[0], no[0]), jnp.where(test, yes[1], no[1])


def row_total_kernel(q0, q1, q2, q3, before, out, held):
    load_rows((q0, q1, q2, q3), held)
    total = held[0, 0:32, :], factor_of(held, 0)
    for k in range(1, 4):
        total = follow(total, (held[k, 0:32, :], factor_of(held, k)))
    pack(out, *total)


def two_rows(row, other):
    odd = lax.rem(lax.axis_index("z"), 2) == 1
    mine, theirs = unpack(row), unpack(other)
    return odd, theirs, follow(choose(odd, theirs, mine), choose(odd, mine, theirs))


def pair_total_kernel(row, other, out):
    pack(out, *two_rows(row, other)[2])


def quad_total_kernel(row, other, previous, out):
    first = lax.rem(lax.axis_index("z"), 4) < 2
    mine, theirs = two_rows(row, other)[2], unpack(previous)
    pack(out, *follow(choose(first, mine, theirs), choose(first, theirs, mine)))


def incoming_kernel(q0, q1, q2, q3, row, other, previous, quad, e0, e1, e2, e3, held, ready):
    z, x = lax.axis_index("z"), lax.axis_index("x")
    load_rows((q0, q1, q2, q3), held)
    odd, theirs, _ = two_rows(row, other)
    carry = choose(odd, theirs, (jnp.zeros((32, WIDTH), F32), jnp.ones((1, WIDTH), F32)))
    second = lax.rem(z, 4) >= 2
    carry = choose(second, follow(unpack(previous), carry), carry)
    carry, _ = choose(z >= 4, follow(unpack(quad), carry), carry)
    ready[0] = carry
    for k in range(3):
        carry = carry * factor_of(held, k) + held[k, 0:32, :]
        ready[k + 1] = carry
    for d, out in enumerate((e0, e1, e2, e3)):
        out[...] = ready[other_index(x, d)].astype(BF)


def gated_kernel(e0, e1, e2, e3, c, cum, inside, gate, gain, w, g_out, sq_out, send_out, state, pick):
    x, core = lax.axis_index("x"), lax.axis_index("c")
    for d, piece in enumerate((e0, e1, e2, e3)):
        state[row_at(other_index(x, d), 32), :] = piece[...]
    grown = jnp.exp(cum[...])
    squares = jnp.zeros((BLOCK, 128), F32)
    for pair in range(5):
        cols = slice(128 * pair, 128 * pair + 128)
        came = jnp.dot(c[...], state[:, cols], preferred_element_type=F32)
        gated = (inside[:, cols] + spread(grown, pair) * came) * gate[:, cols]
        squares = squares + gated * gated
        g_out[:, cols] = (gated * gain[:, cols]).astype(BF)
    sq_out[...] = jnp.broadcast_to(jnp.sum(squares, axis=1, keepdims=True), (BLOCK, 128))
    for k in range(4):
        rows = row_at(2 * k + 1 - core, ROWS)
        pick[32 * k : 32 * k + 32, :] = g_out[rows, :]
        send_out[32 * k : 32 * k + 32, MODEL:] = square_cols(sq_out[rows, :])
    left = pick[...]
    for n in range(10):
        cols = slice(256 * n, 256 * n + 256)
        send_out[:, cols] = jnp.dot(left, w[:, cols], preferred_element_type=F32).astype(BF)


def square_cols(total):
    high, low = halves(total)
    lane = lax.broadcasted_iota(jnp.int32, total.shape, 1)
    return jnp.where(lane == 0, high.astype(F32), jnp.where(lane == 1, low.astype(F32), 0.0)).astype(BF)


def own_kernel(g, sq, w, out, pick):
    core = lax.axis_index("c")
    lane = lax.broadcasted_iota(jnp.int32, (ROWS, 128), 1)
    for k in range(4):
        rows = row_at(2 * k + core, ROWS)
        pick[32 * k : 32 * k + 32, :] = g[rows, :]
        out[32 * k : 32 * k + 32, MODEL:] = jnp.where(lane == 0, sq[rows, :], 0.0)
    left = pick[...]
    for n in range(10):
        cols = slice(256 * n, 256 * n + 256)
        out[:, cols] = jnp.dot(left, w[:, cols], preferred_element_type=F32)


def pair_kernel(own, came, f0, f1, f2, f3):
    y = lax.axis_index("y")
    for d, out in enumerate((f0, f1, f2, f3)):
        rows = row_at(other_index(y, d), ROWS)
        total = own[rows, :] + came[rows, :].astype(F32)
        out[:, :MODEL] = total[:, :MODEL].astype(out.dtype)
        both = jnp.sum(total[:, MODEL:], axis=1, keepdims=True)
        out[:, MODEL:] = square_cols(jnp.broadcast_to(both, (ROWS, 128))).astype(out.dtype)


def finish_kernel(f0, g1, g2, g3, out):
    total = f0[...] + g1[...].astype(F32) + g2[...].astype(F32) + g3[...].astype(F32)
    squares = jnp.sum(total[:, MODEL:], axis=1, keepdims=True)
    out[...] = (total[:, :MODEL] * lax.rsqrt(squares / DI + 1.0)).astype(BF)


def body(tokens, w_xz, w_bc, w_dt, dt_bias, a_log, conv_x, conv_bc, norm_gain, w_out):
    near = [tokens] + [swapped(tokens, "y", d) for d in (1, 2, 3)]
    w_both = w_xz.reshape(MODEL, 2 * WIDTH)
    near[1:] = [lax.optimization_barrier((piece, w_both))[0] for piece in near[1:]]
    far = [swapped(piece, "c", 1) for piece in near]
    gain = norm_gain[None]
    everything, pre, tail, dt_pre = call(
        project_kernel,
        [((BLOCK, MODEL), BF), ((BLOCK, PRE), BF), ((8, PRE), BF), ((BLOCK, 128), F32)],
        [*near, *far, w_both, w_bc, w_dt.T, gain],
        scratch=[((128, MODEL), BF)],
        flops=2 * BLOCK * MODEL * 1024,
        name="project",
    )
    tail = lax.ppermute(tail, SEQ, [(i, i + 1) for i in range(31)])
    (gate,) = call(gate_kernel, [((BLOCK, WIDTH), F32)], [everything, w_both], flops=2 * BLOCK * MODEL * WIDTH, name="gate")
    v, b, c, step, cum, p0, p1, p2, p3 = call(
        local_kernel,
        [((BLOCK, WIDTH), BF), ((BLOCK, STATE), BF), ((BLOCK, STATE), BF), ((BLOCK, 128), F32), ((BLOCK, 128), F32)]
        + [((PIECE, WIDTH), BF)] * 4,
        [pre, tail, dt_pre, conv_x, conv_bc, dt_bias[None], a_log[None], gate],
        scratch=[((BLOCK + 8, PRE), F32), ((STATE, WIDTH), F32), ((8, 128), F32)],
        flops=2 * BLOCK * STATE * WIDTH,
        name="local",
    )
    rows = [p0] + [swapped(piece, "x", d) for d, piece in ((1, p1), (2, p2), (3, p3))]
    (inside,) = call(
        inside_kernel, [((BLOCK, WIDTH), F32)], [v, b, c, step, cum], flops=20 * BLOCK * BLOCK * 256, name="inside"
    )
    piece = [((PIECE, WIDTH), BF)]
    (row,) = call(row_total_kernel, piece, [*rows, inside], scratch=[((4, PIECE, WIDTH), F32)], name="rowtotal")
    other = swapped(row, "z", 1)
    (two,) = call(pair_total_kernel, piece, [row, other], name="pairtotal")
    previous = swapped(two, "z", 2)
    (four,) = call(quad_total_kernel, piece, [row, other, previous], name="quadtotal")
    quad = swapped(four, "z", 7)
    e0, e1, e2, e3 = call(
        incoming_kernel,
        [((32, WIDTH), BF)] * 4,
        [*rows, row, other, previous, quad],
        scratch=[((4, PIECE, WIDTH), F32), ((4, 32, WIDTH), F32)],
        name="incoming",
    )
    states = [e0] + [swapped(piece, "x", d) for d, piece in ((1, e1), (2, e2), (3, e3))]
    g, squares, send = call(
        gated_kernel,
        [((BLOCK, WIDTH), BF), ((BLOCK, 128), F32), ((128, WIDE), BF)],
        [*states, c, cum, inside, gate, gain, w_out],
        scratch=[((STATE, WIDTH), BF), ((128, WIDTH), BF)],
        flops=2 * 128 * WIDTH * MODEL,
        name="gated",
    )
    came = swapped(send, "c", 1)
    (own,) = call(
        own_kernel, [((128, WIDE), F32)], [g, squares, w_out], scratch=[((128, WIDTH), BF)], flops=2 * 128 * WIDTH * MODEL, name="own"
    )
    f0, f1, f2, f3 = call(pair_kernel, [((ROWS, WIDE), F32)] + [((ROWS, WIDE), BF)] * 3, [own, came], name="pair")
    parts = [f0] + [swapped(piece, "y", d) for d, piece in ((1, f1), (2, f2), (3, f3))]
    (out,) = call(finish_kernel, [((ROWS, MODEL), BF)], parts, name="finish")
    return out


def solution(mesh):
    split = Mesh(mesh.devices.reshape(8, 4, 4, 2), ALL)
    in_specs = (
        P(ALL, None),
        P(None, None, HEAD),
        P(),
        P(None, HEAD),
        P(HEAD),
        P(HEAD),
        P(None, HEAD),
        P(),
        P(HEAD),
        P(HEAD, None),
    )
    return jax.shard_map(body, mesh=split, in_specs=in_specs, out_specs=P(ALL, None), check_vma=False)
```

```python
import jax
import jax.numpy as jnp
from jax import lax
from jax.experimental import pallas as pl
from jax.experimental.pallas import tpu as pltpu
from jax.sharding import Mesh
from jax.sharding import PartitionSpec as P

DI = 5120
SEQ = ("z", "x")
ALL = ("z", "x", "y", "c")
HEAD = ("y", "c")
BF = jnp.bfloat16
F32 = jnp.float32
ROWS = 32
BLOCK = 256
WIDTH = 640
STATE = 128
PRE = WIDTH + 2 * STATE
MODEL = 2560
WIDE = MODEL + 128
PIECE = 40
MASKS = (0, 2, 1, 3)
TOKEN_MASKS = (0, 1, 3, 2)


def whole(count):
    return [pl.BlockSpec(memory_space=pltpu.VMEM)] * count


def call(body, outs, args, scratch=(), flops=0, name=None):
    return pl.pallas_call(
        body,
        out_shape=[jax.ShapeDtypeStruct(s, t) for s, t in outs],
        in_specs=whole(len(args)),
        out_specs=whole(len(outs)),
        scratch_shapes=[pltpu.VMEM(s, t) for s, t in scratch],
        compiler_params=pltpu.CompilerParams(vmem_limit_bytes=24 << 20),
        cost_estimate=pl.CostEstimate(flops=flops, transcendentals=0, bytes_accessed=flops // 500),
        name=name,
    )(*args)


def swapped(value, axis, mask):
    return lax.ppermute(value, axis, [(i, i ^ mask) for i in range(lax.axis_size(axis))])


def exchanged(pieces, axis, masks):
    return [swapped(piece, axis, mask) if mask else piece for mask, piece in zip(masks, pieces)]


def other_index(index, mask):
    return lax.bitwise_xor(index, jnp.int32(mask))


def row_at(index, rows):
    return pl.ds(pl.multiple_of(index * rows, rows), rows)


def project_kernel(t0, t1, t2, t3, o0, o1, o2, o3, w, w_bc, w_dt, early, all_out, pre_out, tail_out, dt_out, w_steps):
    y, c = lax.axis_index("y"), lax.axis_index("c")
    for d, own, other in zip(TOKEN_MASKS, (t0, t1, t2, t3), (o0, o1, o2, o3)):
        source = other_index(y, d)
        all_out[row_at(source * 2 + c, ROWS), :] = own[...]
        all_out[row_at(source * 2 + 1 - c, ROWS), :] = other[...]
    tokens = all_out[...]
    w_steps[...] = jnp.zeros(w_steps.shape, BF)
    w_steps[0 : w_dt.shape[0], :] = w_dt[...]
    for lo, hi in ((0, 256), (256, 512), (512, WIDTH)):
        part = jnp.dot(tokens, w[:, lo:hi], preferred_element_type=F32).astype(BF)
        pre_out[:, lo:hi] = part
        tail_out[:, lo:hi] = part[BLOCK - 8 :]
    part = jnp.dot(tokens, w_bc[...], preferred_element_type=F32).astype(BF)
    pre_out[:, WIDTH:] = part
    tail_out[:, WIDTH:] = part[BLOCK - 8 :]
    dt_out[...] = lax.dot_general(tokens, w_steps[...], (((1,), (1,)), ((), ())), preferred_element_type=F32)


def gate_kernel(tokens, w, out):
    for lo, hi in ((0, 256), (256, 512), (512, WIDTH)):
        gate = jnp.dot(tokens[...], w[:, WIDTH + lo : WIDTH + hi], preferred_element_type=F32)
        out[:, lo:hi] = jax.nn.silu(gate.astype(BF).astype(F32))


def spread(value, pair):
    rows = value.shape[0]
    lane = lax.broadcasted_iota(jnp.int32, (rows, 128), 1)
    left = jnp.broadcast_to(value[:, 2 * pair : 2 * pair + 1], (rows, 128))
    right = jnp.broadcast_to(value[:, 2 * pair + 1 : 2 * pair + 2], (rows, 128))
    return jnp.where(lane < 64, left, right)


def halves(value):
    high = value.astype(BF)
    return high, (value - high.astype(F32)).astype(BF)


def decay_rows(factor):
    high, low = halves(factor)
    row = lax.broadcasted_iota(jnp.int32, factor.shape, 0)
    return jnp.where(row == 0, high.astype(F32), jnp.where(row == 1, low.astype(F32), 0.0)).astype(BF)


def local_kernel(
    pre,
    tail,
    dt_pre,
    conv_x,
    conv_bc,
    bias,
    a_log,
    before,
    v_out,
    b_out,
    c_out,
    dt_out,
    cum_out,
    p0,
    p1,
    p2,
    p3,
    ext,
    state,
    small,
):
    x = lax.axis_index("x")
    ext[0:8, :] = tail[...].astype(F32)
    ext[8 : 8 + BLOCK, :] = pre[...].astype(F32)
    small[...] = jnp.zeros(small.shape, F32)
    small[0:1, 0 : bias.shape[1]] = bias[...]
    small[1:2, 0 : bias.shape[1]] = a_log[...]
    step = jax.nn.softplus(dt_pre[...] + small[0:1, :])
    decay = step * (-jnp.exp(small[1:2, :]))
    row = lax.broadcasted_iota(jnp.int32, decay.shape, 0)
    cum = decay
    for k in (1, 2, 4, 8, 16, 32, 64, 128):
        cum = cum + jnp.where(row >= k, pltpu.roll(cum, k, 0), 0.0)
    dt_out[...] = step
    cum_out[...] = cum
    last = cum[BLOCK - 1 : BLOCK, :]
    tail_weight = jnp.exp(last - cum) * step

    def mixed(first, kernel, lo):
        total = jnp.zeros((BLOCK, 128), F32)
        for k in range(4):
            total = total + kernel[k : k + 1, lo : lo + 128].astype(F32) * ext[5 + k : 5 + k + BLOCK, first : first + 128]
        return jax.nn.silu(total).astype(BF)

    b = mixed(WIDTH, conv_bc, 0)
    b_out[...] = b
    c_out[...] = mixed(WIDTH + STATE, conv_bc, STATE)
    factor = jnp.broadcast_to(jnp.exp(last), (8, 128))
    b_rows = b.astype(F32).T.astype(BF)
    for pair in range(5):
        cols = slice(128 * pair, 128 * pair + 128)
        v = mixed(128 * pair, conv_x, 128 * pair)
        v_out[:, cols] = v
        scaled = (spread(tail_weight, pair) * v.astype(F32)).astype(BF)
        state[:, cols] = jnp.dot(b_rows, scaled, preferred_element_type=F32)
        extra = decay_rows(spread(factor, pair))
        for out in (p0, p1, p2, p3):
            out[32:40, cols] = extra
    for d, out in zip(MASKS, (p0, p1, p2, p3)):
        out[0:32, :] = state[row_at(other_index(x, d), 32), :].astype(BF)


def inside_kernel(v, b, c, step, cum, out):
    scores = jnp.dot(c[...], b[...].astype(F32).T.astype(BF), preferred_element_type=F32)
    t = lax.broadcasted_iota(jnp.int32, (BLOCK, BLOCK), 0)
    s = lax.broadcasted_iota(jnp.int32, (BLOCK, BLOCK), 1)
    scores = jnp.where(t >= s, scores, 0.0)
    cum_all = cum[...]
    cum_rows = cum_all.T
    step_rows = step[...].T
    lane = lax.broadcasted_iota(jnp.int32, (BLOCK, 128), 1)
    for pair in range(5):
        cols = slice(128 * pair, 128 * pair + 128)
        value = v[:, cols]
        parts = []
        for h in (2 * pair, 2 * pair + 1):
            differ = jnp.broadcast_to(cum_all[:, h : h + 1], (BLOCK, BLOCK)) - cum_rows[h : h + 1, :]
            weight = jnp.exp(jnp.minimum(differ, 0.0)) * (scores * step_rows[h : h + 1, :])
            parts.append(jnp.dot(weight.astype(BF), value, preferred_element_type=F32))
        out[:, cols] = jnp.where(lane < 64, parts[0], parts[1])


def load_rows(pieces, held):
    x = lax.axis_index("x")
    for d, piece in zip(MASKS, pieces):
        held[other_index(x, d)] = piece[...].astype(F32)


def factor_of(held, k):
    return held[k, 32:33, :] + held[k, 33:34, :]


def pack(out, total, factor):
    out[0:32, :] = total.astype(BF)
    out[32:40, :] = decay_rows(jnp.broadcast_to(factor, (8, WIDTH)))


def unpack(ref):
    return ref[0:32, :].astype(F32), ref[32:33, :].astype(F32) + ref[33:34, :].astype(F32)


def follow(earlier, later):
    return earlier[0] * later[1] + later[0], earlier[1] * later[1]


def choose(test, yes, no):
    return jnp.where(test, yes[0], no[0]), jnp.where(test, yes[1], no[1])


def row_total_kernel(q0, q1, q2, q3, before, out, held):
    load_rows((q0, q1, q2, q3), held)
    total = held[0, 0:32, :], factor_of(held, 0)
    for k in range(1, 4):
        total = follow(total, (held[k, 0:32, :], factor_of(held, k)))
    pack(out, *total)


def two_rows(row, other):
    odd = lax.rem(lax.axis_index("z"), 2) == 1
    mine, theirs = unpack(row), unpack(other)
    return odd, theirs, follow(choose(odd, theirs, mine), choose(odd, mine, theirs))


def pair_total_kernel(row, other, out):
    pack(out, *two_rows(row, other)[2])


def quad_total_kernel(row, other, previous, out):
    first = lax.rem(lax.axis_index("z"), 4) < 2
    mine, theirs = two_rows(row, other)[2], unpack(previous)
    pack(out, *follow(choose(first, mine, theirs), choose(first, theirs, mine)))


def incoming_kernel(q0, q1, q2, q3, row, other, previous, quad, e0, e1, e2, e3, held, ready):
    z, x = lax.axis_index("z"), lax.axis_index("x")
    load_rows((q0, q1, q2, q3), held)
    odd, theirs, _ = two_rows(row, other)
    carry = choose(odd, theirs, (jnp.zeros((32, WIDTH), F32), jnp.ones((1, WIDTH), F32)))
    second = lax.rem(z, 4) >= 2
    carry = choose(second, follow(unpack(previous), carry), carry)
    carry, _ = choose(z >= 4, follow(unpack(quad), carry), carry)
    ready[0] = carry
    for k in range(3):
        carry = carry * factor_of(held, k) + held[k, 0:32, :]
        ready[k + 1] = carry
    for d, out in zip(MASKS, (e0, e1, e2, e3)):
        out[...] = ready[other_index(x, d)].astype(BF)


def gated_kernel(e0, e1, e2, e3, c, cum, inside, gate, gain, w, g_out, sq_out, send_out, state, pick):
    x, core = lax.axis_index("x"), lax.axis_index("c")
    for d, piece in zip(MASKS, (e0, e1, e2, e3)):
        state[row_at(other_index(x, d), 32), :] = piece[...]
    grown = jnp.exp(cum[...])
    squares = jnp.zeros((BLOCK, 128), F32)
    for pair in range(5):
        cols = slice(128 * pair, 128 * pair + 128)
        came = jnp.dot(c[...], state[:, cols], preferred_element_type=F32)
        gated = (inside[:, cols] + spread(grown, pair) * came) * gate[:, cols]
        squares = squares + gated * gated
        g_out[:, cols] = (gated * gain[:, cols]).astype(BF)
    sq_out[...] = jnp.broadcast_to(jnp.sum(squares, axis=1, keepdims=True), (BLOCK, 128))
    for k in range(4):
        rows = row_at(2 * k + 1 - core, ROWS)
        pick[32 * k : 32 * k + 32, :] = g_out[rows, :]
        send_out[32 * k : 32 * k + 32, MODEL:] = square_cols(sq_out[rows, :])
    left = pick[...]
    for n in range(10):
        cols = slice(256 * n, 256 * n + 256)
        send_out[:, cols] = jnp.dot(left, w[:, cols], preferred_element_type=F32).astype(BF)


def square_cols(total):
    high, low = halves(total)
    lane = lax.broadcasted_iota(jnp.int32, total.shape, 1)
    return jnp.where(lane == 0, high.astype(F32), jnp.where(lane == 1, low.astype(F32), 0.0)).astype(BF)


def own_kernel(g, sq, w, out, pick):
    core = lax.axis_index("c")
    lane = lax.broadcasted_iota(jnp.int32, (ROWS, 128), 1)
    for k in range(4):
        rows = row_at(2 * k + core, ROWS)
        pick[32 * k : 32 * k + 32, :] = g[rows, :]
        out[32 * k : 32 * k + 32, MODEL:] = jnp.where(lane == 0, sq[rows, :], 0.0)
    left = pick[...]
    for n in range(10):
        cols = slice(256 * n, 256 * n + 256)
        out[:, cols] = jnp.dot(left, w[:, cols], preferred_element_type=F32)


def pair_kernel(own, came, f0, f1, f2, f3):
    y = lax.axis_index("y")
    for d, out in zip(MASKS, (f0, f1, f2, f3)):
        rows = row_at(other_index(y, d), ROWS)
        total = own[rows, :] + came[rows, :].astype(F32)
        out[:, :MODEL] = total[:, :MODEL].astype(out.dtype)
        both = jnp.sum(total[:, MODEL:], axis=1, keepdims=True)
        out[:, MODEL:] = square_cols(jnp.broadcast_to(both, (ROWS, 128))).astype(out.dtype)


def finish_kernel(f0, g1, g2, g3, out):
    total = f0[...] + g1[...].astype(F32) + g2[...].astype(F32) + g3[...].astype(F32)
    squares = jnp.sum(total[:, MODEL:], axis=1, keepdims=True)
    out[...] = (total[:, :MODEL] * lax.rsqrt(squares / DI + 1.0)).astype(BF)


def body(tokens, w_xz, w_bc, w_dt, dt_bias, a_log, conv_x, conv_bc, norm_gain, w_out):
    near = exchanged([tokens] * 4, "y", TOKEN_MASKS)
    w_both = w_xz.reshape(MODEL, 2 * WIDTH)
    near[1:] = [lax.optimization_barrier((piece, w_both))[0] for piece in near[1:]]
    far = [swapped(piece, "c", 1) for piece in near]
    gain = norm_gain[None]
    everything, pre, tail, dt_pre = call(
        project_kernel,
        [((BLOCK, MODEL), BF), ((BLOCK, PRE), BF), ((8, PRE), BF), ((BLOCK, 128), F32)],
        [*near, *far, w_both, w_bc, w_dt.T, gain],
        scratch=[((128, MODEL), BF)],
        flops=2 * BLOCK * MODEL * 1024,
        name="project",
    )
    tail = lax.ppermute(tail, SEQ, [(i, i + 1) for i in range(31)])
    (gate,) = call(gate_kernel, [((BLOCK, WIDTH), F32)], [everything, w_both], flops=2 * BLOCK * MODEL * WIDTH, name="gate")
    v, b, c, step, cum, p0, p1, p2, p3 = call(
        local_kernel,
        [((BLOCK, WIDTH), BF), ((BLOCK, STATE), BF), ((BLOCK, STATE), BF), ((BLOCK, 128), F32), ((BLOCK, 128), F32)]
        + [((PIECE, WIDTH), BF)] * 4,
        [pre, tail, dt_pre, conv_x, conv_bc, dt_bias[None], a_log[None], gate],
        scratch=[((BLOCK + 8, PRE), F32), ((STATE, WIDTH), F32), ((8, 128), F32)],
        flops=2 * BLOCK * STATE * WIDTH,
        name="local",
    )
    rows = exchanged([p0, p1, p2, p3], "x", MASKS)
    (inside,) = call(
        inside_kernel, [((BLOCK, WIDTH), F32)], [v, b, c, step, cum], flops=20 * BLOCK * BLOCK * 256, name="inside"
    )
    piece = [((PIECE, WIDTH), BF)]
    (row,) = call(row_total_kernel, piece, [*rows, inside], scratch=[((4, PIECE, WIDTH), F32)], name="rowtotal")
    other = swapped(row, "z", 1)
    (two,) = call(pair_total_kernel, piece, [row, other], name="pairtotal")
    previous = swapped(two, "z", 2)
    (four,) = call(quad_total_kernel, piece, [row, other, previous], name="quadtotal")
    quad = swapped(four, "z", 7)
    e0, e1, e2, e3 = call(
        incoming_kernel,
        [((32, WIDTH), BF)] * 4,
        [*rows, row, other, previous, quad],
        scratch=[((4, PIECE, WIDTH), F32), ((4, 32, WIDTH), F32)],
        name="incoming",
    )
    states = exchanged([e0, e1, e2, e3], "x", MASKS)
    g, squares, send = call(
        gated_kernel,
        [((BLOCK, WIDTH), BF), ((BLOCK, 128), F32), ((128, WIDE), BF)],
        [*states, c, cum, inside, gate, gain, w_out],
        scratch=[((STATE, WIDTH), BF), ((128, WIDTH), BF)],
        flops=2 * 128 * WIDTH * MODEL,
        name="gated",
    )
    came = swapped(send, "c", 1)
    (own,) = call(
        own_kernel, [((128, WIDE), F32)], [g, squares, w_out], scratch=[((128, WIDTH), BF)], flops=2 * 128 * WIDTH * MODEL, name="own"
    )
    f0, f1, f2, f3 = call(pair_kernel, [((ROWS, WIDE), F32)] + [((ROWS, WIDE), BF)] * 3, [own, came], name="pair")
    parts = exchanged([f0, f1, f2, f3], "y", MASKS)
    (out,) = call(finish_kernel, [((ROWS, MODEL), BF)], parts, name="finish")
    return out


def solution(mesh):
    split = Mesh(mesh.devices.reshape(8, 4, 4, 2), ALL)
    in_specs = (
        P(ALL, None),
        P(None, None, HEAD),
        P(),
        P(None, HEAD),
        P(HEAD),
        P(HEAD),
        P(None, HEAD),
        P(),
        P(HEAD),
        P(HEAD, None),
    )
    return jax.shard_map(body, mesh=split, in_specs=in_specs, out_specs=P(ALL, None), check_vma=False)
```

```python
import jax
import jax.numpy as jnp
from jax import lax
from jax.experimental import pallas as pl
from jax.experimental.pallas import tpu as pltpu
from jax.sharding import Mesh
from jax.sharding import PartitionSpec as P

DI = 5120
SEQ = ("z", "x")
ALL = ("z", "x", "y", "c")
HEAD = ("y", "c")
BF = jnp.bfloat16
F32 = jnp.float32
ROWS = 32
BLOCK = 256
WIDTH = 640
STATE = 128
PRE = WIDTH + 2 * STATE
MODEL = 2560
WIDE = MODEL + 128
PIECE = 168
MASKS = (0, 2, 1, 3)
TOKEN_MASKS = (0, 1, 3, 2)


def whole(count):
    return [pl.BlockSpec(memory_space=pltpu.VMEM)] * count


def call(body, outs, args, scratch=(), flops=0, name=None):
    return pl.pallas_call(
        body,
        out_shape=[jax.ShapeDtypeStruct(s, t) for s, t in outs],
        in_specs=whole(len(args)),
        out_specs=whole(len(outs)),
        scratch_shapes=[pltpu.VMEM(s, t) for s, t in scratch],
        compiler_params=pltpu.CompilerParams(vmem_limit_bytes=24 << 20),
        cost_estimate=pl.CostEstimate(flops=flops, transcendentals=0, bytes_accessed=flops // 500),
        name=name,
    )(*args)


def swapped(value, axis, mask):
    return lax.ppermute(value, axis, [(i, i ^ mask) for i in range(lax.axis_size(axis))])


def exchanged(pieces, axis, masks):
    return [swapped(piece, axis, mask) if mask else piece for mask, piece in zip(masks, pieces)]


def other_index(index, mask):
    return lax.bitwise_xor(index, jnp.int32(mask))


def row_at(index, rows):
    return pl.ds(pl.multiple_of(index * rows, rows), rows)


def project_kernel(t0, t1, t2, t3, o0, o1, o2, o3, w, w_bc, w_dt, early, all_out, pre_out, tail_out, dt_out, w_steps):
    y, c = lax.axis_index("y"), lax.axis_index("c")
    for d, own, other in zip(TOKEN_MASKS, (t0, t1, t2, t3), (o0, o1, o2, o3)):
        source = other_index(y, d)
        all_out[row_at(source * 2 + c, ROWS), :] = own[...]
        all_out[row_at(source * 2 + 1 - c, ROWS), :] = other[...]
    tokens = all_out[...]
    w_steps[...] = jnp.zeros(w_steps.shape, BF)
    w_steps[0 : w_dt.shape[0], :] = w_dt[...]
    for lo, hi in ((0, 256), (256, 512), (512, WIDTH)):
        part = jnp.dot(tokens, w[:, lo:hi], preferred_element_type=F32).astype(BF)
        pre_out[:, lo:hi] = part
        tail_out[:, lo:hi] = part[BLOCK - 8 :]
    part = jnp.dot(tokens, w_bc[...], preferred_element_type=F32).astype(BF)
    pre_out[:, WIDTH:] = part
    tail_out[:, WIDTH:] = part[BLOCK - 8 :]
    dt_out[...] = lax.dot_general(tokens, w_steps[...], (((1,), (1,)), ((), ())), preferred_element_type=F32)


def gate_kernel(tokens, w, before, out):
    for lo, hi in ((0, 256), (256, 512), (512, WIDTH)):
        gate = jnp.dot(tokens[...], w[:, WIDTH + lo : WIDTH + hi], preferred_element_type=F32)
        out[:, lo:hi] = jax.nn.silu(gate.astype(BF).astype(F32))


def spread(value, pair):
    rows = value.shape[0]
    lane = lax.broadcasted_iota(jnp.int32, (rows, 128), 1)
    left = jnp.broadcast_to(value[:, 2 * pair : 2 * pair + 1], (rows, 128))
    right = jnp.broadcast_to(value[:, 2 * pair + 1 : 2 * pair + 2], (rows, 128))
    return jnp.where(lane < 64, left, right)


def halves(value):
    high = value.astype(BF)
    return high, (value - high.astype(F32)).astype(BF)


def mixed(ext, first, kernel, lo, rows):
    total = jnp.zeros((rows, 128), F32)
    for k in range(4):
        total = total + kernel[k : k + 1, lo : lo + 128].astype(F32) * ext[5 + k : 5 + k + rows, first : first + 128]
    return jax.nn.silu(total).astype(BF)


def prepare_kernel(
    pre,
    dt_pre,
    conv_x,
    conv_bc,
    bias,
    a_log,
    v_out,
    b_out,
    c_out,
    dt_out,
    cum_out,
    weight_out,
    factor_out,
    state_out,
    ext,
    small,
):
    ext[0:8, :] = jnp.zeros((8, PRE), F32)
    ext[8 : 8 + BLOCK, :] = pre[...].astype(F32)
    small[...] = jnp.zeros(small.shape, F32)
    small[0:1, 0 : bias.shape[1]] = bias[...]
    small[1:2, 0 : bias.shape[1]] = a_log[...]
    step = jax.nn.softplus(dt_pre[...] + small[0:1, :])
    decay = step * (-jnp.exp(small[1:2, :]))
    row = lax.broadcasted_iota(jnp.int32, decay.shape, 0)
    cum = decay
    for k in (1, 2, 4, 8, 16, 32, 64, 128):
        cum = cum + jnp.where(row >= k, pltpu.roll(cum, k, 0), 0.0)
    dt_out[...] = step
    cum_out[...] = cum
    last = cum[BLOCK - 1 : BLOCK, :]
    weight = jnp.exp(last - cum) * step
    weight_out[...] = weight[0:8, :]
    factor_out[...] = jnp.broadcast_to(jnp.exp(last), (8, 128))
    weight = jnp.where(row >= 3, weight, 0.0)
    b = mixed(ext, WIDTH, conv_bc, 0, BLOCK)
    b_out[...] = b
    c_out[...] = mixed(ext, WIDTH + STATE, conv_bc, STATE, BLOCK)
    b_rows = b.astype(F32).T.astype(BF)
    for pair in range(5):
        cols = slice(128 * pair, 128 * pair + 128)
        v = mixed(ext, 128 * pair, conv_x, 128 * pair, BLOCK)
        v_out[:, cols] = v
        scaled = (spread(weight, pair) * v.astype(F32)).astype(BF)
        state_out[:, cols] = jnp.dot(b_rows, scaled, preferred_element_type=F32)


def decay_rows(factor):
    high, low = halves(factor)
    row = lax.broadcasted_iota(jnp.int32, (8, 128), 0)
    return jnp.where(row == 0, high.astype(F32), jnp.where(row == 1, low.astype(F32), 0.0)).astype(BF)


def local_kernel(tail, pre, conv_x, conv_bc, weight, factor, main, v_out, b_out, c_out, p0, p1, p2, p3, ext, state):
    x = lax.axis_index("x")
    first = jnp.logical_and(lax.axis_index("z") == 0, x == 0)
    ext[0:8, :] = jnp.where(first, 0.0, tail[...].astype(F32))
    ext[8:16, :] = pre[0:8, :].astype(F32)
    b = mixed(ext, WIDTH, conv_bc, 0, 8)
    b_out[...] = b
    c_out[...] = mixed(ext, WIDTH + STATE, conv_bc, STATE, 8)
    b_rows = jnp.broadcast_to(b.astype(F32)[None], (16, 8, 128)).reshape(128, 128).T
    extra = decay_rows(factor[0:1, :])
    for pair in range(5):
        cols = slice(128 * pair, 128 * pair + 128)
        v = mixed(ext, 128 * pair, conv_x, 128 * pair, 8)
        v_out[:, cols] = v
        scaled = (spread(weight[...], pair) * v.astype(F32)).astype(BF).astype(F32)
        total = main[:, cols]
        for k in range(3):
            total = total + b_rows[:, k : k + 1] * scaled[k : k + 1, :]
        state[:, cols] = total
    for d, out in zip(MASKS, (p0, p1, p2, p3)):
        rows = row_at(other_index(x, d), 32)
        for pair in range(5):
            out[32 * pair : 32 * pair + 32, :] = state[rows, 128 * pair : 128 * pair + 128].astype(BF)
        out[160:168, :] = extra


def inside_kernel(v, b, c, v_first, b_first, c_first, step, cum, out, c_out, values, b_all):
    values[...] = v[...]
    values[0:8, :] = v_first[...]
    b_all[...] = b[...]
    b_all[0:8, :] = b_first[...]
    c_out[...] = c[...]
    c_out[0:8, :] = c_first[...]
    scores = jnp.dot(c_out[...], b_all[...].astype(F32).T.astype(BF), preferred_element_type=F32)
    t = lax.broadcasted_iota(jnp.int32, (BLOCK, BLOCK), 0)
    s = lax.broadcasted_iota(jnp.int32, (BLOCK, BLOCK), 1)
    scores = jnp.where(t >= s, scores, 0.0)
    cum_all = cum[...]
    cum_rows = cum_all.T
    step_rows = step[...].T
    lane = lax.broadcasted_iota(jnp.int32, (BLOCK, 128), 1)
    for pair in range(5):
        cols = slice(128 * pair, 128 * pair + 128)
        value = values[:, cols]
        parts = []
        for h in (2 * pair, 2 * pair + 1):
            differ = jnp.broadcast_to(cum_all[:, h : h + 1], (BLOCK, BLOCK)) - cum_rows[h : h + 1, :]
            weight = jnp.exp(jnp.minimum(differ, 0.0)) * (scores * step_rows[h : h + 1, :])
            parts.append(jnp.dot(weight.astype(BF), value, preferred_element_type=F32))
        out[:, cols] = jnp.where(lane < 64, parts[0], parts[1])


def load_rows(pieces, held):
    x = lax.axis_index("x")
    for d, piece in zip(MASKS, pieces):
        held[other_index(x, d)] = piece[...].astype(F32)


def split(piece):
    return [piece[32 * k : 32 * k + 32] for k in range(5)], piece[160:161] + piece[161:162]


def unpack(ref):
    return split(ref[...].astype(F32))


def pack(out, item):
    for k, part in enumerate(item[0]):
        out[32 * k : 32 * k + 32, :] = part.astype(BF)
    out[160:168, :] = decay_rows(item[1])


def follow(earlier, later):
    return [e * spread(later[1], k) + l for k, (e, l) in enumerate(zip(earlier[0], later[0]))], earlier[1] * later[1]


def choose(test, yes, no):
    return [jnp.where(test, y, n) for y, n in zip(yes[0], no[0])], jnp.where(test, yes[1], no[1])


def row_total_kernel(q0, q1, q2, q3, before, before_too, out, held):
    load_rows((q0, q1, q2, q3), held)
    total = split(held[0])
    for k in range(1, 4):
        total = follow(total, split(held[k]))
    pack(out, total)


def two_rows(row, other):
    odd = lax.rem(lax.axis_index("z"), 2) == 1
    mine, theirs = unpack(row), unpack(other)
    return odd, theirs, follow(choose(odd, theirs, mine), choose(odd, mine, theirs))


def pair_total_kernel(row, other, out):
    pack(out, two_rows(row, other)[2])


def quad_total_kernel(row, other, previous, out):
    first = lax.rem(lax.axis_index("z"), 4) < 2
    mine, theirs = two_rows(row, other)[2], unpack(previous)
    pack(out, follow(choose(first, mine, theirs), choose(first, theirs, mine)))


def incoming_kernel(q0, q1, q2, q3, row, other, previous, quad, e0, e1, e2, e3, held, ready):
    z, x = lax.axis_index("z"), lax.axis_index("x")
    load_rows((q0, q1, q2, q3), held)
    odd, theirs, _ = two_rows(row, other)
    carry = choose(odd, theirs, ([jnp.zeros((32, 128), F32)] * 5, jnp.ones((1, 128), F32)))
    second = lax.rem(z, 4) >= 2
    carry = choose(second, follow(unpack(previous), carry), carry)
    carry = choose(z >= 4, follow(unpack(quad), carry), carry)
    for k in range(4):
        for j, part in enumerate(carry[0]):
            ready[k, :, 128 * j : 128 * j + 128] = part
        if k < 3:
            carry = follow(carry, split(held[k]))
    for d, out in zip(MASKS, (e0, e1, e2, e3)):
        out[...] = ready[other_index(x, d)].astype(BF)


def gated_kernel(e0, e1, e2, e3, c, cum, inside, gate, gain, w, g_out, sq_out, send_out, state, pick):
    x, core = lax.axis_index("x"), lax.axis_index("c")
    for d, piece in zip(MASKS, (e0, e1, e2, e3)):
        state[row_at(other_index(x, d), 32), :] = piece[...]
    grown = jnp.exp(cum[...])
    squares = jnp.zeros((BLOCK, 128), F32)
    for pair in range(5):
        cols = slice(128 * pair, 128 * pair + 128)
        came = jnp.dot(c[...], state[:, cols], preferred_element_type=F32)
        gated = (inside[:, cols] + spread(grown, pair) * came) * gate[:, cols]
        squares = squares + gated * gated
        g_out[:, cols] = (gated * gain[:, cols]).astype(BF)
    sq_out[...] = jnp.broadcast_to(jnp.sum(squares, axis=1, keepdims=True), (BLOCK, 128))
    for k in range(4):
        rows = row_at(2 * k + 1 - core, ROWS)
        pick[32 * k : 32 * k + 32, :] = g_out[rows, :]
        send_out[32 * k : 32 * k + 32, MODEL:] = square_cols(sq_out[rows, :])
    left = pick[...]
    for n in range(10):
        cols = slice(256 * n, 256 * n + 256)
        send_out[:, cols] = jnp.dot(left, w[:, cols], preferred_element_type=F32).astype(BF)


def square_cols(total):
    high, low = halves(total)
    lane = lax.broadcasted_iota(jnp.int32, total.shape, 1)
    return jnp.where(lane == 0, high.astype(F32), jnp.where(lane == 1, low.astype(F32), 0.0)).astype(BF)


def own_kernel(g, sq, w, out, pick):
    core = lax.axis_index("c")
    lane = lax.broadcasted_iota(jnp.int32, (ROWS, 128), 1)
    for k in range(4):
        rows = row_at(2 * k + core, ROWS)
        pick[32 * k : 32 * k + 32, :] = g[rows, :]
        out[32 * k : 32 * k + 32, MODEL:] = jnp.where(lane == 0, sq[rows, :], 0.0)
    left = pick[...]
    for n in range(10):
        cols = slice(256 * n, 256 * n + 256)
        out[:, cols] = jnp.dot(left, w[:, cols], preferred_element_type=F32)


def pair_kernel(own, came, f0, f1, f2, f3):
    y = lax.axis_index("y")
    for d, out in zip(MASKS, (f0, f1, f2, f3)):
        rows = row_at(other_index(y, d), ROWS)
        total = own[rows, :] + came[rows, :].astype(F32)
        out[:, :MODEL] = total[:, :MODEL].astype(out.dtype)
        both = jnp.sum(total[:, MODEL:], axis=1, keepdims=True)
        out[:, MODEL:] = square_cols(jnp.broadcast_to(both, (ROWS, 128))).astype(out.dtype)


def finish_kernel(f0, g1, g2, g3, out):
    total = f0[...] + g1[...].astype(F32) + g2[...].astype(F32) + g3[...].astype(F32)
    squares = jnp.sum(total[:, MODEL:], axis=1, keepdims=True)
    out[...] = (total[:, :MODEL] * lax.rsqrt(squares / DI + 1.0)).astype(BF)


def body(tokens, w_xz, w_bc, w_dt, dt_bias, a_log, conv_x, conv_bc, norm_gain, w_out):
    near = exchanged([tokens] * 4, "y", TOKEN_MASKS)
    w_both = w_xz.reshape(MODEL, 2 * WIDTH)
    near[1:] = [lax.optimization_barrier((piece, w_both))[0] for piece in near[1:]]
    far = [swapped(piece, "c", 1) for piece in near]
    gain = norm_gain[None]
    everything, pre, tail, dt_pre = call(
        project_kernel,
        [((BLOCK, MODEL), BF), ((BLOCK, PRE), BF), ((8, PRE), BF), ((BLOCK, 128), F32)],
        [*near, *far, w_both, w_bc, w_dt.T, gain],
        scratch=[((128, MODEL), BF)],
        flops=2 * BLOCK * MODEL * 1024,
        name="project",
    )
    tail = lax.ppermute(tail, SEQ, [(i, (i + 1) % 32) for i in range(32)])
    v, b, c, step, cum, weight, factor, main = call(
        prepare_kernel,
        [((BLOCK, WIDTH), BF), ((BLOCK, STATE), BF), ((BLOCK, STATE), BF), ((BLOCK, 128), F32), ((BLOCK, 128), F32)]
        + [((8, 128), F32), ((8, 128), F32), ((STATE, WIDTH), F32)],
        [pre, dt_pre, conv_x, conv_bc, dt_bias[None], a_log[None]],
        scratch=[((BLOCK + 8, PRE), F32), ((8, 128), F32)],
        flops=2 * BLOCK * STATE * WIDTH,
        name="prepare",
    )
    v_first, b_first, c_first, p0, p1, p2, p3 = call(
        local_kernel,
        [((8, WIDTH), BF), ((8, STATE), BF), ((8, STATE), BF)] + [((PIECE, 128), BF)] * 4,
        [tail, pre, conv_x, conv_bc, weight, factor, main],
        scratch=[((16, PRE), F32), ((STATE, WIDTH), F32)],
        name="local",
    )
    rows = exchanged([p0, p1, p2, p3], "x", MASKS)
    inside, c_all = call(
        inside_kernel,
        [((BLOCK, WIDTH), F32), ((BLOCK, STATE), BF)],
        [v, b, c, v_first, b_first, c_first, step, cum],
        scratch=[((BLOCK, WIDTH), BF), ((BLOCK, STATE), BF)],
        flops=20 * BLOCK * BLOCK * 256,
        name="inside",
    )
    (gate,) = call(
        gate_kernel, [((BLOCK, WIDTH), F32)], [everything, w_both, v_first], flops=2 * BLOCK * MODEL * WIDTH, name="gate"
    )
    piece = [((PIECE, 128), BF)]
    (row,) = call(row_total_kernel, piece, [*rows, inside, gate], scratch=[((4, PIECE, 128), F32)], name="rowtotal")
    other = swapped(row, "z", 1)
    (two,) = call(pair_total_kernel, piece, [row, other], name="pairtotal")
    previous = swapped(two, "z", 2)
    (four,) = call(quad_total_kernel, piece, [row, other, previous], name="quadtotal")
    quad = swapped(four, "z", 7)
    e0, e1, e2, e3 = call(
        incoming_kernel,
        [((32, WIDTH), BF)] * 4,
        [*rows, row, other, previous, quad],
        scratch=[((4, PIECE, 128), F32), ((4, 32, WIDTH), F32)],
        name="incoming",
    )
    states = exchanged([e0, e1, e2, e3], "x", MASKS)
    g, squares, send = call(
        gated_kernel,
        [((BLOCK, WIDTH), BF), ((BLOCK, 128), F32), ((128, WIDE), BF)],
        [*states, c_all, cum, inside, gate, gain, w_out],
        scratch=[((STATE, WIDTH), BF), ((128, WIDTH), BF)],
        flops=2 * 128 * WIDTH * MODEL,
        name="gated",
    )
    came = swapped(send, "c", 1)
    (own,) = call(
        own_kernel, [((128, WIDE), F32)], [g, squares, w_out], scratch=[((128, WIDTH), BF)], flops=2 * 128 * WIDTH * MODEL, name="own"
    )
    f0, f1, f2, f3 = call(pair_kernel, [((ROWS, WIDE), F32)] + [((ROWS, WIDE), BF)] * 3, [own, came], name="pair")
    parts = exchanged([f0, f1, f2, f3], "y", MASKS)
    (out,) = call(finish_kernel, [((ROWS, MODEL), BF)], parts, name="finish")
    return out


def solution(mesh):
    split = Mesh(mesh.devices.reshape(8, 4, 4, 2), ALL)
    in_specs = (
        P(ALL, None),
        P(None, None, HEAD),
        P(),
        P(None, HEAD),
        P(HEAD),
        P(HEAD),
        P(None, HEAD),
        P(),
        P(HEAD),
        P(HEAD, None),
    )
    return jax.shard_map(body, mesh=split, in_specs=in_specs, out_specs=P(ALL, None), check_vma=False)
```

```python
import jax
import jax.numpy as jnp
from jax import lax
from jax.experimental import pallas as pl
from jax.experimental.pallas import tpu as pltpu
from jax.sharding import Mesh
from jax.sharding import PartitionSpec as P

DI = 5120
SEQ = ("z", "x")
ALL = ("z", "x", "y", "c")
HEAD = ("y", "c")
BF = jnp.bfloat16
F32 = jnp.float32
ROWS = 32
BLOCK = 256
WIDTH = 640
STATE = 128
PRE = WIDTH + 2 * STATE
MODEL = 2560
WIDE = MODEL + 128
PIECE = 168
MASKS = (0, 2, 1, 3)
FIRST = (2,)
REST = (1, 3, 0)
TOKEN_MASKS = (0, 1, 3, 2)


def whole(count):
    return [pl.BlockSpec(memory_space=pltpu.VMEM)] * count


def call(body, outs, args, scratch=(), flops=0):
    return pl.pallas_call(
        body,
        out_shape=[jax.ShapeDtypeStruct(s, t) for s, t in outs],
        in_specs=whole(len(args)),
        out_specs=whole(len(outs)),
        scratch_shapes=[pltpu.VMEM(s, t) for s, t in scratch],
        compiler_params=pltpu.CompilerParams(vmem_limit_bytes=24 << 20),
        cost_estimate=pl.CostEstimate(flops=flops, transcendentals=0, bytes_accessed=flops // 500),
    )(*args)


def swapped(value, axis, mask):
    return lax.ppermute(value, axis, [(i, i ^ mask) for i in range(lax.axis_size(axis))])


def exchanged(pieces, axis, masks):
    return [swapped(piece, axis, mask) if mask else piece for mask, piece in zip(masks, pieces)]


def other_index(index, mask):
    return lax.bitwise_xor(index, jnp.int32(mask))


def row_at(index, rows):
    return pl.ds(pl.multiple_of(index * rows, rows), rows)


def project_kernel(t0, t1, t2, t3, o0, o1, o2, o3, w, w_bc, early, all_out, pre_out, tail_out):
    y, c = lax.axis_index("y"), lax.axis_index("c")
    for d, own, other in zip(TOKEN_MASKS, (t0, t1, t2, t3), (o0, o1, o2, o3)):
        source = other_index(y, d)
        all_out[row_at(source * 2 + c, ROWS), :] = own[...]
        all_out[row_at(source * 2 + 1 - c, ROWS), :] = other[...]
    tokens = all_out[...]
    for lo, hi in ((0, 256), (256, 512), (512, WIDTH)):
        part = jnp.dot(tokens, w[:, lo:hi], preferred_element_type=F32).astype(BF)
        pre_out[:, lo:hi] = part
        tail_out[:, lo:hi] = part[BLOCK - 8 :]
    part = jnp.dot(tokens, w_bc[...], preferred_element_type=F32).astype(BF)
    pre_out[:, WIDTH:] = part
    tail_out[:, WIDTH:] = part[BLOCK - 8 :]


def gate_kernel(tokens, w, before, out):
    for lo, hi in ((0, 256), (256, 512), (512, WIDTH)):
        gate = jnp.dot(tokens[...], w[:, WIDTH + lo : WIDTH + hi], preferred_element_type=F32)
        out[:, lo:hi] = jax.nn.silu(gate.astype(BF).astype(F32))


def spread(value, pair):
    rows = value.shape[0]
    lane = lax.broadcasted_iota(jnp.int32, (rows, 128), 1)
    left = jnp.broadcast_to(value[:, 2 * pair : 2 * pair + 1], (rows, 128))
    right = jnp.broadcast_to(value[:, 2 * pair + 1 : 2 * pair + 2], (rows, 128))
    return jnp.where(lane < 64, left, right)


def halves(value):
    high = value.astype(BF)
    return high, (value - high.astype(F32)).astype(BF)


def mixed(ext, first, kernel, lo, rows):
    total = jnp.zeros((rows, 128), F32)
    for k in range(4):
        total = total + kernel[k : k + 1, lo : lo + 128].astype(F32) * ext[5 + k : 5 + k + rows, first : first + 128]
    return jax.nn.silu(total).astype(BF)


def prepare_kernel(
    pre,
    tokens,
    w_dt,
    conv_x,
    conv_bc,
    bias,
    a_log,
    v_out,
    b_out,
    c_out,
    dt_out,
    cum_out,
    weight_out,
    factor_out,
    state_out,
    ext,
    small,
    w_steps,
):
    w_steps[...] = jnp.zeros(w_steps.shape, BF)
    w_steps[0 : w_dt.shape[0], :] = w_dt[...]
    dt_pre = lax.dot_general(tokens[...], w_steps[...], (((1,), (1,)), ((), ())), preferred_element_type=F32)
    ext[0:8, :] = jnp.zeros((8, PRE), F32)
    ext[8 : 8 + BLOCK, :] = pre[...].astype(F32)
    small[...] = jnp.zeros(small.shape, F32)
    small[0:1, 0 : bias.shape[1]] = bias[...]
    small[1:2, 0 : bias.shape[1]] = a_log[...]
    step = jax.nn.softplus(dt_pre + small[0:1, :])
    decay = step * (-jnp.exp(small[1:2, :]))
    row = lax.broadcasted_iota(jnp.int32, decay.shape, 0)
    cum = decay
    for k in (1, 2, 4, 8, 16, 32, 64, 128):
        cum = cum + jnp.where(row >= k, pltpu.roll(cum, k, 0), 0.0)
    dt_out[...] = step
    cum_out[...] = cum
    last = cum[BLOCK - 1 : BLOCK, :]
    weight = jnp.exp(last - cum) * step
    weight_out[...] = weight[0:8, :]
    factor_out[...] = jnp.broadcast_to(jnp.exp(last), (8, 128))
    weight = jnp.where(row >= 3, weight, 0.0)
    b = mixed(ext, WIDTH, conv_bc, 0, BLOCK)
    b_out[...] = b
    c_out[...] = mixed(ext, WIDTH + STATE, conv_bc, STATE, BLOCK)
    b_rows = b.astype(F32).T.astype(BF)
    for pair in range(5):
        cols = slice(128 * pair, 128 * pair + 128)
        v = mixed(ext, 128 * pair, conv_x, 128 * pair, BLOCK)
        v_out[:, cols] = v
        scaled = (spread(weight, pair) * v.astype(F32)).astype(BF)
        state_out[:, cols] = jnp.dot(b_rows, scaled, preferred_element_type=F32)


def decay_rows(factor):
    high, low = halves(factor)
    row = lax.broadcasted_iota(jnp.int32, (8, 128), 0)
    return jnp.where(row == 0, high.astype(F32), jnp.where(row == 1, low.astype(F32), 0.0)).astype(BF)


def local_kernel(tail, pre, conv_x, conv_bc, weight, factor, main, v_out, b_out, c_out, p0, p1, p2, p3, ext, state):
    x = lax.axis_index("x")
    first = jnp.logical_and(lax.axis_index("z") == 0, x == 0)
    ext[0:8, :] = jnp.where(first, 0.0, tail[...].astype(F32))
    ext[8:16, :] = pre[0:8, :].astype(F32)
    b = mixed(ext, WIDTH, conv_bc, 0, 8)
    b_out[...] = b
    c_out[...] = mixed(ext, WIDTH + STATE, conv_bc, STATE, 8)
    b_rows = jnp.broadcast_to(b.astype(F32)[None], (16, 8, 128)).reshape(128, 128).T
    extra = decay_rows(factor[0:1, :])
    for pair in range(5):
        cols = slice(128 * pair, 128 * pair + 128)
        v = mixed(ext, 128 * pair, conv_x, 128 * pair, 8)
        v_out[:, cols] = v
        scaled = (spread(weight[...], pair) * v.astype(F32)).astype(BF).astype(F32)
        total = main[:, cols]
        for k in range(3):
            total = total + b_rows[:, k : k + 1] * scaled[k : k + 1, :]
        state[:, cols] = total
    for d, out in zip(MASKS, (p0, p1, p2, p3)):
        rows = row_at(other_index(x, d), 32)
        for pair in range(5):
            out[32 * pair : 32 * pair + 32, :] = state[rows, 128 * pair : 128 * pair + 128].astype(BF)
        out[160:168, :] = extra


def inside_kernel(v, b, c, v_first, b_first, c_first, step, cum, out, c_out, values, b_all):
    values[...] = v[...]
    values[0:8, :] = v_first[...]
    b_all[...] = b[...]
    b_all[0:8, :] = b_first[...]
    c_out[...] = c[...]
    c_out[0:8, :] = c_first[...]
    scores = jnp.dot(c_out[...], b_all[...].astype(F32).T.astype(BF), preferred_element_type=F32)
    t = lax.broadcasted_iota(jnp.int32, (BLOCK, BLOCK), 0)
    s = lax.broadcasted_iota(jnp.int32, (BLOCK, BLOCK), 1)
    scores = jnp.where(t >= s, scores, 0.0)
    cum_all = cum[...]
    cum_rows = cum_all.T
    step_rows = step[...].T
    lane = lax.broadcasted_iota(jnp.int32, (BLOCK, 128), 1)
    for pair in range(5):
        cols = slice(128 * pair, 128 * pair + 128)
        value = values[:, cols]
        parts = []
        for h in (2 * pair, 2 * pair + 1):
            differ = jnp.broadcast_to(cum_all[:, h : h + 1], (BLOCK, BLOCK)) - cum_rows[h : h + 1, :]
            weight = jnp.exp(jnp.minimum(differ, 0.0)) * (scores * step_rows[h : h + 1, :])
            parts.append(jnp.dot(weight.astype(BF), value, preferred_element_type=F32))
        out[:, cols] = jnp.where(lane < 64, parts[0], parts[1])


def load_rows(pieces, held):
    x = lax.axis_index("x")
    for d, piece in zip(MASKS, pieces):
        held[other_index(x, d)] = piece[...].astype(F32)


def split(piece):
    return [piece[32 * k : 32 * k + 32] for k in range(5)], piece[160:161] + piece[161:162]


def unpack(ref):
    return split(ref[...].astype(F32))


def pack(out, item):
    for k, part in enumerate(item[0]):
        out[32 * k : 32 * k + 32, :] = part.astype(BF)
    out[160:168, :] = decay_rows(item[1])


def follow(earlier, later):
    return [e * spread(later[1], k) + l for k, (e, l) in enumerate(zip(earlier[0], later[0]))], earlier[1] * later[1]


def choose(test, yes, no):
    return [jnp.where(test, y, n) for y, n in zip(yes[0], no[0])], jnp.where(test, yes[1], no[1])


def row_total_kernel(q0, q1, q2, q3, before, before_too, out, held):
    load_rows((q0, q1, q2, q3), held)
    total = split(held[0])
    for k in range(1, 4):
        total = follow(total, split(held[k]))
    pack(out, total)


def two_rows(row, other):
    odd = lax.rem(lax.axis_index("z"), 2) == 1
    mine, theirs = unpack(row), unpack(other)
    return odd, theirs, follow(choose(odd, theirs, mine), choose(odd, mine, theirs))


def pair_total_kernel(row, other, out):
    pack(out, two_rows(row, other)[2])


def quad_total_kernel(row, other, previous, out):
    first = lax.rem(lax.axis_index("z"), 4) < 2
    mine, theirs = two_rows(row, other)[2], unpack(previous)
    pack(out, follow(choose(first, mine, theirs), choose(first, theirs, mine)))


def incoming_kernel(q0, q1, q2, q3, row, other, previous, quad, e0, e1, e2, e3, held, ready):
    z, x = lax.axis_index("z"), lax.axis_index("x")
    load_rows((q0, q1, q2, q3), held)
    odd, theirs, _ = two_rows(row, other)
    carry = choose(odd, theirs, ([jnp.zeros((32, 128), F32)] * 5, jnp.ones((1, 128), F32)))
    second = lax.rem(z, 4) >= 2
    carry = choose(second, follow(unpack(previous), carry), carry)
    carry = choose(z >= 4, follow(unpack(quad), carry), carry)
    for k in range(4):
        for j, part in enumerate(carry[0]):
            ready[k, :, 128 * j : 128 * j + 128] = part
        if k < 3:
            carry = follow(carry, split(held[k]))
    for d, out in zip(MASKS, (e0, e1, e2, e3)):
        out[...] = ready[other_index(x, d)].astype(BF)


def square_cols(total):
    high, low = halves(total)
    lane = lax.broadcasted_iota(jnp.int32, total.shape, 1)
    return jnp.where(lane == 0, high.astype(F32), jnp.where(lane == 1, low.astype(F32), 0.0)).astype(BF)


def project_rows(masks, side, state, c, cum, inside, gate, gain, w, out):
    y = lax.axis_index("y")
    rows = [row_at(2 * other_index(y, mask) + side, ROWS) for mask in masks]

    def picked(ref, cols):
        return jnp.concatenate([ref[r, cols] for r in rows], axis=0)

    states = picked(c, slice(0, STATE))
    grown = jnp.exp(picked(cum, slice(0, 128)))
    squares = jnp.zeros(grown.shape, F32)
    left = []
    for pair in range(5):
        cols = slice(128 * pair, 128 * pair + 128)
        came = jnp.dot(states, state[:, cols], preferred_element_type=F32)
        gated = (picked(inside, cols) + spread(grown, pair) * came) * picked(gate, cols)
        squares = squares + gated * gated
        left.append((gated * gain[:, cols]).astype(BF))
    left = jnp.concatenate(left, axis=1)
    for n in range(10):
        part = jnp.dot(left, w[:, 256 * n : 256 * n + 256], preferred_element_type=F32)
        out[:, 256 * n : 256 * n + 256] = part.astype(out.dtype)
    out[:, MODEL:] = square_cols(jnp.broadcast_to(jnp.sum(squares, axis=1, keepdims=True), squares.shape)).astype(out.dtype)


def send_kernel(e0, e1, e2, e3, c, cum, inside, gate, gain, w, state, out):
    x = lax.axis_index("x")
    for d, piece in zip(MASKS, (e0, e1, e2, e3)):
        state[row_at(other_index(x, d), 32), :] = piece[...]
    project_rows(FIRST + REST, 1 - lax.axis_index("c"), state, c, cum, inside, gate, gain, w, out)


def keep_first_kernel(state, c, cum, inside, gate, gain, w, out):
    project_rows(FIRST, lax.axis_index("c"), state, c, cum, inside, gate, gain, w, out)


def keep_rest_kernel(state, c, cum, inside, gate, gain, w, before, out):
    project_rows(REST, lax.axis_index("c"), state, c, cum, inside, gate, gain, w, out)


def pair_kernel(own, came, *outs):
    skip = came.shape[0] - own.shape[0] if len(outs) > 1 else 0
    for k, out in enumerate(outs):
        mine, theirs = slice(ROWS * k, ROWS * k + ROWS), slice(skip + ROWS * k, skip + ROWS * k + ROWS)
        total = own[mine, :] + came[theirs, :].astype(F32)
        out[:, :MODEL] = total[:, :MODEL].astype(out.dtype)
        both = jnp.sum(total[:, MODEL:], axis=1, keepdims=True)
        out[:, MODEL:] = square_cols(jnp.broadcast_to(both, (ROWS, 128))).astype(out.dtype)


def finish_kernel(f0, g1, g2, g3, out):
    total = f0[...] + g1[...].astype(F32) + g2[...].astype(F32) + g3[...].astype(F32)
    squares = jnp.sum(total[:, MODEL:], axis=1, keepdims=True)
    out[...] = (total[:, :MODEL] * lax.rsqrt(squares / DI + 1.0)).astype(BF)


def body(tokens, w_xz, w_bc, w_dt, dt_bias, a_log, conv_x, conv_bc, norm_gain, w_out):
    near = exchanged([tokens] * 4, "y", TOKEN_MASKS)
    w_both = w_xz.reshape(MODEL, 2 * WIDTH)
    near[1:] = [lax.optimization_barrier((piece, w_both))[0] for piece in near[1:]]
    far = [swapped(piece, "c", 1) for piece in near]
    gain = norm_gain[None]
    everything, pre, tail = call(
        project_kernel,
        [((BLOCK, MODEL), BF), ((BLOCK, PRE), BF), ((8, PRE), BF)],
        [*near, *far, w_both, w_bc, gain],
        flops=2 * BLOCK * MODEL * 1024,
    )
    tail = lax.ppermute(tail, SEQ, [(i, (i + 1) % 32) for i in range(32)])
    v, b, c, step, cum, weight, factor, main = call(
        prepare_kernel,
        [((BLOCK, WIDTH), BF), ((BLOCK, STATE), BF), ((BLOCK, STATE), BF), ((BLOCK, 128), F32), ((BLOCK, 128), F32)]
        + [((8, 128), F32), ((8, 128), F32), ((STATE, WIDTH), F32)],
        [pre, everything, w_dt.T, conv_x, conv_bc, dt_bias[None], a_log[None]],
        scratch=[((BLOCK + 8, PRE), F32), ((8, 128), F32), ((128, MODEL), BF)],
        flops=2 * BLOCK * STATE * WIDTH,
    )
    v_first, b_first, c_first, p0, p1, p2, p3 = call(
        local_kernel,
        [((8, WIDTH), BF), ((8, STATE), BF), ((8, STATE), BF)] + [((PIECE, 128), BF)] * 4,
        [tail, pre, conv_x, conv_bc, weight, factor, main],
        scratch=[((16, PRE), F32), ((STATE, WIDTH), F32)],
    )
    rows = exchanged([p0, p1, p2, p3], "x", MASKS)
    inside, c_all = call(
        inside_kernel,
        [((BLOCK, WIDTH), F32), ((BLOCK, STATE), BF)],
        [v, b, c, v_first, b_first, c_first, step, cum],
        scratch=[((BLOCK, WIDTH), BF), ((BLOCK, STATE), BF)],
        flops=20 * BLOCK * BLOCK * 256,
    )
    (gate,) = call(gate_kernel, [((BLOCK, WIDTH), F32)], [everything, w_both, v_first], flops=2 * BLOCK * MODEL * WIDTH)
    piece = [((PIECE, 128), BF)]
    (row,) = call(row_total_kernel, piece, [*rows, inside, gate], scratch=[((4, PIECE, 128), F32)])
    other = swapped(row, "z", 1)
    (two,) = call(pair_total_kernel, piece, [row, other])
    previous = swapped(two, "z", 2)
    (four,) = call(quad_total_kernel, piece, [row, other, previous])
    quad = swapped(four, "z", 7)
    e0, e1, e2, e3 = call(
        incoming_kernel,
        [((32, WIDTH), BF)] * 4,
        [*rows, row, other, previous, quad],
        scratch=[((4, PIECE, 128), F32), ((4, 32, WIDTH), F32)],
    )
    states = exchanged([e0, e1, e2, e3], "x", MASKS)
    shared = [c_all, cum, inside, gate, gain, w_out]
    flops = 2 * 96 * WIDTH * MODEL
    state, send = call(send_kernel, [((STATE, WIDTH), BF), ((128, WIDE), BF)], [*states, *shared], flops=flops)
    came = swapped(send, "c", 1)
    (own,) = call(keep_first_kernel, [((ROWS, WIDE), F32)], [state, *shared], flops=flops)
    (first,) = call(pair_kernel, [((ROWS, WIDE), BF)], [own, came])
    arrived = swapped(first, "y", FIRST[0])
    (own,) = call(keep_rest_kernel, [((96, WIDE), F32)], [state, *shared, first], flops=flops)
    one, three, here = call(pair_kernel, [((ROWS, WIDE), BF), ((ROWS, WIDE), BF), ((ROWS, WIDE), F32)], [own, came])
    (out,) = call(
        finish_kernel, [((ROWS, MODEL), BF)], [here, arrived, swapped(one, "y", REST[0]), swapped(three, "y", REST[1])]
    )
    return out


def solution(mesh):
    split = Mesh(mesh.devices.reshape(8, 4, 4, 2), ALL)
    in_specs = (
        P(ALL, None),
        P(None, None, HEAD),
        P(),
        P(None, HEAD),
        P(HEAD),
        P(HEAD),
        P(None, HEAD),
        P(),
        P(HEAD),
        P(HEAD, None),
    )

    return jax.shard_map(body, mesh=split, in_specs=in_specs, out_specs=P(ALL, None), check_vma=False)
```

```python
import jax
import jax.numpy as jnp
from jax import lax
from jax.experimental import pallas as pl
from jax.experimental.pallas import tpu as pltpu
from jax.sharding import Mesh
from jax.sharding import PartitionSpec as P

DI = 5120
SEQ = ("z", "x")
ALL = ("z", "x", "y", "c")
HEAD = ("y", "c")
BF = jnp.bfloat16
F32 = jnp.float32
ROWS = 32
BLOCK = 256
WIDTH = 640
STATE = 128
PRE = WIDTH + 2 * STATE
MODEL = 2560
WIDE = MODEL + 128
PIECE = 168
MASKS = (0, 2, 1, 3)
FIRST = (2,)
REST = (1, 3, 0)
TOKEN_MASKS = (0, 1, 3, 2)


def whole(count):
    return [pl.BlockSpec(memory_space=pltpu.VMEM)] * count


def call(body, outs, args, scratch=(), flops=0):
    return pl.pallas_call(
        body,
        out_shape=[jax.ShapeDtypeStruct(s, t) for s, t in outs],
        in_specs=whole(len(args)),
        out_specs=whole(len(outs)),
        scratch_shapes=[pltpu.VMEM(s, t) for s, t in scratch],
        compiler_params=pltpu.CompilerParams(vmem_limit_bytes=24 << 20),
        cost_estimate=pl.CostEstimate(flops=flops, transcendentals=0, bytes_accessed=flops // 500),
    )(*args)


def swapped(value, axis, mask):
    return lax.ppermute(value, axis, [(i, i ^ mask) for i in range(lax.axis_size(axis))])


def exchanged(pieces, axis, masks):
    return [swapped(piece, axis, mask) if mask else piece for mask, piece in zip(masks, pieces)]


def other_index(index, mask):
    return lax.bitwise_xor(index, jnp.int32(mask))


def row_at(index, rows):
    return pl.ds(pl.multiple_of(index * rows, rows), rows)


def gain_kernel(gain, out):
    out[...] = gain[...]


def project_into(tokens, w, w_bc, out):
    for lo, hi in ((0, 256), (256, 512), (512, WIDTH)):
        out[:, lo:hi] = jnp.dot(tokens[...], w[:, lo:hi], preferred_element_type=F32).astype(BF)
    out[:, WIDTH:] = jnp.dot(tokens[...], w_bc[...], preferred_element_type=F32).astype(BF)


def project_early_kernel(t0, t1, t2, t3, o0, o3, w, w_bc, out, tokens):
    for k, piece in enumerate((t0, t1, t2, t3, o0, o3)):
        tokens[32 * k : 32 * k + 32, :] = piece[...]
    project_into(tokens, w, w_bc, out)


def project_kernel(t0, t1, t2, t3, o0, o1, o2, o3, part, w, w_bc, early, all_out, pre_out, tail_out, late, rest):
    y, c = lax.axis_index("y"), lax.axis_index("c")
    near = [row_at(other_index(y, mask) * 2 + c, ROWS) for mask in TOKEN_MASKS]
    far = [row_at(other_index(y, mask) * 2 + 1 - c, ROWS) for mask in TOKEN_MASKS]
    late[0:32, :] = o1[...]
    late[32:64, :] = o2[...]
    project_into(late, w, w_bc, rest)
    for rows, piece in zip(near + far, (t0, t1, t2, t3, o0, o1, o2, o3)):
        all_out[rows, :] = piece[...]
    for k, rows in enumerate(near + [far[0], far[3]]):
        pre_out[rows, :] = part[32 * k : 32 * k + 32, :]
    for k, rows in enumerate(far[1:3]):
        pre_out[rows, :] = rest[32 * k : 32 * k + 32, :]
    tail_out[...] = pre_out[BLOCK - 8 :, :]


def gate_kernel(tokens, w, before, out):
    for lo, hi in ((0, 256), (256, 512), (512, WIDTH)):
        gate = jnp.dot(tokens[...], w[:, WIDTH + lo : WIDTH + hi], preferred_element_type=F32)
        out[:, lo:hi] = jax.nn.silu(gate.astype(BF).astype(F32))


def spread(value, pair):
    rows = value.shape[0]
    lane = lax.broadcasted_iota(jnp.int32, (rows, 128), 1)
    left = jnp.broadcast_to(value[:, 2 * pair : 2 * pair + 1], (rows, 128))
    right = jnp.broadcast_to(value[:, 2 * pair + 1 : 2 * pair + 2], (rows, 128))
    return jnp.where(lane < 64, left, right)


def halves(value):
    high = value.astype(BF)
    return high, (value - high.astype(F32)).astype(BF)


def mixed(ext, first, kernel, lo, rows):
    total = jnp.zeros((rows, 128), F32)
    for k in range(4):
        total = total + kernel[k : k + 1, lo : lo + 128].astype(F32) * ext[5 + k : 5 + k + rows, first : first + 128]
    return jax.nn.silu(total).astype(BF)


def prepare_kernel(
    pre,
    tokens,
    w_dt,
    conv_x,
    conv_bc,
    bias,
    a_log,
    v_out,
    b_out,
    c_out,
    dt_out,
    cum_out,
    weight_out,
    factor_out,
    state_out,
    ext,
    small,
    w_steps,
):
    w_steps[...] = jnp.zeros(w_steps.shape, BF)
    w_steps[0 : w_dt.shape[0], :] = w_dt[...]
    dt_pre = lax.dot_general(tokens[...], w_steps[...], (((1,), (1,)), ((), ())), preferred_element_type=F32)
    ext[0:8, :] = jnp.zeros((8, PRE), F32)
    ext[8 : 8 + BLOCK, :] = pre[...].astype(F32)
    small[...] = jnp.zeros(small.shape, F32)
    small[0:1, 0 : bias.shape[1]] = bias[...]
    small[1:2, 0 : bias.shape[1]] = a_log[...]
    step = jax.nn.softplus(dt_pre + small[0:1, :])
    decay = step * (-jnp.exp(small[1:2, :]))
    row = lax.broadcasted_iota(jnp.int32, decay.shape, 0)
    cum = decay
    for k in (1, 2, 4, 8, 16, 32, 64, 128):
        cum = cum + jnp.where(row >= k, pltpu.roll(cum, k, 0), 0.0)
    dt_out[...] = step
    cum_out[...] = cum
    last = cum[BLOCK - 1 : BLOCK, :]
    weight = jnp.exp(last - cum) * step
    weight_out[...] = weight[0:8, :]
    factor_out[...] = jnp.broadcast_to(jnp.exp(last), (8, 128))
    weight = jnp.where(row >= 3, weight, 0.0)
    b = mixed(ext, WIDTH, conv_bc, 0, BLOCK)
    b_out[...] = b
    c_out[...] = mixed(ext, WIDTH + STATE, conv_bc, STATE, BLOCK)
    b_rows = b.astype(F32).T.astype(BF)
    for pair in range(5):
        cols = slice(128 * pair, 128 * pair + 128)
        v = mixed(ext, 128 * pair, conv_x, 128 * pair, BLOCK)
        v_out[:, cols] = v
        scaled = (spread(weight, pair) * v.astype(F32)).astype(BF)
        state_out[:, cols] = jnp.dot(b_rows, scaled, preferred_element_type=F32)


def decay_rows(factor):
    high, low = halves(factor)
    row = lax.broadcasted_iota(jnp.int32, (8, 128), 0)
    return jnp.where(row == 0, high.astype(F32), jnp.where(row == 1, low.astype(F32), 0.0)).astype(BF)


def local_kernel(tail, pre, conv_x, conv_bc, weight, factor, main, v_out, b_out, c_out, p0, p1, p2, p3, ext, state):
    x = lax.axis_index("x")
    first = jnp.logical_and(lax.axis_index("z") == 0, x == 0)
    ext[0:8, :] = jnp.where(first, 0.0, tail[...].astype(F32))
    ext[8:16, :] = pre[0:8, :].astype(F32)
    b = mixed(ext, WIDTH, conv_bc, 0, 8)
    b_out[...] = b
    c_out[...] = mixed(ext, WIDTH + STATE, conv_bc, STATE, 8)
    b_rows = jnp.broadcast_to(b.astype(F32)[None], (16, 8, 128)).reshape(128, 128).T
    extra = decay_rows(factor[0:1, :])
    for pair in range(5):
        cols = slice(128 * pair, 128 * pair + 128)
        v = mixed(ext, 128 * pair, conv_x, 128 * pair, 8)
        v_out[:, cols] = v
        scaled = (spread(weight[...], pair) * v.astype(F32)).astype(BF).astype(F32)
        total = main[:, cols]
        for k in range(3):
            total = total + b_rows[:, k : k + 1] * scaled[k : k + 1, :]
        state[:, cols] = total
    for d, out in zip(MASKS, (p0, p1, p2, p3)):
        rows = row_at(other_index(x, d), 32)
        for pair in range(5):
            out[32 * pair : 32 * pair + 32, :] = state[rows, 128 * pair : 128 * pair + 128].astype(BF)
        out[160:168, :] = extra


def inside_kernel(v, b, c, v_first, b_first, c_first, step, cum, out, c_out, values, b_all):
    values[...] = v[...]
    values[0:8, :] = v_first[...]
    b_all[...] = b[...]
    b_all[0:8, :] = b_first[...]
    c_out[...] = c[...]
    c_out[0:8, :] = c_first[...]
    scores = jnp.dot(c_out[...], b_all[...].astype(F32).T.astype(BF), preferred_element_type=F32)
    t = lax.broadcasted_iota(jnp.int32, (BLOCK, BLOCK), 0)
    s = lax.broadcasted_iota(jnp.int32, (BLOCK, BLOCK), 1)
    scores = jnp.where(t >= s, scores, 0.0)
    cum_all = cum[...]
    cum_rows = cum_all.T
    step_rows = step[...].T
    lane = lax.broadcasted_iota(jnp.int32, (BLOCK, 128), 1)
    for pair in range(5):
        cols = slice(128 * pair, 128 * pair + 128)
        value = values[:, cols]
        parts = []
        for h in (2 * pair, 2 * pair + 1):
            differ = jnp.broadcast_to(cum_all[:, h : h + 1], (BLOCK, BLOCK)) - cum_rows[h : h + 1, :]
            weight = jnp.exp(jnp.minimum(differ, 0.0)) * (scores * step_rows[h : h + 1, :])
            parts.append(jnp.dot(weight.astype(BF), value, preferred_element_type=F32))
        out[:, cols] = jnp.where(lane < 64, parts[0], parts[1])


def load_rows(pieces, held):
    x = lax.axis_index("x")
    for d, piece in zip(MASKS, pieces):
        held[other_index(x, d)] = piece[...].astype(F32)


def split(piece):
    return [piece[32 * k : 32 * k + 32] for k in range(5)], piece[160:161] + piece[161:162]


def unpack(ref):
    return split(ref[...].astype(F32))


def pack(out, item):
    for k, part in enumerate(item[0]):
        out[32 * k : 32 * k + 32, :] = part.astype(BF)
    out[160:168, :] = decay_rows(item[1])


def follow(earlier, later):
    return [e * spread(later[1], k) + l for k, (e, l) in enumerate(zip(earlier[0], later[0]))], earlier[1] * later[1]


def choose(test, yes, no):
    return [jnp.where(test, y, n) for y, n in zip(yes[0], no[0])], jnp.where(test, yes[1], no[1])


def row_total_kernel(q0, q1, q2, q3, before, before_too, out, held):
    load_rows((q0, q1, q2, q3), held)
    total = split(held[0])
    for k in range(1, 4):
        total = follow(total, split(held[k]))
    pack(out, total)


def two_rows(row, other):
    odd = lax.rem(lax.axis_index("z"), 2) == 1
    mine, theirs = unpack(row), unpack(other)
    return odd, theirs, follow(choose(odd, theirs, mine), choose(odd, mine, theirs))


def pair_total_kernel(row, other, out):
    pack(out, two_rows(row, other)[2])


def quad_total_kernel(row, other, previous, out):
    first = lax.rem(lax.axis_index("z"), 4) < 2
    mine, theirs = two_rows(row, other)[2], unpack(previous)
    pack(out, follow(choose(first, mine, theirs), choose(first, theirs, mine)))


def incoming_kernel(q0, q1, q2, q3, row, other, previous, quad, e0, e1, e2, e3, held, ready):
    z, x = lax.axis_index("z"), lax.axis_index("x")
    load_rows((q0, q1, q2, q3), held)
    odd, theirs, _ = two_rows(row, other)
    carry = choose(odd, theirs, ([jnp.zeros((32, 128), F32)] * 5, jnp.ones((1, 128), F32)))
    second = lax.rem(z, 4) >= 2
    carry = choose(second, follow(unpack(previous), carry), carry)
    carry = choose(z >= 4, follow(unpack(quad), carry), carry)
    for k in range(4):
        for j, part in enumerate(carry[0]):
            ready[k, :, 128 * j : 128 * j + 128] = part
        if k < 3:
            carry = follow(carry, split(held[k]))
    for d, out in zip(MASKS, (e0, e1, e2, e3)):
        out[...] = ready[other_index(x, d)].astype(BF)


def square_cols(total):
    high, low = halves(total)
    lane = lax.broadcasted_iota(jnp.int32, total.shape, 1)
    return jnp.where(lane == 0, high.astype(F32), jnp.where(lane == 1, low.astype(F32), 0.0)).astype(BF)


def project_rows(masks, side, state, c, cum, inside, gate, gain, w, out):
    y = lax.axis_index("y")
    rows = [row_at(2 * other_index(y, mask) + side, ROWS) for mask in masks]

    def picked(ref, cols):
        return jnp.concatenate([ref[r, cols] for r in rows], axis=0)

    states = picked(c, slice(0, STATE))
    grown = jnp.exp(picked(cum, slice(0, 128)))
    squares = jnp.zeros(grown.shape, F32)
    left = []
    for pair in range(5):
        cols = slice(128 * pair, 128 * pair + 128)
        came = jnp.dot(states, state[:, cols], preferred_element_type=F32)
        gated = (picked(inside, cols) + spread(grown, pair) * came) * picked(gate, cols)
        squares = squares + gated * gated
        left.append((gated * gain[:, cols]).astype(BF))
    left = jnp.concatenate(left, axis=1)
    for n in range(10):
        part = jnp.dot(left, w[:, 256 * n : 256 * n + 256], preferred_element_type=F32)
        out[:, 256 * n : 256 * n + 256] = part.astype(out.dtype)
    out[:, MODEL:] = square_cols(jnp.broadcast_to(jnp.sum(squares, axis=1, keepdims=True), squares.shape)).astype(out.dtype)


def send_kernel(e0, e1, e2, e3, c, cum, inside, gate, gain, w, state, out):
    x = lax.axis_index("x")
    for d, piece in zip(MASKS, (e0, e1, e2, e3)):
        state[row_at(other_index(x, d), 32), :] = piece[...]
    project_rows(FIRST + REST, 1 - lax.axis_index("c"), state, c, cum, inside, gate, gain, w, out)


def keep_first_kernel(state, c, cum, inside, gate, gain, w, out):
    project_rows(FIRST, lax.axis_index("c"), state, c, cum, inside, gate, gain, w, out)


def keep_rest_kernel(state, c, cum, inside, gate, gain, w, before, out):
    project_rows(REST, lax.axis_index("c"), state, c, cum, inside, gate, gain, w, out)


def pair_kernel(own, came, *outs):
    skip = came.shape[0] - own.shape[0] if len(outs) > 1 else 0
    for k, out in enumerate(outs):
        mine, theirs = slice(ROWS * k, ROWS * k + ROWS), slice(skip + ROWS * k, skip + ROWS * k + ROWS)
        total = own[mine, :] + came[theirs, :].astype(F32)
        out[:, :MODEL] = total[:, :MODEL].astype(out.dtype)
        both = jnp.sum(total[:, MODEL:], axis=1, keepdims=True)
        out[:, MODEL:] = square_cols(jnp.broadcast_to(both, (ROWS, 128))).astype(out.dtype)


def finish_kernel(f0, g1, g2, g3, out):
    total = f0[...] + g1[...].astype(F32) + g2[...].astype(F32) + g3[...].astype(F32)
    squares = jnp.sum(total[:, MODEL:], axis=1, keepdims=True)
    out[...] = (total[:, :MODEL] * lax.rsqrt(squares / DI + 1.0)).astype(BF)


def body(tokens, w_xz, w_bc, w_dt, dt_bias, a_log, conv_x, conv_bc, norm_gain, w_out):
    w_both = w_xz.reshape(MODEL, 2 * WIDTH)
    near, far = [tokens], [swapped(tokens, "c", 1)]
    for mask in TOKEN_MASKS[1:]:
        near.append(swapped(tokens, "y", mask))
    near[3], w_both = lax.optimization_barrier((near[3], w_both))
    for mask, piece in zip(TOKEN_MASKS[1:], near[1:]):
        far.append(swapped(piece, "c", 1))
    (gain,) = call(gain_kernel, [((1, WIDTH), F32)], [norm_gain[None]])
    (part,) = call(
        project_early_kernel,
        [((192, PRE), BF)],
        [*near, far[0], far[3], w_both, w_bc],
        scratch=[((192, MODEL), BF)],
        flops=2 * 192 * MODEL * 1024,
    )
    everything, pre, tail = call(
        project_kernel,
        [((BLOCK, MODEL), BF), ((BLOCK, PRE), BF), ((8, PRE), BF)],
        [*near, *far, part, w_both, w_bc, gain],
        scratch=[((64, MODEL), BF), ((64, PRE), BF)],
        flops=2 * 64 * MODEL * 1024,
    )
    tail = lax.ppermute(tail, SEQ, [(i, (i + 1) % 32) for i in range(32)])
    v, b, c, step, cum, weight, factor, main = call(
        prepare_kernel,
        [((BLOCK, WIDTH), BF), ((BLOCK, STATE), BF), ((BLOCK, STATE), BF), ((BLOCK, 128), F32), ((BLOCK, 128), F32)]
        + [((8, 128), F32), ((8, 128), F32), ((STATE, WIDTH), F32)],
        [pre, everything, w_dt.T, conv_x, conv_bc, dt_bias[None], a_log[None]],
        scratch=[((BLOCK + 8, PRE), F32), ((8, 128), F32), ((128, MODEL), BF)],
        flops=2 * BLOCK * STATE * WIDTH,
    )
    v_first, b_first, c_first, p0, p1, p2, p3 = call(
        local_kernel,
        [((8, WIDTH), BF), ((8, STATE), BF), ((8, STATE), BF)] + [((PIECE, 128), BF)] * 4,
        [tail, pre, conv_x, conv_bc, weight, factor, main],
        scratch=[((16, PRE), F32), ((STATE, WIDTH), F32)],
    )
    rows = exchanged([p0, p1, p2, p3], "x", MASKS)
    inside, c_all = call(
        inside_kernel,
        [((BLOCK, WIDTH), F32), ((BLOCK, STATE), BF)],
        [v, b, c, v_first, b_first, c_first, step, cum],
        scratch=[((BLOCK, WIDTH), BF), ((BLOCK, STATE), BF)],
        flops=20 * BLOCK * BLOCK * 256,
    )
    (gate,) = call(gate_kernel, [((BLOCK, WIDTH), F32)], [everything, w_both, v_first], flops=2 * BLOCK * MODEL * WIDTH)
    piece = [((PIECE, 128), BF)]
    (row,) = call(row_total_kernel, piece, [*rows, inside, gate], scratch=[((4, PIECE, 128), F32)])
    other = swapped(row, "z", 1)
    (two,) = call(pair_total_kernel, piece, [row, other])
    previous = swapped(two, "z", 2)
    (four,) = call(quad_total_kernel, piece, [row, other, previous])
    quad = swapped(four, "z", 7)
    e0, e1, e2, e3 = call(
        incoming_kernel,
        [((32, WIDTH), BF)] * 4,
        [*rows, row, other, previous, quad],
        scratch=[((4, PIECE, 128), F32), ((4, 32, WIDTH), F32)],
    )
    states = exchanged([e0, e1, e2, e3], "x", MASKS)
    shared = [c_all, cum, inside, gate, gain, w_out]
    flops = 2 * 96 * WIDTH * MODEL
    state, send = call(send_kernel, [((STATE, WIDTH), BF), ((128, WIDE), BF)], [*states, *shared], flops=flops)
    came = swapped(send, "c", 1)
    (own,) = call(keep_first_kernel, [((ROWS, WIDE), F32)], [state, *shared], flops=flops)
    (first,) = call(pair_kernel, [((ROWS, WIDE), BF)], [own, came])
    arrived = swapped(first, "y", FIRST[0])
    (own,) = call(keep_rest_kernel, [((96, WIDE), F32)], [state, *shared, first], flops=flops)
    one, three, here = call(pair_kernel, [((ROWS, WIDE), BF), ((ROWS, WIDE), BF), ((ROWS, WIDE), F32)], [own, came])
    (out,) = call(
        finish_kernel, [((ROWS, MODEL), BF)], [here, arrived, swapped(one, "y", REST[0]), swapped(three, "y", REST[1])]
    )
    return out


def solution(mesh):
    split = Mesh(mesh.devices.reshape(8, 4, 4, 2), ALL)
    in_specs = (
        P(ALL, None),
        P(None, None, HEAD),
        P(),
        P(None, HEAD),
        P(HEAD),
        P(HEAD),
        P(None, HEAD),
        P(),
        P(HEAD),
        P(HEAD, None),
    )

    return jax.shard_map(body, mesh=split, in_specs=in_specs, out_specs=P(ALL, None), check_vma=False)
```

```python
import jax
import jax.numpy as jnp
from jax import lax
from jax.experimental import pallas as pl
from jax.experimental.pallas import tpu as pltpu
from jax.sharding import Mesh
from jax.sharding import PartitionSpec as P

DI = 5120
SEQ = ("z", "x")
ALL = ("z", "x", "y", "c")
HEAD = ("y", "c")
BF = jnp.bfloat16
F32 = jnp.float32
ROWS = 32
BLOCK = 256
WIDTH = 640
STATE = 128
PRE = WIDTH + 2 * STATE
MODEL = 2560
WIDE = MODEL + 128
PIECE = 168
MASKS = (0, 2, 1, 3)
FIRST = (2,)
REST = (1, 3, 0)
TOKEN_MASKS = (0, 1, 3, 2)


def whole(count):
    return [pl.BlockSpec(memory_space=pltpu.VMEM)] * count


def call(body, outs, args, scratch=(), flops=0):
    return pl.pallas_call(
        body,
        out_shape=[jax.ShapeDtypeStruct(s, t) for s, t in outs],
        in_specs=whole(len(args)),
        out_specs=whole(len(outs)),
        scratch_shapes=[pltpu.VMEM(s, t) for s, t in scratch],
        compiler_params=pltpu.CompilerParams(vmem_limit_bytes=24 << 20),
        cost_estimate=pl.CostEstimate(flops=flops, transcendentals=0, bytes_accessed=flops // 500),
    )(*args)


def swapped(value, axis, mask):
    return lax.ppermute(value, axis, [(i, i ^ mask) for i in range(lax.axis_size(axis))])


def exchanged(pieces, axis, masks):
    return [swapped(piece, axis, mask) if mask else piece for mask, piece in zip(masks, pieces)]


def other_index(index, mask):
    return lax.bitwise_xor(index, jnp.int32(mask))


def row_at(index, rows):
    return pl.ds(pl.multiple_of(index * rows, rows), rows)


def gain_kernel(gain, out):
    out[...] = gain[...]


def project_into(tokens, w, w_bc, out):
    for lo, hi in ((0, 256), (256, 512), (512, WIDTH)):
        out[:, lo:hi] = jnp.dot(tokens[...], w[:, lo:hi], preferred_element_type=F32).astype(BF)
    out[:, WIDTH:] = jnp.dot(tokens[...], w_bc[...], preferred_element_type=F32).astype(BF)


def project_early_kernel(t0, t1, t2, t3, o0, o3, w, w_bc, out, tokens):
    for k, piece in enumerate((t0, t1, t2, t3, o0, o3)):
        tokens[32 * k : 32 * k + 32, :] = piece[...]
    project_into(tokens, w, w_bc, out)


def project_kernel(o1, o2, part, w, w_bc, early, pre_out, tail_out, late, rest):
    y, c = lax.axis_index("y"), lax.axis_index("c")
    near = [row_at(other_index(y, mask) * 2 + c, ROWS) for mask in TOKEN_MASKS]
    far = [row_at(other_index(y, mask) * 2 + 1 - c, ROWS) for mask in TOKEN_MASKS]
    late[0:32, :] = o1[...]
    late[32:64, :] = o2[...]
    project_into(late, w, w_bc, rest)
    for k, rows in enumerate(near + [far[0], far[3]]):
        pre_out[rows, :] = part[32 * k : 32 * k + 32, :]
    for k, rows in enumerate(far[1:3]):
        pre_out[rows, :] = rest[32 * k : 32 * k + 32, :]
    tail_out[...] = pre_out[BLOCK - 8 :, :]


def gate_kernel(tokens, w, before, out):
    for lo, hi in ((0, 256), (256, 512), (512, WIDTH)):
        gate = jnp.dot(tokens[...], w[:, WIDTH + lo : WIDTH + hi], preferred_element_type=F32)
        out[:, lo:hi] = jax.nn.silu(gate.astype(BF).astype(F32))


def spread(value, pair):
    rows = value.shape[0]
    lane = lax.broadcasted_iota(jnp.int32, (rows, 128), 1)
    left = jnp.broadcast_to(value[:, 2 * pair : 2 * pair + 1], (rows, 128))
    right = jnp.broadcast_to(value[:, 2 * pair + 1 : 2 * pair + 2], (rows, 128))
    return jnp.where(lane < 64, left, right)


def halves(value):
    high = value.astype(BF)
    return high, (value - high.astype(F32)).astype(BF)


def mixed(ext, first, kernel, lo, rows):
    total = jnp.zeros((rows, 128), F32)
    for k in range(4):
        total = total + kernel[k : k + 1, lo : lo + 128].astype(F32) * ext[5 + k : 5 + k + rows, first : first + 128]
    return jax.nn.silu(total).astype(BF)


def prepare_kernel(
    pre,
    t0,
    t1,
    t2,
    t3,
    o0,
    o1,
    o2,
    o3,
    w_dt,
    conv_x,
    conv_bc,
    bias,
    a_log,
    tokens,
    v_out,
    b_out,
    c_out,
    dt_out,
    cum_out,
    weight_out,
    factor_out,
    state_out,
    ext,
    small,
    w_steps,
):
    y, c = lax.axis_index("y"), lax.axis_index("c")
    for mask, own, other in zip(TOKEN_MASKS, (t0, t1, t2, t3), (o0, o1, o2, o3)):
        tokens[row_at(other_index(y, mask) * 2 + c, ROWS), :] = own[...]
        tokens[row_at(other_index(y, mask) * 2 + 1 - c, ROWS), :] = other[...]
    w_steps[...] = jnp.zeros(w_steps.shape, BF)
    w_steps[0 : w_dt.shape[0], :] = w_dt[...]
    dt_pre = lax.dot_general(tokens[...], w_steps[...], (((1,), (1,)), ((), ())), preferred_element_type=F32)
    ext[0:8, :] = jnp.zeros((8, PRE), F32)
    ext[8 : 8 + BLOCK, :] = pre[...].astype(F32)
    small[...] = jnp.zeros(small.shape, F32)
    small[0:1, 0 : bias.shape[1]] = bias[...]
    small[1:2, 0 : bias.shape[1]] = a_log[...]
    step = jax.nn.softplus(dt_pre + small[0:1, :])
    decay = step * (-jnp.exp(small[1:2, :]))
    row = lax.broadcasted_iota(jnp.int32, decay.shape, 0)
    cum = decay
    for k in (1, 2, 4, 8, 16, 32, 64, 128):
        cum = cum + jnp.where(row >= k, pltpu.roll(cum, k, 0), 0.0)
    dt_out[...] = step
    cum_out[...] = cum
    last = cum[BLOCK - 1 : BLOCK, :]
    weight = jnp.exp(last - cum) * step
    weight_out[...] = weight[0:8, :]
    factor_out[...] = jnp.broadcast_to(jnp.exp(last), (8, 128))
    weight = jnp.where(row >= 3, weight, 0.0)
    b = mixed(ext, WIDTH, conv_bc, 0, BLOCK)
    b_out[...] = b
    c_out[...] = mixed(ext, WIDTH + STATE, conv_bc, STATE, BLOCK)
    b_rows = b.astype(F32).T.astype(BF)
    for pair in range(5):
        cols = slice(128 * pair, 128 * pair + 128)
        v = mixed(ext, 128 * pair, conv_x, 128 * pair, BLOCK)
        v_out[:, cols] = v
        scaled = (spread(weight, pair) * v.astype(F32)).astype(BF)
        state_out[:, cols] = jnp.dot(b_rows, scaled, preferred_element_type=F32)


def decay_rows(factor):
    high, low = halves(factor)
    row = lax.broadcasted_iota(jnp.int32, (8, 128), 0)
    return jnp.where(row == 0, high.astype(F32), jnp.where(row == 1, low.astype(F32), 0.0)).astype(BF)


def local_kernel(tail, pre, conv_x, conv_bc, weight, factor, main, v_out, b_out, c_out, p0, p1, p2, p3, ext, state):
    x = lax.axis_index("x")
    first = jnp.logical_and(lax.axis_index("z") == 0, x == 0)
    ext[0:8, :] = jnp.where(first, 0.0, tail[...].astype(F32))
    ext[8:16, :] = pre[0:8, :].astype(F32)
    b = mixed(ext, WIDTH, conv_bc, 0, 8)
    b_out[...] = b
    c_out[...] = mixed(ext, WIDTH + STATE, conv_bc, STATE, 8)
    b_rows = jnp.broadcast_to(b.astype(F32)[None], (16, 8, 128)).reshape(128, 128).T
    extra = decay_rows(factor[0:1, :])
    for pair in range(5):
        cols = slice(128 * pair, 128 * pair + 128)
        v = mixed(ext, 128 * pair, conv_x, 128 * pair, 8)
        v_out[:, cols] = v
        scaled = (spread(weight[...], pair) * v.astype(F32)).astype(BF).astype(F32)
        total = main[:, cols]
        for k in range(3):
            total = total + b_rows[:, k : k + 1] * scaled[k : k + 1, :]
        state[:, cols] = total
    for d, out in zip(MASKS, (p0, p1, p2, p3)):
        rows = row_at(other_index(x, d), 32)
        for pair in range(5):
            out[32 * pair : 32 * pair + 32, :] = state[rows, 128 * pair : 128 * pair + 128].astype(BF)
        out[160:168, :] = extra


def inside_kernel(v, b, c, v_first, b_first, c_first, step, cum, out, c_out, values, b_all):
    values[...] = v[...]
    values[0:8, :] = v_first[...]
    b_all[...] = b[...]
    b_all[0:8, :] = b_first[...]
    c_out[...] = c[...]
    c_out[0:8, :] = c_first[...]
    scores = jnp.dot(c_out[...], b_all[...].astype(F32).T.astype(BF), preferred_element_type=F32)
    t = lax.broadcasted_iota(jnp.int32, (BLOCK, BLOCK), 0)
    s = lax.broadcasted_iota(jnp.int32, (BLOCK, BLOCK), 1)
    scores = jnp.where(t >= s, scores, 0.0)
    cum_all = cum[...]
    cum_rows = cum_all.T
    step_rows = step[...].T
    lane = lax.broadcasted_iota(jnp.int32, (BLOCK, 128), 1)
    for pair in range(5):
        cols = slice(128 * pair, 128 * pair + 128)
        value = values[:, cols]
        parts = []
        for h in (2 * pair, 2 * pair + 1):
            differ = jnp.broadcast_to(cum_all[:, h : h + 1], (BLOCK, BLOCK)) - cum_rows[h : h + 1, :]
            weight = jnp.exp(jnp.minimum(differ, 0.0)) * (scores * step_rows[h : h + 1, :])
            parts.append(jnp.dot(weight.astype(BF), value, preferred_element_type=F32))
        out[:, cols] = jnp.where(lane < 64, parts[0], parts[1])


def load_rows(pieces, held):
    x = lax.axis_index("x")
    for d, piece in zip(MASKS, pieces):
        held[other_index(x, d)] = piece[...].astype(F32)


def split(piece):
    return [piece[32 * k : 32 * k + 32] for k in range(5)], piece[160:161] + piece[161:162]


def unpack(ref):
    return split(ref[...].astype(F32))


def pack(out, item):
    for k, part in enumerate(item[0]):
        out[32 * k : 32 * k + 32, :] = part.astype(BF)
    out[160:168, :] = decay_rows(item[1])


def follow(earlier, later):
    return [e * spread(later[1], k) + l for k, (e, l) in enumerate(zip(earlier[0], later[0]))], earlier[1] * later[1]


def choose(test, yes, no):
    return [jnp.where(test, y, n) for y, n in zip(yes[0], no[0])], jnp.where(test, yes[1], no[1])


def row_total_kernel(q0, q1, q2, q3, before, before_too, out, held):
    load_rows((q0, q1, q2, q3), held)
    total = split(held[0])
    for k in range(1, 4):
        total = follow(total, split(held[k]))
    pack(out, total)


def two_rows(row, other):
    odd = lax.rem(lax.axis_index("z"), 2) == 1
    mine, theirs = unpack(row), unpack(other)
    return odd, theirs, follow(choose(odd, theirs, mine), choose(odd, mine, theirs))


def pair_total_kernel(row, other, out):
    pack(out, two_rows(row, other)[2])


def quad_total_kernel(row, other, previous, out):
    first = lax.rem(lax.axis_index("z"), 4) < 2
    mine, theirs = two_rows(row, other)[2], unpack(previous)
    pack(out, follow(choose(first, mine, theirs), choose(first, theirs, mine)))


def incoming_kernel(q0, q1, q2, q3, row, other, previous, quad, e0, e1, e2, e3, held, ready):
    z, x = lax.axis_index("z"), lax.axis_index("x")
    load_rows((q0, q1, q2, q3), held)
    odd, theirs, _ = two_rows(row, other)
    carry = choose(odd, theirs, ([jnp.zeros((32, 128), F32)] * 5, jnp.ones((1, 128), F32)))
    second = lax.rem(z, 4) >= 2
    carry = choose(second, follow(unpack(previous), carry), carry)
    carry = choose(z >= 4, follow(unpack(quad), carry), carry)
    for k in range(4):
        for j, part in enumerate(carry[0]):
            ready[k, :, 128 * j : 128 * j + 128] = part
        if k < 3:
            carry = follow(carry, split(held[k]))
    for d, out in zip(MASKS, (e0, e1, e2, e3)):
        out[...] = ready[other_index(x, d)].astype(BF)


def square_cols(total):
    high, low = halves(total)
    lane = lax.broadcasted_iota(jnp.int32, total.shape, 1)
    return jnp.where(lane == 0, high.astype(F32), jnp.where(lane == 1, low.astype(F32), 0.0)).astype(BF)


def project_rows(masks, side, state, c, cum, inside, gate, gain, w, *outs):
    y = lax.axis_index("y")
    rows = [row_at(2 * other_index(y, mask) + side, ROWS) for mask in masks]

    def picked(ref, cols):
        return jnp.concatenate([ref[r, cols] for r in rows], axis=0)

    states = picked(c, slice(0, STATE))
    grown = jnp.exp(picked(cum, slice(0, 128)))
    squares = jnp.zeros(grown.shape, F32)
    left = []
    for pair in range(5):
        cols = slice(128 * pair, 128 * pair + 128)
        came = jnp.dot(states, state[:, cols], preferred_element_type=F32)
        gated = (picked(inside, cols) + spread(grown, pair) * came) * picked(gate, cols)
        squares = squares + gated * gated
        left.append((gated * gain[:, cols]).astype(BF))
    left = jnp.concatenate(left, axis=1)
    sums = square_cols(jnp.broadcast_to(jnp.sum(squares, axis=1, keepdims=True), squares.shape))
    for n in range(10):
        cols = slice(256 * n, 256 * n + 256)
        part = jnp.dot(left, w[:, cols], preferred_element_type=F32)
        first = 0
        for out in outs:
            out[:, cols] = part[first : first + out.shape[0]].astype(out.dtype)
            first += out.shape[0]
    first = 0
    for out in outs:
        out[:, MODEL:] = sums[first : first + out.shape[0]].astype(out.dtype)
        first += out.shape[0]


def send_kernel(e0, e1, e2, e3, c, cum, inside, gate, gain, w, state, out, out_rest):
    x = lax.axis_index("x")
    for d, piece in zip(MASKS, (e0, e1, e2, e3)):
        state[row_at(other_index(x, d), 32), :] = piece[...]
    project_rows(FIRST + REST, 1 - lax.axis_index("c"), state, c, cum, inside, gate, gain, w, out, out_rest)


def keep_first_kernel(state, c, cum, inside, gate, gain, w, out):
    project_rows(FIRST, lax.axis_index("c"), state, c, cum, inside, gate, gain, w, out)


def keep_rest_kernel(state, c, cum, inside, gate, gain, w, before, out):
    project_rows(REST, lax.axis_index("c"), state, c, cum, inside, gate, gain, w, out)


def pair_kernel(own, came, *outs):
    for k, out in enumerate(outs):
        rows = slice(ROWS * k, ROWS * k + ROWS)
        total = own[rows, :] + came[rows, :].astype(F32)
        out[:, :MODEL] = total[:, :MODEL].astype(out.dtype)
        both = jnp.sum(total[:, MODEL:], axis=1, keepdims=True)
        out[:, MODEL:] = square_cols(jnp.broadcast_to(both, (ROWS, 128))).astype(out.dtype)


def finish_kernel(f0, g1, g2, g3, out):
    total = f0[...] + g1[...].astype(F32) + g2[...].astype(F32) + g3[...].astype(F32)
    squares = jnp.sum(total[:, MODEL:], axis=1, keepdims=True)
    out[...] = (total[:, :MODEL] * lax.rsqrt(squares / DI + 1.0)).astype(BF)


def body(tokens, w_xz, w_bc, w_dt, dt_bias, a_log, conv_x, conv_bc, norm_gain, w_out):
    w_both = w_xz.reshape(MODEL, 2 * WIDTH)
    near, far = [tokens], [swapped(tokens, "c", 1)]
    for mask in TOKEN_MASKS[1:]:
        near.append(swapped(tokens, "y", mask))
    near[3], w_both = lax.optimization_barrier((near[3], w_both))
    for mask, piece in zip(TOKEN_MASKS[1:], near[1:]):
        far.append(swapped(piece, "c", 1))
    (gain,) = call(gain_kernel, [((1, WIDTH), F32)], [norm_gain[None]])
    (part,) = call(
        project_early_kernel,
        [((192, PRE), BF)],
        [*near, far[0], far[3], w_both, w_bc],
        scratch=[((192, MODEL), BF)],
        flops=2 * 192 * MODEL * 1024,
    )
    pre, tail = call(
        project_kernel,
        [((BLOCK, PRE), BF), ((8, PRE), BF)],
        [far[1], far[2], part, w_both, w_bc, gain],
        scratch=[((64, MODEL), BF), ((64, PRE), BF)],
        flops=2 * 64 * MODEL * 1024,
    )
    tail = lax.ppermute(tail, SEQ, [(i, (i + 1) % 32) for i in range(32)])
    everything, v, b, c, step, cum, weight, factor, main = call(
        prepare_kernel,
        [((BLOCK, MODEL), BF), ((BLOCK, WIDTH), BF), ((BLOCK, STATE), BF), ((BLOCK, STATE), BF), ((BLOCK, 128), F32), ((BLOCK, 128), F32)]
        + [((8, 128), F32), ((8, 128), F32), ((STATE, WIDTH), F32)],
        [pre, *near, *far, w_dt.T, conv_x, conv_bc, dt_bias[None], a_log[None]],
        scratch=[((BLOCK + 8, PRE), F32), ((8, 128), F32), ((128, MODEL), BF)],
        flops=2 * BLOCK * STATE * WIDTH,
    )
    v_first, b_first, c_first, p0, p1, p2, p3 = call(
        local_kernel,
        [((8, WIDTH), BF), ((8, STATE), BF), ((8, STATE), BF)] + [((PIECE, 128), BF)] * 4,
        [tail, pre, conv_x, conv_bc, weight, factor, main],
        scratch=[((16, PRE), F32), ((STATE, WIDTH), F32)],
    )
    rows = exchanged([p0, p1, p2, p3], "x", MASKS)
    inside, c_all = call(
        inside_kernel,
        [((BLOCK, WIDTH), F32), ((BLOCK, STATE), BF)],
        [v, b, c, v_first, b_first, c_first, step, cum],
        scratch=[((BLOCK, WIDTH), BF), ((BLOCK, STATE), BF)],
        flops=20 * BLOCK * BLOCK * 256,
    )
    (gate,) = call(gate_kernel, [((BLOCK, WIDTH), F32)], [everything, w_both, v_first], flops=2 * BLOCK * MODEL * WIDTH)
    piece = [((PIECE, 128), BF)]
    (row,) = call(row_total_kernel, piece, [*rows, inside, gate], scratch=[((4, PIECE, 128), F32)])
    other = swapped(row, "z", 1)
    (two,) = call(pair_total_kernel, piece, [row, other])
    previous = swapped(two, "z", 2)
    (four,) = call(quad_total_kernel, piece, [row, other, previous])
    quad = swapped(four, "z", 7)
    e0, e1, e2, e3 = call(
        incoming_kernel,
        [((32, WIDTH), BF)] * 4,
        [*rows, row, other, previous, quad],
        scratch=[((4, PIECE, 128), F32), ((4, 32, WIDTH), F32)],
    )
    states = exchanged([e0, e1, e2, e3], "x", MASKS)
    shared = [c_all, cum, inside, gate, gain, w_out]
    flops = 2 * 96 * WIDTH * MODEL
    state, send, send_rest = call(
        send_kernel, [((STATE, WIDTH), BF), ((ROWS, WIDE), BF), ((96, WIDE), BF)], [*states, *shared], flops=flops
    )
    came = swapped(send, "c", 1)
    came_rest = swapped(send_rest, "c", 1)
    (own,) = call(keep_first_kernel, [((ROWS, WIDE), F32)], [state, *shared], flops=flops)
    (first,) = call(pair_kernel, [((ROWS, WIDE), BF)], [own, came])
    arrived = swapped(first, "y", FIRST[0])
    (own,) = call(keep_rest_kernel, [((96, WIDE), F32)], [state, *shared, first], flops=flops)
    one, three, here = call(
        pair_kernel, [((ROWS, WIDE), BF), ((ROWS, WIDE), BF), ((ROWS, WIDE), F32)], [own, came_rest]
    )
    (out,) = call(
        finish_kernel, [((ROWS, MODEL), BF)], [here, arrived, swapped(one, "y", REST[0]), swapped(three, "y", REST[1])]
    )
    return out


def solution(mesh):
    split = Mesh(mesh.devices.reshape(8, 4, 4, 2), ALL)
    in_specs = (
        P(ALL, None),
        P(None, None, HEAD),
        P(),
        P(None, HEAD),
        P(HEAD),
        P(HEAD),
        P(None, HEAD),
        P(),
        P(HEAD),
        P(HEAD, None),
    )

    return jax.shard_map(body, mesh=split, in_specs=in_specs, out_specs=P(ALL, None), check_vma=False)
```

```python
import jax
import jax.numpy as jnp
from jax import lax
from jax.experimental import pallas as pl
from jax.experimental.pallas import tpu as pltpu
from jax.sharding import Mesh
from jax.sharding import PartitionSpec as P

DI = 5120
SEQ = ("z", "x")
ALL = ("z", "x", "y", "c")
HEAD = ("y", "c")
BF = jnp.bfloat16
F32 = jnp.float32
ROWS = 32
BLOCK = 256
WIDTH = 640
STATE = 128
PRE = WIDTH + 2 * STATE
MODEL = 2560
WIDE = MODEL + 128
PIECE = 168
MASKS = (0, 2, 1, 3)
FIRST = (2,)
REST = (1, 3, 0)
TOKEN_MASKS = (0, 1, 3, 2)


def whole(count):
    return [pl.BlockSpec(memory_space=pltpu.VMEM)] * count


def call(body, outs, args, scratch=(), flops=0):
    return pl.pallas_call(
        body,
        out_shape=[jax.ShapeDtypeStruct(s, t) for s, t in outs],
        in_specs=whole(len(args)),
        out_specs=whole(len(outs)),
        scratch_shapes=[pltpu.VMEM(s, t) for s, t in scratch],
        compiler_params=pltpu.CompilerParams(vmem_limit_bytes=24 << 20),
        cost_estimate=pl.CostEstimate(flops=flops, transcendentals=0, bytes_accessed=flops // 500),
    )(*args)


def swapped(value, axis, mask):
    return lax.ppermute(value, axis, [(i, i ^ mask) for i in range(lax.axis_size(axis))])


def exchanged(pieces, axis, masks):
    return [swapped(piece, axis, mask) if mask else piece for mask, piece in zip(masks, pieces)]


def other_index(index, mask):
    return lax.bitwise_xor(index, jnp.int32(mask))


def row_at(index, rows):
    return pl.ds(pl.multiple_of(index * rows, rows), rows)


def gain_kernel(gain, out):
    out[...] = gain[...]


def project_into(tokens, w, w_bc, out):
    for lo, hi in ((0, 256), (256, 512), (512, WIDTH)):
        out[:, lo:hi] = jnp.dot(tokens[...], w[:, lo:hi], preferred_element_type=F32).astype(BF)
    out[:, WIDTH:] = jnp.dot(tokens[...], w_bc[...], preferred_element_type=F32).astype(BF)


def project_three_kernel(a, b, c, w, w_bc, out, tokens):
    for k, piece in enumerate((a, b, c)):
        tokens[32 * k : 32 * k + 32, :] = piece[...]
    project_into(tokens, w, w_bc, out)


def project_kernel(o1, o2, part_zero, part, w, w_bc, early, pre_out, tail_out, late, rest):
    y, c = lax.axis_index("y"), lax.axis_index("c")
    near = [row_at(other_index(y, mask) * 2 + c, ROWS) for mask in TOKEN_MASKS]
    far = [row_at(other_index(y, mask) * 2 + 1 - c, ROWS) for mask in TOKEN_MASKS]
    late[0:32, :] = o1[...]
    late[32:64, :] = o2[...]
    project_into(late, w, w_bc, rest)
    for k, rows in enumerate((near[0], near[3], far[0])):
        pre_out[rows, :] = part_zero[32 * k : 32 * k + 32, :]
    for k, rows in enumerate((near[1], near[2], far[3])):
        pre_out[rows, :] = part[32 * k : 32 * k + 32, :]
    for k, rows in enumerate(far[1:3]):
        pre_out[rows, :] = rest[32 * k : 32 * k + 32, :]
    tail_out[...] = pre_out[BLOCK - 8 :, :]


def gate_kernel(tokens, w, before, out):
    for lo, hi in ((0, 256), (256, 512), (512, WIDTH)):
        gate = jnp.dot(tokens[...], w[:, WIDTH + lo : WIDTH + hi], preferred_element_type=F32)
        out[:, lo:hi] = jax.nn.silu(gate.astype(BF).astype(F32))


def spread(value, pair):
    rows = value.shape[0]
    lane = lax.broadcasted_iota(jnp.int32, (rows, 128), 1)
    left = jnp.broadcast_to(value[:, 2 * pair : 2 * pair + 1], (rows, 128))
    right = jnp.broadcast_to(value[:, 2 * pair + 1 : 2 * pair + 2], (rows, 128))
    return jnp.where(lane < 64, left, right)


def halves(value):
    high = value.astype(BF)
    return high, (value - high.astype(F32)).astype(BF)


def mixed(ext, first, kernel, lo, rows):
    total = jnp.zeros((rows, 128), F32)
    for k in range(4):
        total = total + kernel[k : k + 1, lo : lo + 128].astype(F32) * ext[5 + k : 5 + k + rows, first : first + 128]
    return jax.nn.silu(total).astype(BF)


def prepare_kernel(
    pre,
    t0,
    t1,
    t2,
    t3,
    o0,
    o1,
    o2,
    o3,
    w_dt,
    conv_x,
    conv_bc,
    bias,
    a_log,
    tokens,
    v_out,
    b_out,
    c_out,
    dt_out,
    cum_out,
    weight_out,
    factor_out,
    state_out,
    ext,
    small,
    w_steps,
):
    y, c = lax.axis_index("y"), lax.axis_index("c")
    for mask, own, other in zip(TOKEN_MASKS, (t0, t1, t2, t3), (o0, o1, o2, o3)):
        tokens[row_at(other_index(y, mask) * 2 + c, ROWS), :] = own[...]
        tokens[row_at(other_index(y, mask) * 2 + 1 - c, ROWS), :] = other[...]
    w_steps[...] = jnp.zeros(w_steps.shape, BF)
    w_steps[0 : w_dt.shape[0], :] = w_dt[...]
    dt_pre = lax.dot_general(tokens[...], w_steps[...], (((1,), (1,)), ((), ())), preferred_element_type=F32)
    ext[0:8, :] = jnp.zeros((8, PRE), F32)
    ext[8 : 8 + BLOCK, :] = pre[...].astype(F32)
    small[...] = jnp.zeros(small.shape, F32)
    small[0:1, 0 : bias.shape[1]] = bias[...]
    small[1:2, 0 : bias.shape[1]] = a_log[...]
    step = jax.nn.softplus(dt_pre + small[0:1, :])
    decay = step * (-jnp.exp(small[1:2, :]))
    row = lax.broadcasted_iota(jnp.int32, decay.shape, 0)
    cum = decay
    for k in (1, 2, 4, 8, 16, 32, 64, 128):
        cum = cum + jnp.where(row >= k, pltpu.roll(cum, k, 0), 0.0)
    dt_out[...] = step
    cum_out[...] = cum
    last = cum[BLOCK - 1 : BLOCK, :]
    weight = jnp.exp(last - cum) * step
    weight_out[...] = weight[0:8, :]
    factor_out[...] = jnp.broadcast_to(jnp.exp(last), (8, 128))
    weight = jnp.where(row >= 3, weight, 0.0)
    b = mixed(ext, WIDTH, conv_bc, 0, BLOCK)
    b_out[...] = b
    c_out[...] = mixed(ext, WIDTH + STATE, conv_bc, STATE, BLOCK)
    b_rows = b.astype(F32).T.astype(BF)
    for pair in range(5):
        cols = slice(128 * pair, 128 * pair + 128)
        v = mixed(ext, 128 * pair, conv_x, 128 * pair, BLOCK)
        v_out[:, cols] = v
        scaled = (spread(weight, pair) * v.astype(F32)).astype(BF)
        state_out[:, cols] = jnp.dot(b_rows, scaled, preferred_element_type=F32)


def decay_rows(factor):
    high, low = halves(factor)
    row = lax.broadcasted_iota(jnp.int32, (8, 128), 0)
    return jnp.where(row == 0, high.astype(F32), jnp.where(row == 1, low.astype(F32), 0.0)).astype(BF)


def local_kernel(tail, pre, conv_x, conv_bc, weight, factor, main, v_out, b_out, c_out, p0, p1, p2, p3, ext, state):
    x = lax.axis_index("x")
    first = jnp.logical_and(lax.axis_index("z") == 0, x == 0)
    ext[0:8, :] = jnp.where(first, 0.0, tail[...].astype(F32))
    ext[8:16, :] = pre[0:8, :].astype(F32)
    b = mixed(ext, WIDTH, conv_bc, 0, 8)
    b_out[...] = b
    c_out[...] = mixed(ext, WIDTH + STATE, conv_bc, STATE, 8)
    b_rows = jnp.broadcast_to(b.astype(F32)[None], (16, 8, 128)).reshape(128, 128).T
    extra = decay_rows(factor[0:1, :])
    for pair in range(5):
        cols = slice(128 * pair, 128 * pair + 128)
        v = mixed(ext, 128 * pair, conv_x, 128 * pair, 8)
        v_out[:, cols] = v
        scaled = (spread(weight[...], pair) * v.astype(F32)).astype(BF).astype(F32)
        total = main[:, cols]
        for k in range(3):
            total = total + b_rows[:, k : k + 1] * scaled[k : k + 1, :]
        state[:, cols] = total
    for d, out in zip(MASKS, (p0, p1, p2, p3)):
        rows = row_at(other_index(x, d), 32)
        for pair in range(5):
            out[32 * pair : 32 * pair + 32, :] = state[rows, 128 * pair : 128 * pair + 128].astype(BF)
        out[160:168, :] = extra


def inside_kernel(v, b, c, v_first, b_first, c_first, step, cum, out, c_out, values, b_all):
    values[...] = v[...]
    values[0:8, :] = v_first[...]
    b_all[...] = b[...]
    b_all[0:8, :] = b_first[...]
    c_out[...] = c[...]
    c_out[0:8, :] = c_first[...]
    scores = jnp.dot(c_out[...], b_all[...].astype(F32).T.astype(BF), preferred_element_type=F32)
    t = lax.broadcasted_iota(jnp.int32, (BLOCK, BLOCK), 0)
    s = lax.broadcasted_iota(jnp.int32, (BLOCK, BLOCK), 1)
    scores = jnp.where(t >= s, scores, 0.0)
    cum_all = cum[...]
    cum_rows = cum_all.T
    step_rows = step[...].T
    lane = lax.broadcasted_iota(jnp.int32, (BLOCK, 128), 1)
    for pair in range(5):
        cols = slice(128 * pair, 128 * pair + 128)
        value = values[:, cols]
        parts = []
        for h in (2 * pair, 2 * pair + 1):
            differ = jnp.broadcast_to(cum_all[:, h : h + 1], (BLOCK, BLOCK)) - cum_rows[h : h + 1, :]
            weight = jnp.exp(jnp.minimum(differ, 0.0)) * (scores * step_rows[h : h + 1, :])
            parts.append(jnp.dot(weight.astype(BF), value, preferred_element_type=F32))
        out[:, cols] = jnp.where(lane < 64, parts[0], parts[1])


def load_rows(pieces, held):
    x = lax.axis_index("x")
    for d, piece in zip(MASKS, pieces):
        held[other_index(x, d)] = piece[...].astype(F32)


def split(piece):
    return [piece[32 * k : 32 * k + 32] for k in range(5)], piece[160:161] + piece[161:162]


def unpack(ref):
    return split(ref[...].astype(F32))


def pack(out, item):
    for k, part in enumerate(item[0]):
        out[32 * k : 32 * k + 32, :] = part.astype(BF)
    out[160:168, :] = decay_rows(item[1])


def follow(earlier, later):
    return [e * spread(later[1], k) + l for k, (e, l) in enumerate(zip(earlier[0], later[0]))], earlier[1] * later[1]


def choose(test, yes, no):
    return [jnp.where(test, y, n) for y, n in zip(yes[0], no[0])], jnp.where(test, yes[1], no[1])


def row_total_kernel(q0, q1, q2, q3, before, before_too, out, held):
    load_rows((q0, q1, q2, q3), held)
    total = split(held[0])
    for k in range(1, 4):
        total = follow(total, split(held[k]))
    pack(out, total)


def two_rows(row, other):
    odd = lax.rem(lax.axis_index("z"), 2) == 1
    mine, theirs = unpack(row), unpack(other)
    return odd, theirs, follow(choose(odd, theirs, mine), choose(odd, mine, theirs))


def pair_total_kernel(row, other, before, out):
    pack(out, two_rows(row, other)[2])


def quad_total_kernel(row, other, previous, out):
    first = lax.rem(lax.axis_index("z"), 4) < 2
    mine, theirs = two_rows(row, other)[2], unpack(previous)
    pack(out, follow(choose(first, mine, theirs), choose(first, theirs, mine)))


def incoming_kernel(q0, q1, q2, q3, row, other, previous, quad, e0, e1, e2, e3, held, ready):
    z, x = lax.axis_index("z"), lax.axis_index("x")
    load_rows((q0, q1, q2, q3), held)
    odd, theirs, _ = two_rows(row, other)
    carry = choose(odd, theirs, ([jnp.zeros((32, 128), F32)] * 5, jnp.ones((1, 128), F32)))
    second = lax.rem(z, 4) >= 2
    carry = choose(second, follow(unpack(previous), carry), carry)
    carry = choose(z >= 4, follow(unpack(quad), carry), carry)
    for k in range(4):
        for j, part in enumerate(carry[0]):
            ready[k, :, 128 * j : 128 * j + 128] = part
        if k < 3:
            carry = follow(carry, split(held[k]))
    for d, out in zip(MASKS, (e0, e1, e2, e3)):
        out[...] = ready[other_index(x, d)].astype(BF)


def square_cols(total):
    high, low = halves(total)
    lane = lax.broadcasted_iota(jnp.int32, total.shape, 1)
    return jnp.where(lane == 0, high.astype(F32), jnp.where(lane == 1, low.astype(F32), 0.0)).astype(BF)


def order_kernel(c, cum, inside, gate, c_out, grown_out, inside_out, gate_out):
    y, core = lax.axis_index("y"), lax.axis_index("c")
    start = 0
    for masks in (FIRST, REST):
        for side, mask in [(side, mask) for side in (1 - core, core) for mask in masks]:
            source = row_at(2 * other_index(y, mask) + side, ROWS)
            rows = slice(start, start + 32)
            start += 32
            c_out[rows, :] = c[source, :]
            inside_out[rows, :] = inside[source, :]
            gate_out[rows, :] = gate[source, :]
            grown = jnp.exp(cum[source, :])
            for pair in range(5):
                grown_out[rows, 128 * pair : 128 * pair + 128] = spread(grown, pair)


def project_rows(rows, state, c, grown, inside, gate, gain, w, *outs):
    squares = jnp.zeros((rows.stop - rows.start, 128), F32)
    left = []
    for pair in range(5):
        cols = slice(128 * pair, 128 * pair + 128)
        came = jnp.dot(c[rows, :], state[:, cols], preferred_element_type=F32)
        gated = (inside[rows, cols] + grown[rows, cols] * came) * gate[rows, cols]
        squares = squares + gated * gated
        left.append((gated * gain[:, cols]).astype(BF))
    left = jnp.concatenate(left, axis=1)
    sums = square_cols(jnp.broadcast_to(jnp.sum(squares, axis=1, keepdims=True), squares.shape))
    for n in range(10):
        cols = slice(256 * n, 256 * n + 256)
        part = jnp.dot(left, w[:, cols], preferred_element_type=F32)
        first = 0
        for out in outs:
            out[:, cols] = part[first : first + out.shape[0]].astype(out.dtype)
            first += out.shape[0]
    first = 0
    for out in outs:
        out[:, MODEL:] = sums[first : first + out.shape[0]].astype(out.dtype)
        first += out.shape[0]


def first_kernel(e0, e1, e2, e3, c, grown, inside, gate, gain, w, state, send, keep):
    x = lax.axis_index("x")
    for d, piece in zip(MASKS, (e0, e1, e2, e3)):
        state[row_at(other_index(x, d), 32), :] = piece[...]
    project_rows(slice(0, 64), state, c, grown, inside, gate, gain, w, send, keep)


def send_rest_kernel(state, c, grown, inside, gate, gain, w, out):
    project_rows(slice(64, 160), state, c, grown, inside, gate, gain, w, out)


def keep_rest_kernel(state, c, grown, inside, gate, gain, w, before, out):
    project_rows(slice(160, 256), state, c, grown, inside, gate, gain, w, out)


def pair_kernel(own, came, *outs):
    for k, out in enumerate(outs):
        rows = slice(ROWS * k, ROWS * k + ROWS)
        total = own[rows, :] + came[rows, :].astype(F32)
        out[:, :MODEL] = total[:, :MODEL].astype(out.dtype)
        both = jnp.sum(total[:, MODEL:], axis=1, keepdims=True)
        out[:, MODEL:] = square_cols(jnp.broadcast_to(both, (ROWS, 128))).astype(out.dtype)


def add_kernel(f0, g1, out):
    out[...] = f0[...] + g1[...].astype(F32)


def finish_kernel(f0, g2, g3, out):
    total = f0[...] + g2[...].astype(F32) + g3[...].astype(F32)
    squares = jnp.sum(total[:, MODEL:], axis=1, keepdims=True)
    out[...] = (total[:, :MODEL] * lax.rsqrt(squares / DI + 1.0)).astype(BF)


def body(tokens, w_xz, w_bc, w_dt, dt_bias, a_log, conv_x, conv_bc, norm_gain, w_out):
    w_both = w_xz.reshape(MODEL, 2 * WIDTH)
    near, far = [tokens], [swapped(tokens, "c", 1)]
    for mask in TOKEN_MASKS[1:]:
        near.append(swapped(tokens, "y", mask))
    near[3], w_both = lax.optimization_barrier((near[3], w_both))
    for mask, piece in zip(TOKEN_MASKS[1:], near[1:]):
        far.append(swapped(piece, "c", 1))
    (gain,) = call(gain_kernel, [((1, WIDTH), F32)], [norm_gain[None]])
    parts = []
    for pieces in ((near[0], near[3], far[0]), (near[1], near[2], far[3])):
        parts += call(
            project_three_kernel,
            [((96, PRE), BF)],
            [*pieces, w_both, w_bc],
            scratch=[((96, MODEL), BF)],
            flops=2 * 96 * MODEL * 1024,
        )
    pre, tail = call(
        project_kernel,
        [((BLOCK, PRE), BF), ((8, PRE), BF)],
        [far[1], far[2], *parts, w_both, w_bc, gain],
        scratch=[((64, MODEL), BF), ((64, PRE), BF)],
        flops=2 * 64 * MODEL * 1024,
    )
    tail = lax.ppermute(tail, SEQ, [(i, (i + 1) % 32) for i in range(32)])
    everything, v, b, c, step, cum, weight, factor, main = call(
        prepare_kernel,
        [((BLOCK, MODEL), BF), ((BLOCK, WIDTH), BF), ((BLOCK, STATE), BF), ((BLOCK, STATE), BF), ((BLOCK, 128), F32), ((BLOCK, 128), F32)]
        + [((8, 128), F32), ((8, 128), F32), ((STATE, WIDTH), F32)],
        [pre, *near, *far, w_dt.T, conv_x, conv_bc, dt_bias[None], a_log[None]],
        scratch=[((BLOCK + 8, PRE), F32), ((8, 128), F32), ((128, MODEL), BF)],
        flops=2 * BLOCK * STATE * WIDTH,
    )
    v_first, b_first, c_first, p0, p1, p2, p3 = call(
        local_kernel,
        [((8, WIDTH), BF), ((8, STATE), BF), ((8, STATE), BF)] + [((PIECE, 128), BF)] * 4,
        [tail, pre, conv_x, conv_bc, weight, factor, main],
        scratch=[((16, PRE), F32), ((STATE, WIDTH), F32)],
    )
    rows = exchanged([p0, p1, p2, p3], "x", MASKS)
    inside, c_all = call(
        inside_kernel,
        [((BLOCK, WIDTH), F32), ((BLOCK, STATE), BF)],
        [v, b, c, v_first, b_first, c_first, step, cum],
        scratch=[((BLOCK, WIDTH), BF), ((BLOCK, STATE), BF)],
        flops=20 * BLOCK * BLOCK * 256,
    )
    (gate,) = call(gate_kernel, [((BLOCK, WIDTH), F32)], [everything, w_both, v_first], flops=2 * BLOCK * MODEL * WIDTH)
    piece = [((PIECE, 128), BF)]
    (row,) = call(row_total_kernel, piece, [*rows, inside, gate], scratch=[((4, PIECE, 128), F32)])
    other = swapped(row, "z", 1)
    c_all, grown, inside, gate = call(
        order_kernel,
        [((BLOCK, STATE), BF), ((BLOCK, WIDTH), F32), ((BLOCK, WIDTH), F32), ((BLOCK, WIDTH), F32)],
        [c_all, cum, inside, gate],
    )
    (two,) = call(pair_total_kernel, piece, [row, other, c_all])
    previous = swapped(two, "z", 2)
    (four,) = call(quad_total_kernel, piece, [row, other, previous])
    quad = swapped(four, "z", 7)
    e0, e1, e2, e3 = call(
        incoming_kernel,
        [((32, WIDTH), BF)] * 4,
        [*rows, row, other, previous, quad],
        scratch=[((4, PIECE, 128), F32), ((4, 32, WIDTH), F32)],
    )
    states = exchanged([e0, e1, e2, e3], "x", MASKS)
    shared = [c_all, grown, inside, gate, gain, w_out]
    flops = 2 * 96 * WIDTH * MODEL
    state, send, own = call(
        first_kernel, [((STATE, WIDTH), BF), ((ROWS, WIDE), BF), ((ROWS, WIDE), F32)], [*states, *shared], flops=flops
    )
    came = swapped(send, "c", 1)
    (send_rest,) = call(send_rest_kernel, [((96, WIDE), BF)], [state, *shared], flops=flops)
    came_rest = swapped(send_rest, "c", 1)
    (first,) = call(pair_kernel, [((ROWS, WIDE), BF)], [own, came])
    arrived = swapped(first, "y", FIRST[0])
    (own,) = call(keep_rest_kernel, [((96, WIDE), F32)], [state, *shared, first], flops=flops)
    one, three, here = call(
        pair_kernel, [((ROWS, WIDE), BF), ((ROWS, WIDE), BF), ((ROWS, WIDE), F32)], [own, came_rest]
    )
    (here,) = call(add_kernel, [((ROWS, WIDE), F32)], [here, arrived])
    (out,) = call(
        finish_kernel, [((ROWS, MODEL), BF)], [here, swapped(one, "y", REST[0]), swapped(three, "y", REST[1])]
    )
    return out


def solution(mesh):
    split = Mesh(mesh.devices.reshape(8, 4, 4, 2), ALL)
    in_specs = (
        P(ALL, None),
        P(None, None, HEAD),
        P(),
        P(None, HEAD),
        P(HEAD),
        P(HEAD),
        P(None, HEAD),
        P(),
        P(HEAD),
        P(HEAD, None),
    )

    return jax.shard_map(body, mesh=split, in_specs=in_specs, out_specs=P(ALL, None), check_vma=False)
```
